128 devices in a mesh: row: 8 (over x, z_hi), col: 16 (over z_lo, y, core).
Axes of the slice: x: 4, y: 4, z: 4 (z_hi: 2, z_lo: 2; z = z_hi * 2 + z_lo), core: 2. Of those that a mesh axis runs over, the one named last changes fastest.
Arguments:
- covariance: float32 [16384, 16384], P('row', 'col'), may hold values from -1 to 560
- seed_index: int32 [128], replicated, may hold values from 0 to 16383, as said below
Outputs:
- basis: float32 [16384, 384], P('row')
- projection: float32 [384, 256], replicated
- first_pass: float32 [384, 256], replicated
The draws below stay inside these ranges and needn't reach their ends.
Inputs may be any that keep to these rules, and one draw needn't show every extreme that they name: `seed_index`: 128 distinct column indices.
All inputs are finite; a program needn't handle non-finite values.
Results may differ from the reference program's by a relative error of at most 0.00019.
Values sent between devices are 32-bit elements; how exact they have to be, the bound alone decides.
No kernel may reach another device: no remote copies, remote signals or barrier semaphores. Data moves between devices by JAX's collectives and lax.ppermute only.
A program may use at most 128 MiB of HBM per device.

```python
import jax
import jax.numpy as jnp
from jax import lax

N = 16384
B = 128
ITERS = 2


def draw_covariance(key, part):
    first_key = jax.random.fold_in(key, 11)
    second_key = jax.random.fold_in(key, 12)
    place = jnp.arange(N, dtype=jnp.float32) / jnp.float32(N - 1)
    noise = jax.random.normal(first_key, (N, N), jnp.float32)
    loading = jnp.exp(jax.random.uniform(second_key, (N,), jnp.float32, jnp.log(8.0), jnp.log(40.0)))
    loading = loading * (1.0 + 2.0 * place)
    symmetric = (noise + noise.T) * (3.0 / (2.0 * N) ** 0.5)
    return symmetric + jnp.diag(loading)


def draw_seed_index(key, part):
    order = jax.random.permutation(jax.random.fold_in(key, 21), N)
    return order[:B].astype(jnp.int32)


def setup_inputs(seed: int = 0) -> dict:
    arg_keys = jax.random.split(jax.random.key(seed), 3)
    covariance = draw_covariance(jax.random.fold_in(arg_keys[2], 71), 0)
    seed_index = draw_seed_index(jax.random.fold_in(arg_keys[2], 71), 0)
    return dict(covariance=covariance, seed_index=seed_index)


def product(left, right):
    return jnp.dot(left.astype(jnp.float32), right.astype(jnp.float32), precision=lax.Precision.HIGHEST, preferred_element_type=jnp.float32)

def orthonormal(block):
    gram = product(block.T, block)
    lower = jnp.linalg.cholesky(gram)
    basis_block = jax.scipy.linalg.solve_triangular(lower, block.T, lower=True).T
    return (basis_block, lower.T)

def reference(covariance, seed_index):
    start = jnp.take(covariance, seed_index.astype(jnp.int32), axis=1)
    current, upper = orthonormal(start)
    blocks = [current]
    projection = jnp.zeros(((ITERS + 1) * B, ITERS * B), jnp.float32)
    first_pass = jnp.zeros(((ITERS + 1) * B, ITERS * B), jnp.float32)
    for section in range(ITERS):
        image = product(covariance, current)
        stacked = jnp.concatenate(blocks, axis=1)
        first = product(stacked.T, image)
        once = image - product(stacked, first)
        second = product(stacked.T, once)
        twice = once - product(stacked, second)
        current, upper = orthonormal(twice)
        projection = projection.at[:(section + 1) * B, section * B:(section + 1) * B].set(first + second)
        projection = projection.at[(section + 1) * B:(section + 2) * B, section * B:(section + 1) * B].set(upper)
        first_pass = first_pass.at[:(section + 1) * B, section * B:(section + 1) * B].set(first)
        blocks.append(current)
    basis = jnp.concatenate(blocks, axis=1) * jnp.float32(N ** 0.5)
    return (basis, projection, first_pass)
```

```python
import jax
import jax.numpy as jnp
import numpy as np
from jax import lax
from jax.sharding import Mesh, PartitionSpec as P

ROWS = "row"
CHIP = "chip"
CORE = "core"
ALL = (ROWS, CHIP, CORE)
SWAP = [(0, 1), (1, 0)]


def product(left, right):
    return jnp.dot(left, right, precision=lax.Precision.HIGHEST, preferred_element_type=jnp.float32)


def scattered(parts, axis):
    return jnp.sum(lax.all_to_all(parts, axis, 0, 0, tiled=True), axis=0)


def gathered(part, axis):
    copies = jnp.broadcast_to(part, (lax.axis_size(axis), *part.shape))
    return lax.all_to_all(copies, axis, 0, 0, tiled=True)


def other_core(value):
    return lax.ppermute(value, CORE, SWAP)


def turned(rows, chips, cores):
    return [
        ((r * chips + a) * cores + b, (a * chips + r) * cores + b)
        for r in range(rows)
        for a in range(chips)
        for b in range(cores)
    ]


def in_order(mine, theirs, core):
    first = core == 0
    return jnp.concatenate([jnp.where(first, mine, theirs), jnp.where(first, theirs, mine)])


def small_algebra(g00, cee, g01, g11, g12, g22, order):
    f32 = jnp.float32
    eye = jnp.eye(g00.shape[0], dtype=f32)

    def factor(gram):
        lower = jnp.linalg.cholesky(gram)
        inverse = jax.scipy.linalg.solve_triangular(lower, eye, lower=True)
        return lower.T, inverse.T

    g02 = g11 + product(cee.T, g01)
    r0, x0 = factor(g00)
    m00 = product(x0.T, product(g00, x0))
    u0 = product(cee, x0)
    h_first = product(x0.T, product(g01, x0)) + product(m00, product(r0, u0))
    h_full = h_first + (h_first - product(m00, h_first))
    d0 = product(x0, h_full) - u0
    t = product(g01, x0) - product(g00, d0)
    n = product(g11, x0) - product(g01.T, d0)
    r1, x1 = factor(product(x0.T, n) - product(d0.T, t))
    a1 = product(x0, x1)
    b1 = product(d0, x1)
    f1 = product(cee, b1)
    s0 = product(g02, a1) - product(g01, b1) - product(g00, f1)
    s1 = product(g12, a1) - product(g11, b1) - product(g01.T, f1)
    first0 = product(x0.T, s0)
    first1 = product(a1.T, s1) - product(b1.T, s0)
    tx = product(t, x1)
    m01 = product(x0.T, tx)
    m11 = product(a1.T, product(n, x1)) - product(b1.T, tx)
    full0 = first0 + (first0 - product(m00, first0) - product(m01, first1))
    full1 = first1 + (first1 - product(m01.T, first0) - product(m11, first1))
    b = b1 + product(a1, full1)
    c = f1 + product(x0, full0) - product(b1, full1)
    w0 = product(g02, a1) - product(g01, b) - product(g00, c)
    w1 = product(g12, a1) - product(g11, b) - product(g01.T, c)
    w2 = product(g22, a1) - product(g12.T, b) - product(g02.T, c)
    r2, x2 = factor(product(a1.T, w2) - product(b.T, w1) - product(c.T, w0))
    zero = jnp.zeros_like(x0)
    mix = jnp.block(
        [[x0, -b1, -product(c, x2)], [zero, a1, -product(b, x2)], [zero, zero, product(a1, x2)]]
    ) * f32(order**0.5)
    projection = jnp.block([[h_full, full0], [r1, full1], [zero, r2]])
    first_pass = jnp.block([[h_first, first0], [zero, first1], [zero, zero]])
    return mix, projection, first_pass


def local(covariance, seed_index):
    height, breadth = covariance.shape
    width = seed_index.shape[0]
    rows, chips, cores = (lax.axis_size(a) for a in ALL)
    row, chip, core = (lax.axis_index(a) for a in ALL)
    order = height * rows
    share = breadth // rows
    half = height // cores
    offsets = seed_index - row * height
    inside = (offsets >= 0) & (offsets < height)
    picked = jnp.take(covariance, jnp.clip(offsets, 0, height - 1), axis=0)
    picked = jnp.where(inside[:, None], picked, 0.0)
    start_piece = scattered(picked.reshape(width, rows, share).transpose(1, 0, 2), ROWS).T
    start = gathered(start_piece, ROWS).reshape(breadth, width)
    lines = (chip * cores + core) * breadth + jnp.arange(breadth, dtype=jnp.int32)
    hot = lines[:, None] == seed_index[None, :]
    rest = jnp.where(jnp.any(hot, axis=1)[:, None], 0.0, start)
    g00 = product(start.T, start)
    cee = product(hot.astype(jnp.float32).T, start)
    partial = product(covariance, rest)
    halves = (partial[:half], partial[half:])
    extras = (g00, cee)
    first = core == 0
    keep = jnp.concatenate([jnp.where(first, halves[0], halves[1]), jnp.where(first, extras[0], extras[1])])
    send = jnp.concatenate([jnp.where(first, halves[1], halves[0]), jnp.where(first, extras[1], extras[0])])
    summed = keep + other_core(send)
    parts = jnp.concatenate(
        [summed[:half].reshape(chips, half // chips, width), summed[half:].reshape(chips, width // chips, width)], axis=1
    )
    mine = gathered(scattered(parts, CHIP), CHIP)
    theirs = other_core(mine)
    cut = half // chips
    step_mine, step_theirs = (v[:, :cut].reshape(half, width) for v in (mine, theirs))
    extra_mine, extra_theirs = (v[:, cut:].reshape(width, width) for v in (mine, theirs))
    g00 = jnp.where(first, extra_mine, extra_theirs)
    cee = jnp.where(first, extra_theirs, extra_mine)
    step = in_order(step_mine, step_theirs, core)
    g11 = product(step.T, step)
    partial = product(covariance.T, step)
    parts = jnp.concatenate([partial.reshape(rows, share, width), g11.reshape(rows, width // rows, width)], axis=1)
    piece = jnp.concatenate([scattered(parts, ROWS), start_piece])
    piece = lax.ppermute(piece, ALL, turned(rows, chips, cores))
    mine = gathered(piece, CHIP)
    extra = width // rows
    next_mine = mine[:, :share].reshape(half, width)
    g11 = mine[:, share : share + extra].reshape(width, width)
    start_mine = mine[:, share + extra :].reshape(half, width)
    grams = jnp.concatenate(
        [product(start_mine.T, step_mine), product(step_mine.T, next_mine), product(next_mine.T, next_mine)]
    )
    cut = grams.shape[0] // 2
    send = jnp.concatenate([next_mine, start_mine, jnp.where(first, grams[cut:], grams[:cut])])
    got = other_core(send)
    next_theirs, start_theirs = got[:half], got[half : 2 * half]
    grams = jnp.where(first, grams[:cut], grams[cut:]) + got[2 * half :]
    grams = jnp.sum(gathered(grams, ROWS), axis=0)
    grams = in_order(grams, other_core(grams), core)
    g01, g12, g22 = (grams[i * width : (i + 1) * width] for i in range(3))
    mix, projection, first_pass = small_algebra(g00, cee, g01, g11, g12, g22, order)
    mine = jnp.concatenate([start_mine, step_mine, next_mine], axis=1)
    theirs = jnp.concatenate([start_theirs, step_theirs, next_theirs], axis=1)
    basis = product(in_order(mine, theirs, core), mix)
    return basis, projection, first_pass


def solution(mesh):
    rows, cols = mesh.devices.shape
    fine = Mesh(mesh.devices.reshape(rows, cols // 2, 2), ALL)
    return jax.shard_map(
        local,
        mesh=fine,
        in_specs=(P(ROWS, (CHIP, CORE)), P()),
        out_specs=(P(ROWS, None), P(), P()),
        check_vma=False,
    )
```

```python
import jax
import jax.numpy as jnp
from jax import lax
from jax.experimental import pallas as pl
from jax.experimental.pallas import tpu as pltpu
from jax.sharding import Mesh, PartitionSpec as P

ROWS = "row"
CHIP = "chip"
CORE = "core"
ALL = (ROWS, CHIP, CORE)
SWAP = [(0, 1), (1, 0)]
W = 128
f32 = jnp.float32
HI = lax.Precision.HIGHEST


def dot(a, b, dims):
    return lax.dot_general(a, b, (dims, ((), ())), precision=HI, preferred_element_type=f32)


def nn(a, b):
    return dot(a, b, ((1,), (0,)))


def tn(a, b):
    return dot(a, b, ((0,), (0,)))


def nt(a, b):
    return dot(a, b, ((1,), (1,)))


def product(left, right):
    return jnp.dot(left, right, precision=lax.Precision.HIGH, preferred_element_type=f32)


def factor(gram, work, upper, inverse, unroll=1):
    sub = lax.broadcasted_iota(jnp.int32, (8, W), 0)
    lane = lax.broadcasted_iota(jnp.int32, (8, W), 1)
    work[:, :W] = gram
    work[:, W:] = (lax.broadcasted_iota(jnp.int32, (W, W), 0) == lax.broadcasted_iota(jnp.int32, (W, W), 1)).astype(f32)
    def step(j, carry):
        base = pl.multiple_of(j * 8, 8)
        left = work[pl.ds(base, 8), :W]
        right = work[pl.ds(base, 8), W:]
        turned = pltpu.roll(left, (W - base) % W, 1)
        cols = [jnp.broadcast_to(turned[:, k : k + 1], (8, W)) for k in range(8)]
        scale = jnp.zeros((8, W), f32)
        for k in range(8):
            def line(v): return jnp.broadcast_to(v[k : k + 1, :], (8, W))
            pivot = line(cols[k])
            root = lax.rsqrt(pivot)
            root = root * (1.5 - 0.5 * pivot * root * root)
            weight = jnp.where(sub > k, cols[k] * (root * root), 0.0)
            scale = jnp.where(sub == k, root, scale)
            left = left - weight * line(left)
            right = right - weight * line(right)
            for m in range(k + 1, 8):
                cols[m] = cols[m] - weight * line(cols[m])
        left = jnp.where(lane >= base + sub, left * scale, 0.0)
        right = right * scale
        upper[pl.ds(base, 8), :] = left
        inverse[pl.ds(base, 8), :] = right
        panel = jnp.concatenate([left, right], axis=1)
        work[...] = work[...] - tn(left, panel)
        return carry
    lax.fori_loop(0, W // 8, step, 0, unroll=unroll)


def first_factor(g00, upper, inverse, work):
    factor(g00[...], work, upper, inverse)


def middle(g00, cee, g01, g11, inv0, first, full, upper1, comb1, image1, gram_p, g02, work, inv1):
    li0 = inv0[...]
    x0 = li0.T
    u = nt(cee[...], li0)
    side = jnp.concatenate([g00[...], g01[...]], axis=1)
    gram = jnp.concatenate([side, jnp.concatenate([g01[...].T, g11[...]], axis=1)])
    h = nn(li0, nn(side, jnp.concatenate([u, x0])))
    g00x0 = nt(gram[:, :W], li0)
    m00 = nn(li0, g00x0[:W])
    h_full = h + (h - nn(m00, h))
    first[...] = h
    full[...] = h_full
    comb = jnp.concatenate([u - nn(x0, h_full), x0])
    y = nn(gram, comb)
    factor(tn(comb, y), work, upper1, inv1)
    li1 = inv1[...]
    c1 = nt(comb, li1)
    y1 = nt(y, li1)
    comb1[...] = c1
    image1[:W, :] = nn(cee[...], c1[:W])
    image1[W:, :] = c1
    m01 = nn(li0, y1[:W])
    gram_p[:W, :W] = m00
    gram_p[:W, W:] = m01
    gram_p[W:, :W] = m01.T
    gram_p[W:, W:] = tn(c1, y1)
    g02[...] = g11[...] + tn(cee[...], g01[...])


def last(
    scale, g00, g01, g02, g11, g12, g22, inv0, first, full, upper1, comb1, image1, gram_p, mix, projection, first_pass, work, upper2, inv2
):
    li0 = inv0[...]
    c1 = comb1[...]
    i1 = image1[...]
    a01, a02, a12 = g01[...], g02[...], g12[...]
    gram = jnp.concatenate(
        [
            jnp.concatenate([g00[...], a01, a02], axis=1),
            jnp.concatenate([a01.T, g11[...], a12], axis=1),
            jnp.concatenate([a02.T, a12.T, g22[...]], axis=1),
        ]
    )
    s = nn(gram, i1)
    h = jnp.concatenate([nn(li0, s[:W]), tn(c1, s[: 2 * W])])
    h_full = h + (h - nn(gram_p[...], h))
    back = nn(c1, h_full[W:])
    comb = jnp.concatenate([i1[:W] - (back[:W] + tn(li0, h_full[:W])), i1[W : 2 * W] - back[W:], i1[2 * W :]])
    factor(tn(comb, nn(gram, comb)), work, upper2, inv2)
    zero = jnp.zeros((W, W), f32)
    mix[:W, :W] = li0.T * scale
    mix[W:, :W] = jnp.zeros((2 * W, W), f32)
    mix[: 2 * W, W : 2 * W] = c1 * scale
    mix[2 * W :, W : 2 * W] = zero
    mix[:, 2 * W :] = nt(comb, inv2[...]) * scale
    projection[:W, :W] = full[...]
    projection[W : 2 * W, :W] = upper1[...]
    projection[2 * W :, :W] = zero
    projection[: 2 * W, W:] = h_full
    projection[2 * W :, W:] = upper2[...]
    first_pass[:W, :W] = first[...]
    first_pass[W:, :W] = jnp.zeros((2 * W, W), f32)
    first_pass[: 2 * W, W:] = h
    first_pass[2 * W :, W:] = zero


def kernel(body, shapes, scratch, *args):
    return pl.pallas_call(
        body,
        out_shape=[jax.ShapeDtypeStruct(s, f32) for s in shapes],
        scratch_shapes=[pltpu.VMEM(s, f32) for s in scratch],
    )(*args)


def scattered(parts, axis):
    return jnp.sum(lax.all_to_all(parts, axis, 0, 0, tiled=True), axis=0)


def gathered(part, axis):
    copies = jnp.broadcast_to(part, (lax.axis_size(axis), *part.shape))
    return lax.all_to_all(copies, axis, 0, 0, tiled=True)


def other_core(value):
    return lax.ppermute(value, CORE, SWAP)


def turned(rows, chips, cores):
    return [
        ((r * chips + a) * cores + b, (a * chips + r) * cores + b)
        for r in range(rows)
        for a in range(chips)
        for b in range(cores)
    ]


def in_order(mine, theirs, core):
    first = core == 0
    return jnp.concatenate([jnp.where(first, mine, theirs), jnp.where(first, theirs, mine)])


def local(covariance, seed_index):
    height, breadth = covariance.shape
    width = seed_index.shape[0]
    rows, chips, cores = (lax.axis_size(a) for a in ALL)
    row, chip, core = (lax.axis_index(a) for a in ALL)
    order = height * rows
    share = breadth // rows
    half = height // cores
    cut = half // chips
    bit = width // chips
    square = (width, width)
    first = core == 0
    turn = turned(rows, chips, cores)

    def pick(a, b):
        return jnp.where(first, a, b)

    offsets = seed_index - row * height
    inside = (offsets >= 0) & (offsets < height)
    picked = jnp.take(covariance, jnp.clip(offsets, 0, height - 1), axis=0)
    picked = jnp.where(inside[:, None], picked, 0.0)
    start_piece = scattered(picked.reshape(width, rows, share).transpose(1, 0, 2), ROWS).T
    start = gathered(start_piece, ROWS).reshape(breadth, width)
    start_turned = lax.ppermute(start_piece, ALL, turn)
    lines = (chip * cores + core) * breadth + jnp.arange(breadth, dtype=jnp.int32)
    hot = lines[:, None] == seed_index[None, :]
    rest = jnp.where(jnp.any(hot, axis=1)[:, None], 0.0, start)
    g00 = dot(start, start, ((0,), (0,)))
    cee = dot(hot.astype(f32), start, ((0,), (0,)))
    partial = product(covariance, rest)
    keep = jnp.concatenate([pick(partial[:half], partial[half:]), pick(g00, cee)])
    send = jnp.concatenate([pick(partial[half:], partial[:half]), pick(cee, g00)])
    summed = keep + other_core(send)
    parts = jnp.concatenate([summed[:half].reshape(chips, cut, width), summed[half:].reshape(chips, bit, width)], axis=1)
    mine = gathered(jnp.concatenate([scattered(parts, CHIP), start_turned]), CHIP)
    theirs = other_core(mine)
    step_mine, step_theirs = (v[:, :cut].reshape(half, width) for v in (mine, theirs))
    extra_mine, extra_theirs = (v[:, cut : cut + bit].reshape(square) for v in (mine, theirs))
    start_mine, start_theirs = (v[:, cut + bit :].reshape(half, width) for v in (mine, theirs))
    g00 = pick(extra_mine, extra_theirs)
    cee = pick(extra_theirs, extra_mine)
    upper0, inv0 = kernel(first_factor, [square] * 2, [(width, 2 * width)], g00)
    step = in_order(step_mine, step_theirs, core)
    partial = dot_high(covariance, step)
    grams = [product(start_mine.T, step_mine), product(step_mine.T, step_mine)]
    parts = jnp.concatenate([partial.reshape(rows, share, width)] + [g.reshape(rows, bit, width) for g in grams], axis=1)
    piece = lax.ppermute(scattered(parts, ROWS), ALL, turn)
    mine = gathered(piece, CHIP)
    next_mine = mine[:, :share].reshape(half, width)
    g01 = mine[:, share : share + bit].reshape(square)
    g11 = mine[:, share + bit :].reshape(square)
    both = jnp.concatenate([g01, g11])
    g12, g22 = product(step_mine.T, next_mine), product(next_mine.T, next_mine)
    got = other_core(jnp.concatenate([both, pick(g22, g12)]))
    both = both + got[: 2 * width]
    total = pick(g12, g22) + got[2 * width :]
    next_theirs = other_core(next_mine)
    total = jnp.sum(gathered(total, ROWS), axis=0)
    g01, g11 = both[:width], both[width:]
    first_h, full_h, upper1, comb1, image1, gram_p, g02 = kernel(
        middle,
        [square, square, square, (2 * width, width), (3 * width, width), (2 * width, 2 * width), square],
        [(width, 2 * width), square],
        g00,
        cee,
        g01,
        g11,
        inv0,
    )
    rest_total = other_core(total)
    g12, g22 = pick(total, rest_total), pick(rest_total, total)
    scale = float(order) ** 0.5

    def last_step(*refs):
        last(f32(scale), *refs)

    mix, projection, first_pass = kernel(
        last_step,
        [(3 * width, 3 * width), (3 * width, 2 * width), (3 * width, 2 * width)],
        [(width, 2 * width), square, square],
        g00,
        g01,
        g02,
        g11,
        g12,
        g22,
        inv0,
        first_h,
        full_h,
        upper1,
        comb1,
        image1,
        gram_p,
    )
    mine = jnp.concatenate([start_mine, step_mine, next_mine], axis=1)
    theirs = jnp.concatenate([start_theirs, step_theirs, next_theirs], axis=1)
    basis = product(in_order(mine, theirs, core), mix)
    return basis, projection, first_pass


def dot_high(covariance, step):
    return product(covariance.T, step)


def solution(mesh):
    rows, cols = mesh.devices.shape
    fine = Mesh(mesh.devices.reshape(rows, cols // 2, 2), ALL)
    return jax.shard_map(
        local,
        mesh=fine,
        in_specs=(P(ROWS, (CHIP, CORE)), P()),
        out_specs=(P(ROWS, None), P(), P()),
        check_vma=False,
    )
```

```python
import jax
import jax.numpy as jnp
from jax import lax
from jax.experimental import pallas as pl
from jax.experimental.pallas import tpu as pltpu
from jax.sharding import Mesh, PartitionSpec as P

ROWS = "row"
CHIP = "chip"
CORE = "core"
ALL = (ROWS, CHIP, CORE)
SWAP = [(0, 1), (1, 0)]
W = 128
f32 = jnp.float32
bf16 = jnp.bfloat16
HI = lax.Precision.HIGHEST


def dot(a, b, dims):
    return lax.dot_general(a, b, (dims, ((), ())), precision=HI, preferred_element_type=f32)


def nn(a, b):
    return dot(a, b, ((1,), (0,)))


def tn(a, b):
    return dot(a, b, ((0,), (0,)))


def nt(a, b):
    return dot(a, b, ((1,), (1,)))


def pieces(x):
    a = x.astype(bf16)
    rest = x - a.astype(f32)
    b = rest.astype(bf16)
    return a, b, (rest - b.astype(f32)).astype(bf16)


def outer(left, panel):
    a0, a1, a2 = pieces(left)
    b0, b1, b2 = pieces(panel)
    return lax.dot_general(
        jnp.concatenate([a0, a0, a1, a0, a2, a1]),
        jnp.concatenate([b0, b1, b0, b2, b0, b1]),
        (((0,), (0,)), ((), ())),
        preferred_element_type=f32,
    )


BAND = 16


def factor(gram, work, upper, inverse):
    sub = lax.broadcasted_iota(jnp.int32, (BAND, W), 0)
    lane = lax.broadcasted_iota(jnp.int32, (BAND, W), 1)
    work[:, :W] = gram
    work[:, W:] = (
        lax.broadcasted_iota(jnp.int32, (W, W), 0) == lax.broadcasted_iota(jnp.int32, (W, W), 1)
    ).astype(f32)

    def step(j, carry):
        base = pl.multiple_of(j * BAND, BAND)
        left = work[pl.ds(base, BAND), :W]
        right = work[pl.ds(base, BAND), W:]
        turned = pltpu.roll(left, (W - base) % W, 1)
        cols = [jnp.broadcast_to(turned[:, k : k + 1], (BAND, W)) for k in range(BAND)]
        scale = jnp.zeros((BAND, W), f32)
        for k in range(BAND):
            top = k // 8 * 8

            def line(v):
                return jnp.broadcast_to(v[k : k + 1, :], (BAND - top, W))

            def below(old, new):
                return new if top == 0 else jnp.concatenate([old[:top], new])

            root = lax.rsqrt(line(cols[k]))
            weight = jnp.where(sub[top:] > k, cols[k][top:] * (root * root), 0.0)
            scale = below(scale, jnp.where(sub[top:] == k, root, scale[top:]))
            for m in range(k + 1, BAND):
                cols[m] = below(cols[m], cols[m][top:] - weight * line(cols[m]))
            left = below(left, left[top:] - weight * line(left))
            right = below(right, right[top:] - weight * line(right))
        left = jnp.where(lane >= base + sub, left * scale, 0.0)
        right = right * scale
        upper[pl.ds(base, BAND), :] = left
        inverse[pl.ds(base, BAND), :] = right
        work[...] = work[...] - outer(left, jnp.concatenate([left, right], axis=1))
        return carry

    lax.fori_loop(0, W // BAND, step, 0)


def first_factor(g00, upper, inverse, work):
    factor(g00[...], work, upper, inverse)


def middle(g00, cee, g01, g11, inv0, pack, work, upper1, inv1):
    li0 = inv0[...]
    x0 = li0.T
    u = nt(cee[...], li0)
    side = jnp.concatenate([g00[...], g01[...]], axis=1)
    gram = jnp.concatenate([side, jnp.concatenate([g01[...].T, g11[...]], axis=1)])
    h = nn(li0, nn(side, jnp.concatenate([u, x0])))
    g00x0 = nt(gram[:, :W], li0)
    m00 = nn(li0, g00x0[:W])
    h_full = h + (h - nn(m00, h))
    comb = jnp.concatenate([u - nn(x0, h_full), x0])
    y = nn(gram, comb)
    factor(tn(comb, y), work, upper1, inv1)
    li1 = inv1[...]
    c1 = nt(comb, li1)
    y1 = nt(y, li1)
    m01 = nn(li0, y1[:W])
    blocks = (
        [h, h_full, upper1[...], nn(cee[...], c1[:W]), c1[:W], c1[W:]]
        + [m00, m01, m01.T, tn(c1, y1), g11[...] + tn(cee[...], g01[...])]
        + [g00[...], g01[...], g11[...], li0]
    )
    for i, block in enumerate(blocks):
        pack[i * W : (i + 1) * W, :] = block


PACK = 15


def last(scale, pack, g12, g22, mix, projection, first_pass, work, upper2, inv2):
    first, full, upper1, _, c1_top, c1_low, m00, m01, m10, m11, a02, a00, a01, a11, li0 = (
        pack[i * W : (i + 1) * W, :] for i in range(PACK)
    )
    i1 = pack[3 * W : 6 * W, :]
    c1 = i1[W:]
    a12 = g12[...]
    gram = jnp.concatenate(
        [
            jnp.concatenate([a00, a01, a02], axis=1),
            jnp.concatenate([a01.T, a11, a12], axis=1),
            jnp.concatenate([a02.T, a12.T, g22[...]], axis=1),
        ]
    )
    s = nn(gram, i1)
    h = jnp.concatenate([nn(li0, s[:W]), tn(c1, s[: 2 * W])])
    gram_p = jnp.concatenate([jnp.concatenate([m00, m01], axis=1), jnp.concatenate([m10, m11], axis=1)])
    h_full = h + (h - nn(gram_p, h))
    back = nn(c1, h_full[W:])
    comb = jnp.concatenate([i1[:W] - (back[:W] + tn(li0, h_full[:W])), i1[W : 2 * W] - back[W:], i1[2 * W :]])
    factor(tn(comb, nn(gram, comb)), work, upper2, inv2)
    zero = jnp.zeros((W, W), f32)
    mix[:W, :W] = li0.T * scale
    mix[W:, :W] = jnp.zeros((2 * W, W), f32)
    mix[: 2 * W, W : 2 * W] = c1 * scale
    mix[2 * W :, W : 2 * W] = zero
    mix[:, 2 * W :] = nt(comb, inv2[...]) * scale
    projection[:W, :W] = full
    projection[W : 2 * W, :W] = upper1
    projection[2 * W :, :W] = zero
    projection[: 2 * W, W:] = h_full
    projection[2 * W :, W:] = upper2[...]
    first_pass[:W, :W] = first
    first_pass[W:, :W] = jnp.zeros((2 * W, W), f32)
    first_pass[: 2 * W, W:] = h
    first_pass[2 * W :, W:] = zero


HBM = pl.BlockSpec(memory_space=pltpu.HBM)
VMEM = pl.BlockSpec(memory_space=pltpu.VMEM)
SMEM = pl.BlockSpec(memory_space=pltpu.SMEM)


def room(mib):
    return pltpu.CompilerParams(vmem_limit_bytes=mib * 2**20)


def kernel(body, shapes, scratch, *args):
    return pl.pallas_call(
        body,
        out_shape=[jax.ShapeDtypeStruct(s, f32) for s in shapes],
        in_specs=[VMEM] * len(args),
        out_specs=[VMEM] * len(shapes),
        scratch_shapes=[pltpu.VMEM(s, f32) for s in scratch],
        compiler_params=room(16),
    )(*args)


def halves(x):
    high = x.astype(bf16)
    return high, (x - high.astype(f32)).astype(bf16)


def mm(a, b):
    return lax.dot_general(a, b, (((1,), (0,)), ((), ())), preferred_element_type=f32)


def pick_rows(place, seeds, lanes, covariance, out, buffer, sem):
    count = seeds.shape[0]
    height = covariance.shape[0]
    base = place[0] * height

    def body(i, carry):
        line = jnp.clip(seeds[i] - base, 0, height - 1)
        pltpu.make_async_copy(covariance.at[pl.ds(line, 1), :], buffer.at[pl.ds(i, 1), :], sem).start()
        return carry

    lax.fori_loop(0, count, body, 0, unroll=8)
    offsets = jnp.broadcast_to(lanes[...] - base, (count, count))
    held = jnp.where((offsets >= 0) & (offsets < height), 1.0, 0.0).T > 0
    pltpu.make_async_copy(covariance.at[pl.ds(0, count), :], buffer, sem).wait()
    for p in range(out.shape[0]):
        out[p] = jnp.where(held, buffer[:, p * W : (p + 1) * W], 0.0)


def picked_rows(place, seeds, covariance, parts):
    count = seeds.shape[0]
    return pl.pallas_call(
        pick_rows,
        out_shape=jax.ShapeDtypeStruct((parts, count, W), f32),
        in_specs=[SMEM, SMEM, VMEM, HBM],
        out_specs=VMEM,
        scratch_shapes=[pltpu.VMEM((count, covariance.shape[1]), f32), pltpu.SemaphoreType.DMA],
    )(place, seeds, seeds.reshape(1, count), covariance)


CHUNKS = 8


def chunks_of(covariance, buffer, sems):
    tall = covariance.shape[0] // CHUNKS
    return [
        pltpu.make_async_copy(covariance.at[pl.ds(i * tall, tall), :], buffer.at[i], sems.at[i]) for i in range(CHUNKS)
    ]


def chunk_scratch(covariance):
    height, breadth = covariance.shape
    return [pltpu.VMEM((CHUNKS, height // CHUNKS, breadth), f32), pltpu.SemaphoreType.DMA((CHUNKS,))]


def first_product(place, lanes, covariance, start, keep, send, buffer, sems):
    height, breadth = covariance.shape
    half = height // 2
    tall = height // CHUNKS
    copies = chunks_of(covariance, buffer, sems)
    for copy in copies:
        copy.start()
    lines = lax.broadcasted_iota(jnp.int32, (breadth, W), 0) + place[2] * breadth
    hot = jnp.where(lines == lanes[...], 1.0, 0.0)
    hit = jnp.max(hot, axis=1, keepdims=True) > 0
    block = start[...]
    weights = jnp.concatenate(halves(jnp.where(hit, 0.0, block)), axis=1)
    g00 = tn(block, block)
    hot = hot.astype(bf16)
    cee = sum(lax.dot_general(hot, p, (((0,), (0,)), ((), ())), preferred_element_type=f32) for p in pieces(block))
    first = place[1] == 0
    keep[half:, :] = jnp.where(first, g00, cee)
    send[half:, :] = jnp.where(first, cee, g00)
    for i, copy in enumerate(copies):
        copy.wait()
        high, low = halves(buffer[i])
        both = mm(high, weights)
        value = both[:, :W] + both[:, W:] + mm(low, weights[:, :W])
        rows = slice(i * tall % half, i * tall % half + tall)
        mine = first if i * tall < half else jnp.logical_not(first)

        @pl.when(mine)
        def _():
            keep[rows, :] = value

        @pl.when(jnp.logical_not(mine))
        def _():
            send[rows, :] = value


def image_of_start(place, seeds, covariance, start):
    height = covariance.shape[0]
    shape = jax.ShapeDtypeStruct((height // 2 + W, W), f32)
    return pl.pallas_call(
        first_product,
        out_shape=[shape, shape],
        in_specs=[SMEM, VMEM, HBM, VMEM],
        out_specs=[VMEM] * 2,
        scratch_shapes=chunk_scratch(covariance),
    )(place, seeds.reshape(1, W), covariance, start)


def two_grams(a, b, c, out_a, out_b):
    right = halves(c[...])
    for left, out in ((a, out_a), (b, out_b)):
        high, low = halves(left[...].T)
        both = mm(high, jnp.concatenate(right, axis=1))
        out[...] = both[:, :W] + both[:, W:] + mm(low, right[0])


def grams_of(a, b, c):
    return kernel(two_grams, [(W, W)] * 2, [], a, b, c)


def second_product(place, covariance, mine, theirs, g01, g11, out, buffer, sems, total):
    height, breadth = covariance.shape
    half = height // 2
    tall = height // CHUNKS
    copies = chunks_of(covariance, buffer, sems)
    for copy in copies:
        copy.start()
    first = place[1] == 0
    parts = out.shape[0]
    bit = W // parts
    for p in range(parts):
        out[p, W : W + bit, :] = g01[p * bit : (p + 1) * bit, :]
        out[p, W + bit :, :] = g11[p * bit : (p + 1) * bit, :]
    for i, copy in enumerate(copies):
        rows = slice(i * tall % half, i * tall % half + tall)
        own, other = (mine, theirs) if i * tall < half else (theirs, mine)
        v_high, v_low = halves(jnp.where(first, own[rows, :], other[rows, :]).T)
        copy.wait()
        high, low = halves(buffer[i])
        both = mm(jnp.concatenate([v_high, v_low]), high)
        value = both[:W] + both[W:] + mm(v_high, low)
        if i == 0:
            total[...] = value
        elif i + 1 < CHUNKS:
            total[...] += value
        else:
            value += total[...]
            for p in range(parts):
                out[p, :W, :] = value[:, p * W : (p + 1) * W].T


def image_of_step(place, covariance, mine, theirs, g01, g11):
    breadth = covariance.shape[1]
    parts = breadth // W
    return pl.pallas_call(
        second_product,
        out_shape=jax.ShapeDtypeStruct((parts, W + 2 * (W // parts), W), f32),
        in_specs=[SMEM, HBM] + [VMEM] * 4,
        out_specs=VMEM,
        scratch_shapes=chunk_scratch(covariance) + [pltpu.VMEM((W, breadth), f32)],
    )(place, covariance, mine, theirs, g01, g11)


def basis_rows(core, s0, v0, k0, s1, v1, k1, mix, out, high, low):
    step = pl.program_id(0)
    count = pl.num_programs(0) // 2
    tall = out.shape[0]

    @pl.when(step == 0)
    def _():
        high[...], low[...] = halves(mix[...])

    def rows(parts, line):
        left = jnp.concatenate([p[pl.ds(line, tall), :] for p in parts], axis=1)
        l_high, l_low = halves(left)
        out[...] = mm(l_high, high[...]) + mm(l_low, high[...]) + mm(l_high, low[...])

    @pl.when(step < count)
    def _():
        rows((s0, v0, k0), pl.multiple_of(step * tall, tall))

    @pl.when(step >= count)
    def _():
        rows((s1, v1, k1), pl.multiple_of((step - count) * tall, tall))


def basis_of(core, mine, theirs, mix):
    half = mine[0].shape[0]
    count = half // 512
    return pl.pallas_call(
        basis_rows,
        out_shape=jax.ShapeDtypeStruct((2 * half, mix.shape[1]), f32),
        grid_spec=pltpu.PrefetchScalarGridSpec(
            num_scalar_prefetch=1,
            grid=(2 * count,),
            in_specs=[VMEM] * 7,
            out_specs=pl.BlockSpec(
                (512, mix.shape[1]),
                lambda i, c: (jnp.where(i < count, i + c[0] * count, i - count + (1 - c[0]) * count), 0),
            ),
            scratch_shapes=[pltpu.VMEM(mix.shape, bf16)] * 2,
        ),
        compiler_params=room(24),
    )(core, *mine, *theirs, mix)


def scattered(parts, axis):
    return jnp.sum(lax.all_to_all(parts, axis, 0, 0, tiled=True), axis=0)


def gathered(part, axis):
    copies = jnp.broadcast_to(part, (lax.axis_size(axis), *part.shape))
    return lax.all_to_all(copies, axis, 0, 0, tiled=True)


def other_core(value):
    return lax.ppermute(value, CORE, SWAP)


def turned(rows, chips, cores):
    return [
        ((r * chips + a) * cores + b, (a * chips + r) * cores + b)
        for r in range(rows)
        for a in range(chips)
        for b in range(cores)
    ]


def local(covariance, seed_index):
    height, breadth = covariance.shape
    width = seed_index.shape[0]
    rows, chips, cores = (lax.axis_size(a) for a in ALL)
    row, chip, core = (lax.axis_index(a) for a in ALL)
    order = height * rows
    share = breadth // rows
    half = height // cores
    cut = half // chips
    bit = width // chips
    square = (width, width)
    first = core == 0
    turn = turned(rows, chips, cores)

    def pick(a, b):
        return jnp.where(first, a, b)

    place = jnp.stack([row, core, chip * cores + core]).astype(jnp.int32)
    picked = picked_rows(place, seed_index, covariance, rows)
    start_piece = scattered(picked, ROWS).T
    start = gathered(start_piece, ROWS).reshape(breadth, width)
    start_turned = lax.ppermute(start_piece, ALL, turn)
    keep, send = image_of_start(place, seed_index, covariance, start)
    summed = keep + other_core(send)
    parts = jnp.concatenate([summed[:half].reshape(chips, cut, width), summed[half:].reshape(chips, bit, width)], axis=1)
    mine = gathered(jnp.concatenate([scattered(parts, CHIP), start_turned]), CHIP)
    theirs = other_core(mine)
    step_mine, step_theirs = (v[:, :cut].reshape(half, width) for v in (mine, theirs))
    extra_mine, extra_theirs = (v[:, cut : cut + bit].reshape(square) for v in (mine, theirs))
    start_mine, start_theirs = (v[:, cut + bit :].reshape(half, width) for v in (mine, theirs))
    g00 = pick(extra_mine, extra_theirs)
    cee = pick(extra_theirs, extra_mine)
    upper0, inv0 = kernel(first_factor, [square] * 2, [(width, 2 * width)], g00)
    g01, g11 = grams_of(start_mine, step_mine, step_mine)
    parts = image_of_step(place, covariance, step_mine, step_theirs, g01, g11)
    piece = lax.ppermute(scattered(parts, ROWS), ALL, turn)
    mine = gathered(piece, CHIP)
    mine, upper0, inv0 = lax.optimization_barrier((mine, upper0, inv0))
    next_mine = mine[:, :share].reshape(half, width)
    g01 = mine[:, share : share + bit].reshape(square)
    g11 = mine[:, share + bit :].reshape(square)
    both = jnp.concatenate([g01, g11])
    g12, g22 = grams_of(step_mine, next_mine, next_mine)
    got = other_core(jnp.concatenate([both, pick(g22, g12)]))
    both = both + got[: 2 * width]
    total = pick(g12, g22) + got[2 * width :]
    next_theirs = other_core(next_mine)
    totals = gathered(total, ROWS)
    g01, g11 = both[:width], both[width:]
    (pack,) = kernel(
        middle, [(PACK * width, width)], [(width, 2 * width), square, square], g00, cee, g01, g11, inv0
    )
    totals, pack = lax.optimization_barrier((totals, pack))
    total = jnp.sum(totals, axis=0)
    rest_total = other_core(total)
    g12, g22 = pick(total, rest_total), pick(rest_total, total)
    scale = float(order) ** 0.5

    def last_step(*refs):
        last(f32(scale), *refs)

    mix, projection, first_pass = kernel(
        last_step,
        [(3 * width, 3 * width), (3 * width, 2 * width), (3 * width, 2 * width)],
        [(width, 2 * width), square, square],
        pack,
        g12,
        g22,
    )
    basis = basis_of(place[1:2], (start_mine, step_mine, next_mine), (start_theirs, step_theirs, next_theirs), mix)
    return basis, projection, first_pass


def solution(mesh):
    rows, cols = mesh.devices.shape
    fine = Mesh(mesh.devices.reshape(rows, cols // 2, 2), ALL)
    return jax.shard_map(
        local,
        mesh=fine,
        in_specs=(P(ROWS, (CHIP, CORE)), P()),
        out_specs=(P(ROWS, None), P(), P()),
        check_vma=False,
    )
```

```python
import jax
import jax.numpy as jnp
from jax import lax
from jax.experimental import pallas as pl
from jax.experimental.pallas import tpu as pltpu
from jax.sharding import Mesh, PartitionSpec as P

ROWS = "row"
CHIP = "chip"
CORE = "core"
ALL = (ROWS, CHIP, CORE)
SWAP = [(0, 1), (1, 0)]
W = 128
f32 = jnp.float32
bf16 = jnp.bfloat16
HI = lax.Precision.HIGHEST


def dot(a, b, dims):
    return lax.dot_general(a, b, (dims, ((), ())), precision=HI, preferred_element_type=f32)


def nn(a, b):
    return dot(a, b, ((1,), (0,)))


def tn(a, b):
    return dot(a, b, ((0,), (0,)))


def nt(a, b):
    return dot(a, b, ((1,), (1,)))


def pieces(x):
    a = x.astype(bf16)
    rest = x - a.astype(f32)
    b = rest.astype(bf16)
    return a, b, (rest - b.astype(f32)).astype(bf16)


def outer(left, panel):
    a0, a1, a2 = pieces(left)
    b0, b1, b2 = pieces(panel)
    return lax.dot_general(
        jnp.concatenate([a0, a0, a1, a0, a2, a1]),
        jnp.concatenate([b0, b1, b0, b2, b0, b1]),
        (((0,), (0,)), ((), ())),
        preferred_element_type=f32,
    )


BAND = 16


def factor(gram, work, upper, inverse):
    sub = lax.broadcasted_iota(jnp.int32, (BAND, W), 0)
    lane = lax.broadcasted_iota(jnp.int32, (BAND, W), 1)
    work[:, :W] = gram
    work[:, W:] = (
        lax.broadcasted_iota(jnp.int32, (W, W), 0) == lax.broadcasted_iota(jnp.int32, (W, W), 1)
    ).astype(f32)

    def step(j, carry):
        base = pl.multiple_of(j * BAND, BAND)
        left = work[pl.ds(base, BAND), :W]
        right = work[pl.ds(base, BAND), W:]
        turned = pltpu.roll(left, (W - base) % W, 1)
        cols = [jnp.broadcast_to(turned[:, k : k + 1], (BAND, W)) for k in range(BAND)]
        scale = jnp.zeros((BAND, W), f32)
        for k in range(BAND):
            top = k // 8 * 8

            def line(v):
                return jnp.broadcast_to(v[k : k + 1, :], (BAND - top, W))

            def below(old, new):
                return new if top == 0 else jnp.concatenate([old[:top], new])

            root = lax.rsqrt(line(cols[k]))
            weight = jnp.where(sub[top:] > k, cols[k][top:] * (root * root), 0.0)
            scale = below(scale, jnp.where(sub[top:] == k, root, scale[top:]))
            for m in range(k + 1, BAND):
                cols[m] = below(cols[m], cols[m][top:] - weight * line(cols[m]))
            left = below(left, left[top:] - weight * line(left))
            right = below(right, right[top:] - weight * line(right))
        left = jnp.where(lane >= base + sub, left * scale, 0.0)
        right = right * scale
        upper[pl.ds(base, BAND), :] = left
        inverse[pl.ds(base, BAND), :] = right
        work[...] = work[...] - outer(left, jnp.concatenate([left, right], axis=1))
        return carry

    lax.fori_loop(0, W // BAND, step, 0)


def blocks_of(ref, start, count):
    return ref[:, start : start + count, :].reshape(ref.shape[0] * count, W)


def first_factor(place, mine, theirs, out, work, upper, inverse):
    bit = W // mine.shape[0]
    first = place[1] == 0
    own, other = blocks_of(mine, W, bit), blocks_of(theirs, W, bit)
    g00 = jnp.where(first, own, other)
    factor(g00, work, upper, inverse)
    out[:W, :] = g00
    out[W : 2 * W, :] = jnp.where(first, other, own)
    out[2 * W :, :] = inverse[...]


def middle(start, keep, got, pack, work, upper1, inv1):
    g00, cee, li0 = (start[i * W : (i + 1) * W, :] for i in range(3))
    g01, g11 = (keep[i * W : (i + 1) * W, :] + got[i * W : (i + 1) * W, :] for i in range(2))
    x0 = li0.T
    u = nt(cee, li0)
    side = jnp.concatenate([g00, g01], axis=1)
    gram = jnp.concatenate([side, jnp.concatenate([g01.T, g11], axis=1)])
    h = nn(li0, nn(side, jnp.concatenate([u, x0])))
    g00x0 = nt(gram[:, :W], li0)
    m00 = nn(li0, g00x0[:W])
    h_full = h + (h - nn(m00, h))
    comb = jnp.concatenate([u - nn(x0, h_full), x0])
    y = nn(gram, comb)
    factor(tn(comb, y), work, upper1, inv1)
    li1 = inv1[...]
    c1 = nt(comb, li1)
    y1 = nt(y, li1)
    m01 = nn(li0, y1[:W])
    blocks = (
        [h, h_full, upper1[...], nn(cee, c1[:W]), c1[:W], c1[W:]]
        + [m00, m01, m01.T, tn(c1, y1), g11 + tn(cee, g01)]
        + [g00, g01, g11, li0]
    )
    for i, block in enumerate(blocks):
        pack[i * W : (i + 1) * W, :] = block


PACK = 15


def last(scale, pack, g12, g22, mix, projection, first_pass, work, upper2, inv2):
    first, full, upper1, _, c1_top, c1_low, m00, m01, m10, m11, a02, a00, a01, a11, li0 = (
        pack[i * W : (i + 1) * W, :] for i in range(PACK)
    )
    i1 = pack[3 * W : 6 * W, :]
    c1 = i1[W:]
    a12 = g12[...]
    gram = jnp.concatenate(
        [
            jnp.concatenate([a00, a01, a02], axis=1),
            jnp.concatenate([a01.T, a11, a12], axis=1),
            jnp.concatenate([a02.T, a12.T, g22[...]], axis=1),
        ]
    )
    s = nn(gram, i1)
    h = jnp.concatenate([nn(li0, s[:W]), tn(c1, s[: 2 * W])])
    gram_p = jnp.concatenate([jnp.concatenate([m00, m01], axis=1), jnp.concatenate([m10, m11], axis=1)])
    h_full = h + (h - nn(gram_p, h))
    back = nn(c1, h_full[W:])
    comb = jnp.concatenate([i1[:W] - (back[:W] + tn(li0, h_full[:W])), i1[W : 2 * W] - back[W:], i1[2 * W :]])
    factor(tn(comb, nn(gram, comb)), work, upper2, inv2)
    zero = jnp.zeros((W, W), f32)
    mix[:W, :W] = li0.T * scale
    mix[W:, :W] = jnp.zeros((2 * W, W), f32)
    mix[: 2 * W, W : 2 * W] = c1 * scale
    mix[2 * W :, W : 2 * W] = zero
    mix[:, 2 * W :] = nt(comb, inv2[...]) * scale
    projection[:W, :W] = full
    projection[W : 2 * W, :W] = upper1
    projection[2 * W :, :W] = zero
    projection[: 2 * W, W:] = h_full
    projection[2 * W :, W:] = upper2[...]
    first_pass[:W, :W] = first
    first_pass[W:, :W] = jnp.zeros((2 * W, W), f32)
    first_pass[: 2 * W, W:] = h
    first_pass[2 * W :, W:] = zero


HBM = pl.BlockSpec(memory_space=pltpu.HBM)
VMEM = pl.BlockSpec(memory_space=pltpu.VMEM)
SMEM = pl.BlockSpec(memory_space=pltpu.SMEM)


def room(mib):
    return pltpu.CompilerParams(vmem_limit_bytes=mib * 2**20)


def kernel(body, shapes, scratch, *args):
    return pl.pallas_call(
        body,
        out_shape=[jax.ShapeDtypeStruct(s, f32) for s in shapes],
        in_specs=[VMEM if a.dtype == f32 else SMEM for a in args],
        out_specs=[VMEM] * len(shapes),
        scratch_shapes=[pltpu.VMEM(s, f32) for s in scratch],
        compiler_params=room(16),
    )(*args)


def halves(x):
    high = x.astype(bf16)
    return high, (x - high.astype(f32)).astype(bf16)


def mm(a, b):
    return lax.dot_general(a, b, (((1,), (0,)), ((), ())), preferred_element_type=f32)


def pick_rows(place, seeds, lanes, covariance, out, buffer, sem):
    count = seeds.shape[0]
    height = covariance.shape[0]
    base = place[0] * height

    def row(line, i):
        return pltpu.make_async_copy(covariance.at[pl.ds(line, 1), :], buffer.at[pl.ds(i, 1), :], sem)

    def body(i, found):
        line = seeds[i] - base
        here = (line >= 0) & (line < height)

        @pl.when(here)
        def _():
            row(line, i).start()

        return found + here.astype(jnp.int32)

    found = lax.fori_loop(0, count, body, 0, unroll=8)
    offsets = jnp.broadcast_to(lanes[...] - base, (count, count))
    held = jnp.where((offsets >= 0) & (offsets < height), 1.0, 0.0).T > 0

    def done(i, carry):
        row(0, 0).wait()
        return carry

    lax.fori_loop(0, found, done, 0)
    for p in range(out.shape[0]):
        out[p] = jnp.where(held, buffer[:, p * W : (p + 1) * W], 0.0)


def picked_rows(place, seeds, covariance, parts):
    count = seeds.shape[0]
    return pl.pallas_call(
        pick_rows,
        out_shape=jax.ShapeDtypeStruct((parts, count, W), f32),
        in_specs=[SMEM, SMEM, VMEM, HBM],
        out_specs=VMEM,
        scratch_shapes=[pltpu.VMEM((count, covariance.shape[1]), f32), pltpu.SemaphoreType.DMA],
    )(place, seeds, seeds.reshape(1, count), covariance)


CHUNKS = 8


def chunks_of(covariance, buffer, sems):
    tall = covariance.shape[0] // CHUNKS
    return [
        pltpu.make_async_copy(covariance.at[pl.ds(i * tall, tall), :], buffer.at[i], sems.at[i]) for i in range(CHUNKS)
    ]


def chunk_scratch(covariance):
    height, breadth = covariance.shape
    return [pltpu.VMEM((CHUNKS, height // CHUNKS, breadth), f32), pltpu.SemaphoreType.DMA((CHUNKS,))]


def first_product(place, lanes, covariance, start, keep, send, buffer, sems):
    height, breadth = covariance.shape
    half = height // 2
    tall = height // CHUNKS
    copies = chunks_of(covariance, buffer, sems)
    for copy in copies:
        copy.start()
    lines = lax.broadcasted_iota(jnp.int32, (breadth, W), 0) + place[2] * breadth
    hot = jnp.where(lines == lanes[...], 1.0, 0.0)
    hit = jnp.max(hot, axis=1, keepdims=True) > 0
    block = start[...]
    weights = jnp.concatenate(halves(jnp.where(hit, 0.0, block)), axis=1)
    b0, b1, b2 = pieces(block)
    hot_t, high_t, low_t = hot.T.astype(bf16), b0.astype(f32).T.astype(bf16), b1.astype(f32).T.astype(bf16)
    both = mm(jnp.concatenate([hot_t, high_t]), jnp.concatenate([b0, b1], axis=1))
    cee = both[:W, :W] + both[:W, W:] + mm(hot_t, b2)
    g00 = both[W:, :W] + both[W:, W:] + mm(low_t, b0)
    first = place[1] == 0
    parts = keep.shape[0]
    bit = W // parts
    for p in range(parts):
        lines = slice(p * bit, (p + 1) * bit)
        keep[p, W:, :] = jnp.where(first, g00[lines], cee[lines])
        send[p, W:, :] = jnp.where(first, cee[lines], g00[lines])
    for i, copy in enumerate(copies):
        copy.wait()
        high, low = halves(buffer[i])
        both = mm(high, weights)
        value = both[:, :W] + both[:, W:] + mm(low, weights[:, :W])
        mine = first if i * tall < half else jnp.logical_not(first)

        def store(out):
            for q in range(tall // W):
                out[i * tall % half // W + q, :W, :] = value[q * W : (q + 1) * W, :]

        @pl.when(mine)
        def _():
            store(keep)

        @pl.when(jnp.logical_not(mine))
        def _():
            store(send)


def image_of_start(place, seeds, covariance, start):
    height = covariance.shape[0]
    parts = height // 2 // W
    shape = jax.ShapeDtypeStruct((parts, W + W // parts, W), f32)
    return pl.pallas_call(
        first_product,
        out_shape=[shape, shape],
        in_specs=[SMEM, VMEM, HBM, VMEM],
        out_specs=[VMEM] * 2,
        scratch_shapes=chunk_scratch(covariance),
    )(place, seeds.reshape(1, W), covariance, start)


def cross(a, b):
    right = halves(b)
    high, low = halves(a.T)
    both = mm(high, jnp.concatenate(right, axis=1))
    return both[:, :W] + both[:, W:] + mm(low, right[0])


def step_grams(mine, out):
    bit = W // mine.shape[0]
    step, start = blocks_of(mine, 0, W), blocks_of(mine, W + bit, W)
    out[:W, :] = cross(start, step)
    out[W:, :] = cross(step, step)


def next_grams(place, mine, following, keep, send):
    bit = W // mine.shape[0]
    step, then = blocks_of(mine, 0, W), blocks_of(following, 0, W)
    first = place[1] == 0
    g01, g11 = blocks_of(following, W, bit), blocks_of(following, W + bit, bit)
    g12, g22 = cross(step, then), cross(then, then)
    for out in (keep, send):
        out[:W, :] = g01
        out[W : 2 * W, :] = g11
    keep[2 * W :, :] = jnp.where(first, g12, g22)
    send[2 * W :, :] = jnp.where(first, g22, g12)


def second_product(place, covariance, mine, theirs, grams, out, buffer, sems, total):
    height, breadth = covariance.shape
    half = height // 2
    tall = height // CHUNKS
    copies = chunks_of(covariance, buffer, sems)
    for copy in copies:
        copy.start()
    first = place[1] == 0
    parts = out.shape[0]
    bit = W // parts
    for p in range(parts):
        out[p, W : W + bit, :] = grams[p * bit : (p + 1) * bit, :]
        out[p, W + bit :, :] = grams[W + p * bit : W + (p + 1) * bit, :]
    for i, copy in enumerate(copies):
        lines = slice(i * tall % half // W, (i * tall % half + tall) // W)
        own, other = (mine, theirs) if i * tall < half else (theirs, mine)
        block = jnp.where(first, own[lines, :W, :], other[lines, :W, :]).reshape(tall, W)
        v_high, v_low = halves(block.T)
        copy.wait()
        high, low = halves(buffer[i])
        both = mm(jnp.concatenate([v_high, v_low]), high)
        value = both[:W] + both[W:] + mm(v_high, low)
        if i == 0:
            total[...] = value
        elif i + 1 < CHUNKS:
            total[...] += value
        else:
            value += total[...]
            for p in range(parts):
                out[p, :W, :] = value[:, p * W : (p + 1) * W].T


def image_of_step(place, covariance, mine, theirs, grams):
    breadth = covariance.shape[1]
    parts = breadth // W
    return pl.pallas_call(
        second_product,
        out_shape=jax.ShapeDtypeStruct((parts, W + 2 * (W // parts), W), f32),
        in_specs=[SMEM, HBM] + [VMEM] * 3,
        out_specs=VMEM,
        scratch_shapes=chunk_scratch(covariance) + [pltpu.VMEM((W, breadth), f32)],
    )(place, covariance, mine, theirs, grams)


def basis_rows(core, mine, mine_next, theirs, theirs_next, mix, out, wide, tip):
    step = pl.program_id(0)
    count = pl.num_programs(0) // 2
    tall = out.shape[0]
    parts = tall // W
    bit = W // mine.shape[0]

    @pl.when(step == 0)
    def _():
        high, low = halves(mix[: 2 * W, : 2 * W])
        wide[:, : 2 * W] = high
        wide[:, 2 * W :] = low
        high, low = halves(mix[:, 2 * W :])
        tip[:, :W] = high
        tip[:, W:] = low

    def rows(pair, following, part):
        lines = pl.ds(part, parts)
        left = jnp.concatenate(
            [
                pair[lines, W + bit :, :].reshape(tall, W),
                pair[lines, :W, :].reshape(tall, W),
                following[lines, :W, :].reshape(tall, W),
            ],
            axis=1,
        )
        high, low = halves(left)
        h2, l2 = high[:, : 2 * W], low[:, : 2 * W]
        out[:, : 2 * W] = mm(h2, wide[:, : 2 * W]) + mm(h2, wide[:, 2 * W :]) + mm(l2, wide[:, : 2 * W])
        both = mm(high, tip[...])
        out[:, 2 * W :] = both[:, :W] + both[:, W:] + mm(low, tip[:, :W])

    @pl.when(step < count)
    def _():
        rows(mine, mine_next, step * parts)

    @pl.when(step >= count)
    def _():
        rows(theirs, theirs_next, (step - count) * parts)


def basis_of(core, mine, mine_next, theirs, theirs_next, mix):
    half = mine.shape[0] * W
    tall = 512
    count = half // tall
    return pl.pallas_call(
        basis_rows,
        out_shape=jax.ShapeDtypeStruct((2 * half, mix.shape[1]), f32),
        grid_spec=pltpu.PrefetchScalarGridSpec(
            num_scalar_prefetch=1,
            grid=(2 * count,),
            in_specs=[VMEM] * 5,
            out_specs=pl.BlockSpec(
                (tall, mix.shape[1]),
                lambda i, c: (jnp.where(i < count, i + c[0] * count, i - count + (1 - c[0]) * count), 0),
            ),
            scratch_shapes=[pltpu.VMEM((2 * W, 4 * W), bf16), pltpu.VMEM((3 * W, 2 * W), bf16)],
        ),
        compiler_params=room(24),
    )(core, mine, mine_next, theirs, theirs_next, mix)


def scattered(parts, axis):
    return jnp.sum(lax.all_to_all(parts, axis, 0, 0, tiled=True), axis=0)


def gathered(part, axis):
    copies = jnp.broadcast_to(part, (lax.axis_size(axis), *part.shape))
    return lax.all_to_all(copies, axis, 0, 0, tiled=True)


def other_core(value):
    return lax.ppermute(value, CORE, SWAP)


def turned(rows, chips, cores):
    return [
        ((r * chips + a) * cores + b, (a * chips + r) * cores + b)
        for r in range(rows)
        for a in range(chips)
        for b in range(cores)
    ]


def local(covariance, seed_index):
    height, breadth = covariance.shape
    width = seed_index.shape[0]
    rows, chips, cores = (lax.axis_size(a) for a in ALL)
    row, chip, core = (lax.axis_index(a) for a in ALL)
    order = height * rows
    square = (width, width)
    first = core == 0
    turn = turned(rows, chips, cores)
    place = jnp.stack([row, core, chip * cores + core]).astype(jnp.int32)
    start_piece = scattered(picked_rows(place, seed_index, covariance, rows), ROWS).T
    start_turned = lax.ppermute(start_piece, ALL, turn)
    start = gathered(start_piece, ROWS).reshape(breadth, width)
    start, start_turned = lax.optimization_barrier((start, start_turned))
    keep, send = image_of_start(place, seed_index, covariance, start)
    mine = gathered(jnp.concatenate([scattered(keep + other_core(send), CHIP), start_turned]), CHIP)
    theirs = other_core(mine)
    (grams,) = kernel(step_grams, [(2 * width, width)], [], mine)
    parts = image_of_step(place, covariance, mine, theirs, grams)
    piece = lax.ppermute(scattered(parts, ROWS), ALL, turn)
    (zero_pack,) = kernel(
        first_factor, [(3 * width, width)], [(width, 2 * width), square, square], place, mine, theirs
    )
    mine_next, zero_pack = lax.optimization_barrier((gathered(piece, CHIP), zero_pack))
    keep, send = kernel(next_grams, [(3 * width, width)] * 2, [], place, mine, mine_next)
    got = other_core(send)
    theirs_next = other_core(mine_next)
    totals = gathered(keep[2 * width :] + got[2 * width :], ROWS)
    (pack,) = kernel(middle, [(PACK * width, width)], [(width, 2 * width), square, square], zero_pack, keep, got)
    totals, pack = lax.optimization_barrier((totals, pack))
    total = jnp.sum(totals, axis=0)
    rest_total = other_core(total)
    g12, g22 = jnp.where(first, total, rest_total), jnp.where(first, rest_total, total)
    scale = float(order) ** 0.5

    def last_step(*refs):
        last(f32(scale), *refs)

    mix, projection, first_pass = kernel(
        last_step,
        [(3 * width, 3 * width), (3 * width, 2 * width), (3 * width, 2 * width)],
        [(width, 2 * width), square, square],
        pack,
        g12,
        g22,
    )
    basis = basis_of(place[1:2], mine, mine_next, theirs, theirs_next, mix)
    return basis, projection, first_pass


def solution(mesh):
    rows, cols = mesh.devices.shape
    fine = Mesh(mesh.devices.reshape(rows, cols // 2, 2), ALL)
    return jax.shard_map(
        local,
        mesh=fine,
        in_specs=(P(ROWS, (CHIP, CORE)), P()),
        out_specs=(P(ROWS, None), P(), P()),
        check_vma=False,
    )
```

```python
import jax
import jax.numpy as jnp
from jax import lax
from jax.experimental import pallas as pl
from jax.experimental.pallas import tpu as pltpu
from jax.sharding import Mesh, PartitionSpec as P

ROWS = "row"
CHIP = "chip"
CORE = "core"
ALL = (ROWS, CHIP, CORE)
SWAP = [(0, 1), (1, 0)]
SLOTS = (
    (2, 6, 0, 5, 1, 4, 3, 7),
    (7, 1, 4, 3, 5, 2, 6, 0),
    (1, 5, 0, 4, 3, 7, 2, 6),
    (4, 2, 5, 1, 6, 0, 7, 3),
    (5, 0, 7, 1, 6, 2, 4, 3),
    (1, 4, 0, 6, 3, 5, 2, 7),
    (4, 3, 7, 2, 6, 1, 5, 0),
    (2, 4, 3, 6, 0, 7, 1, 5),
)
W = 128
f32 = jnp.float32
bf16 = jnp.bfloat16
HI = lax.Precision.HIGHEST


def dot(a, b, dims):
    return lax.dot_general(a, b, (dims, ((), ())), precision=HI, preferred_element_type=f32)


def nn(a, b):
    return dot(a, b, ((1,), (0,)))


def tn(a, b):
    return dot(a, b, ((0,), (0,)))


def nt(a, b):
    return dot(a, b, ((1,), (1,)))


def pieces(x):
    a = x.astype(bf16)
    rest = x - a.astype(f32)
    b = rest.astype(bf16)
    return a, b, (rest - b.astype(f32)).astype(bf16)


def outer(left, panel):
    a0, a1, a2 = pieces(left)
    b0, b1, b2 = pieces(panel)
    return lax.dot_general(
        jnp.concatenate([a0, a0, a1, a0, a2, a1]),
        jnp.concatenate([b0, b1, b0, b2, b0, b1]),
        (((0,), (0,)), ((), ())),
        preferred_element_type=f32,
    )


BAND = 16


def factor(gram, work, upper, inverse):
    sub = lax.broadcasted_iota(jnp.int32, (BAND, W), 0)
    lane = lax.broadcasted_iota(jnp.int32, (BAND, W), 1)
    work[:, :W] = gram
    work[:, W:] = (
        lax.broadcasted_iota(jnp.int32, (W, W), 0) == lax.broadcasted_iota(jnp.int32, (W, W), 1)
    ).astype(f32)

    def step(j, carry):
        base = pl.multiple_of(j * BAND, BAND)
        left = work[pl.ds(base, BAND), :W]
        right = work[pl.ds(base, BAND), W:]
        turned = pltpu.roll(left, (W - base) % W, 1)
        cols = [jnp.broadcast_to(turned[:, k : k + 1], (BAND, W)) for k in range(BAND)]
        scale = jnp.zeros((BAND, W), f32)
        for k in range(BAND):
            top = k // 8 * 8

            def line(v):
                return jnp.broadcast_to(v[k : k + 1, :], (BAND - top, W))

            def below(old, new):
                return new if top == 0 else jnp.concatenate([old[:top], new])

            root = lax.rsqrt(line(cols[k]))
            weight = jnp.where(sub[top:] > k, cols[k][top:] * (root * root), 0.0)
            scale = below(scale, jnp.where(sub[top:] == k, root, scale[top:]))
            for m in range(k + 1, BAND):
                cols[m] = below(cols[m], cols[m][top:] - weight * line(cols[m]))
            left = below(left, left[top:] - weight * line(left))
            right = below(right, right[top:] - weight * line(right))
        left = jnp.where(lane >= base + sub, left * scale, 0.0)
        right = right * scale
        upper[pl.ds(base, BAND), :] = left
        inverse[pl.ds(base, BAND), :] = right
        work[...] = work[...] - outer(left, jnp.concatenate([left, right], axis=1))
        return carry

    lax.fori_loop(0, W // BAND, step, 0)


def blocks_of(ref, start, count):
    return ref[:, start : start + count, :].reshape(ref.shape[0] * count, W)


def turned_blocks(ref, place, start, count, parts):
    return jnp.concatenate([ref[place[3 + p], start : start + count, :] for p in parts])


def first_factor(g00, inverse, work, upper):
    factor(g00[:W, :], work, upper, inverse)


def middle(start, inv0, keep, got, pack, work, upper1, inv1):
    g00, cee = start[:W, :], start[W:, :]
    li0 = inv0[...]
    g01, g11 = (keep[i * W : (i + 1) * W, :] + got[i * W : (i + 1) * W, :] for i in range(2))
    x0 = li0.T
    u = nt(cee, li0)
    side = jnp.concatenate([g00, g01], axis=1)
    gram = jnp.concatenate([side, jnp.concatenate([g01.T, g11], axis=1)])
    h = nn(li0, nn(side, jnp.concatenate([u, x0])))
    m00 = nn(li0, nt(g00, li0))
    h_full = h + (h - nn(m00, h))
    comb = jnp.concatenate([u - nn(x0, h_full), x0])
    y = nn(gram, comb)
    factor(tn(comb, y), work, upper1, inv1)
    li1 = inv1[...]
    c1 = nt(comb, li1)
    y1 = nt(y, li1)
    m01 = nn(li0, y1[:W])
    g02 = g11 + tn(cee, g01)
    i1 = jnp.concatenate([nn(cee, c1[:W]), c1])
    s0 = nn(jnp.concatenate([side, g02], axis=1), i1)
    s1 = nn(gram[W:], i1[: 2 * W])
    blocks = (
        [h, h_full, upper1[...], i1[:W], i1[W : 2 * W], i1[2 * W :]]
        + [m00, m01, tn(c1, y1), g02, g00, g01, g11, li0]
        + [nn(li0, s0), tn(c1[:W], s0), s1]
    )
    for i, block in enumerate(blocks):
        pack[i * W : (i + 1) * W, :] = block


PACK = 17


def last(scale, pack, g12, g22, mix, projection, first_pass, work, upper2, inv2):
    first, full, upper1, _, c1_top, c1_low, m00, m01, m11, a02, a00, a01, a11, li0, first0, part1, s1 = (
        pack[i * W : (i + 1) * W, :] for i in range(PACK)
    )
    i1 = pack[3 * W : 6 * W, :]
    c1 = i1[W:]
    a12 = g12[...]
    gram = jnp.concatenate(
        [
            jnp.concatenate([a00, a01, a02], axis=1),
            jnp.concatenate([a01.T, a11, a12], axis=1),
            jnp.concatenate([a02.T, a12.T, g22[...]], axis=1),
        ]
    )
    h = jnp.concatenate([first0, part1 + tn(c1_low, s1 + nn(a12, c1_low))])
    gram_p = jnp.concatenate([jnp.concatenate([m00, m01], axis=1), jnp.concatenate([m01.T, m11], axis=1)])
    h_full = h + (h - nn(gram_p, h))
    zero = jnp.zeros((W, W), f32)
    places = jnp.concatenate([jnp.concatenate([li0.T, zero]), c1], axis=1)
    comb = jnp.concatenate([i1[: 2 * W] - nn(places, h_full), i1[2 * W :]])
    factor(tn(comb, nn(gram, comb)), work, upper2, inv2)
    mix[: 2 * W, : 2 * W] = places * scale
    mix[2 * W :, : 2 * W] = jnp.zeros((W, 2 * W), f32)
    mix[:, 2 * W :] = nt(comb, inv2[...]) * scale
    projection[:W, :W] = full
    projection[W : 2 * W, :W] = upper1
    projection[2 * W :, :W] = zero
    projection[: 2 * W, W:] = h_full
    projection[2 * W :, W:] = upper2[...]
    first_pass[:W, :W] = first
    first_pass[W:, :W] = jnp.zeros((2 * W, W), f32)
    first_pass[: 2 * W, W:] = h
    first_pass[2 * W :, W:] = zero


HBM = pl.BlockSpec(memory_space=pltpu.HBM)
VMEM = pl.BlockSpec(memory_space=pltpu.VMEM)
SMEM = pl.BlockSpec(memory_space=pltpu.SMEM)


def room(mib):
    return pltpu.CompilerParams(vmem_limit_bytes=mib * 2**20)


def kernel(body, shapes, scratch, *args):
    return pl.pallas_call(
        body,
        out_shape=[jax.ShapeDtypeStruct(s, f32) for s in shapes],
        in_specs=[VMEM if a.dtype == f32 else SMEM for a in args],
        out_specs=[VMEM] * len(shapes),
        scratch_shapes=[pltpu.VMEM(s, f32) for s in scratch],
        compiler_params=room(16),
    )(*args)


def halves(x):
    high = x.astype(bf16)
    return high, (x - high.astype(f32)).astype(bf16)


def mm(a, b):
    return lax.dot_general(a, b, (((1,), (0,)), ((), ())), preferred_element_type=f32)


def pick_rows(place, seeds, lanes, covariance, out, buffer, sem):
    count = seeds.shape[0]
    height = covariance.shape[0]
    base = place[0] * height

    def row(line, i):
        return pltpu.make_async_copy(covariance.at[pl.ds(line, 1), :], buffer.at[pl.ds(i, 1), :], sem)

    def body(i, found):
        line = seeds[i] - base
        here = (line >= 0) & (line < height)

        @pl.when(here)
        def _():
            row(line, i).start()

        return found + here.astype(jnp.int32)

    found = lax.fori_loop(0, count, body, 0, unroll=8)
    offsets = jnp.broadcast_to(lanes[...] - base, (count, count))
    held = jnp.where((offsets >= 0) & (offsets < height), 1.0, 0.0).T > 0

    def done(i, carry):
        row(0, 0).wait()
        return carry

    lax.fori_loop(0, found, done, 0)
    for p in range(out.shape[0]):
        out[p] = jnp.where(held, buffer[:, p * W : (p + 1) * W], 0.0)


def picked_rows(place, seeds, covariance, parts):
    count = seeds.shape[0]
    return pl.pallas_call(
        pick_rows,
        out_shape=jax.ShapeDtypeStruct((parts, count, W), f32),
        in_specs=[SMEM, SMEM, VMEM, HBM],
        out_specs=VMEM,
        scratch_shapes=[pltpu.VMEM((count, covariance.shape[1]), f32), pltpu.SemaphoreType.DMA],
    )(place, seeds, seeds.reshape(1, count), covariance)


CHUNKS = 8


def chunks_of(covariance, buffer, sems):
    tall = covariance.shape[0] // CHUNKS
    return [
        pltpu.make_async_copy(covariance.at[pl.ds(i * tall, tall), :], buffer.at[i], sems.at[i]) for i in range(CHUNKS)
    ]


def chunk_scratch(covariance):
    height, breadth = covariance.shape
    return [pltpu.VMEM((CHUNKS, height // CHUNKS, breadth), f32), pltpu.SemaphoreType.DMA((CHUNKS,))]


def first_product(place, lanes, covariance, start, keep, send, buffer, sems):
    height, breadth = covariance.shape
    half = height // 2
    tall = height // CHUNKS
    copies = chunks_of(covariance, buffer, sems)
    for copy in copies:
        copy.start()
    lines = lax.broadcasted_iota(jnp.int32, (breadth, W), 0) + place[2] * breadth
    hot = jnp.where(lines == lanes[...], 1.0, 0.0)
    hit = jnp.max(hot, axis=1, keepdims=True) > 0
    weights = jnp.concatenate(halves(jnp.where(hit, 0.0, start[...])), axis=1)
    first = place[1] == 0
    for i, copy in enumerate(copies):
        copy.wait()
        high, low = halves(buffer[i])
        both = mm(high, weights)
        value = both[:, :W] + both[:, W:] + mm(low, weights[:, :W])
        mine = first if i * tall < half else jnp.logical_not(first)

        def store(out):
            for q in range(tall // W):
                out[i * tall % half // W + q] = value[q * W : (q + 1) * W, :]

        @pl.when(mine)
        def _():
            store(keep)

        @pl.when(jnp.logical_not(mine))
        def _():
            store(send)


def image_of_start(place, seeds, covariance, start):
    height = covariance.shape[0]
    shape = jax.ShapeDtypeStruct((height // 2 // W, W, W), f32)
    return pl.pallas_call(
        first_product,
        out_shape=[shape, shape],
        in_specs=[SMEM, VMEM, HBM, VMEM],
        out_specs=[VMEM] * 2,
        scratch_shapes=chunk_scratch(covariance),
        compiler_params=room(50),
    )(place, seeds.reshape(1, W), covariance, start)


def start_grams(place, lanes, start, out):
    block = start[...]
    lines = lax.broadcasted_iota(jnp.int32, block.shape, 0) + place[2] * block.shape[0]
    hot_t = jnp.where(lines == lanes[...], 1.0, 0.0).T.astype(bf16)
    b0, b1, b2 = pieces(block)
    turned_block = block.T
    high_t, low_t = halves(turned_block)
    both = mm(jnp.concatenate([hot_t, high_t]), jnp.concatenate([b0, b1], axis=1))
    cee = both[:W, :W] + both[:W, W:] + mm(hot_t, b2)
    g00 = both[W:, :W] + both[W:, W:] + mm(low_t, b0)
    parts = out.shape[0]
    bit = W // parts
    for p in range(parts):
        lines = slice(p * bit, (p + 1) * bit)
        out[p, :bit, :] = g00[lines]
        out[p, bit:, :] = cee[lines]


def grams_of_start(place, seeds, start, parts):
    return pl.pallas_call(
        start_grams,
        out_shape=jax.ShapeDtypeStruct((parts, 2 * W // parts, W), f32),
        in_specs=[SMEM, VMEM, VMEM],
        out_specs=VMEM,
        compiler_params=room(16),
    )(place, seeds.reshape(1, W), start)


def cross(a, b):
    right = halves(b)
    high, low = halves(a.T)
    both = mm(high, jnp.concatenate(right, axis=1))
    return both[:, :W] + both[:, W:] + mm(low, right[0])


def step_grams(place, mine, out):
    parts = mine.shape[0]
    step, start = blocks_of(mine, 0, W), turned_blocks(mine, place, W + 2 * W // parts, W, range(parts))
    out[:W, :] = cross(start, step)
    out[W:, :] = cross(step, step)


def next_grams(place, mine, following, keep, send):
    parts = mine.shape[0]
    bit = W // parts
    step = blocks_of(mine, 0, W)
    then, g01, g11 = (
        turned_blocks(following, place, s, n, range(parts)) for s, n in ((0, W), (W, bit), (W + bit, bit))
    )
    first = place[1] == 0
    g12, g22 = cross(step, then), cross(then, then)
    for out in (keep, send):
        out[:W, :] = g01
        out[W : 2 * W, :] = g11
    keep[2 * W :, :] = jnp.where(first, g12, g22)
    send[2 * W :, :] = jnp.where(first, g22, g12)


def second_product(place, covariance, mine, theirs, grams, out, small, buffer, sems, total):
    height, breadth = covariance.shape
    half = height // 2
    tall = height // CHUNKS
    copies = chunks_of(covariance, buffer, sems)
    for copy in copies:
        copy.start()
    first = place[1] == 0
    parts = out.shape[0]
    bit = W // parts
    for p in range(parts):
        out[p, W : W + bit, :] = grams[p * bit : (p + 1) * bit, :]
        out[p, W + bit :, :] = grams[W + p * bit : W + (p + 1) * bit, :]
    for i in range(2):
        lines = W + i * bit
        small[i * W : (i + 1) * W, :] = blocks_of(mine, lines, bit) + blocks_of(theirs, lines, bit)
    for i, copy in enumerate(copies):
        lines = slice(i * tall % half // W, (i * tall % half + tall) // W)
        own, other = (mine, theirs) if i * tall < half else (theirs, mine)
        block = jnp.where(first, own[lines, :W, :], other[lines, :W, :]).reshape(tall, W)
        v_high, v_low = halves(block.T)
        copy.wait()
        high, low = halves(buffer[i])
        both = mm(jnp.concatenate([v_high, v_low]), high)
        value = both[:W] + both[W:] + mm(v_high, low)
        if i == 0:
            total[...] = value
        elif i + 1 < CHUNKS:
            total[...] += value
        else:
            value += total[...]
            for p in range(parts):
                out[p, :W, :] = value[:, p * W : (p + 1) * W].T


def image_of_step(place, covariance, mine, theirs, grams):
    breadth = covariance.shape[1]
    parts = breadth // W
    return pl.pallas_call(
        second_product,
        out_shape=[
            jax.ShapeDtypeStruct((parts, W + 2 * (W // parts), W), f32),
            jax.ShapeDtypeStruct((2 * W, W), f32),
        ],
        in_specs=[SMEM, HBM] + [VMEM] * 3,
        out_specs=[VMEM] * 2,
        scratch_shapes=chunk_scratch(covariance) + [pltpu.VMEM((W, breadth), f32)],
        compiler_params=room(50),
    )(place, covariance, mine, theirs, grams)


def basis_rows(place, mine, mine_next, theirs, theirs_next, mix, out, wide, tip):
    step = pl.program_id(0)
    count = pl.num_programs(0) // 2
    tall = out.shape[0]
    parts = tall // W
    bit = 2 * W // mine.shape[0]

    @pl.when(step == 0)
    def _():
        high, low = halves(mix[: 2 * W, : 2 * W])
        wide[:, : 2 * W] = high
        wide[:, 2 * W :] = low
        high, low = halves(mix[:, 2 * W :])
        tip[:, :W] = high
        tip[:, W:] = low

    def rows(pair, following, part):
        order = [part + p for p in range(parts)]
        left = jnp.concatenate(
            [
                turned_blocks(pair, place, W + bit, W, order),
                pair[pl.ds(part, parts), :W, :].reshape(tall, W),
                turned_blocks(following, place, 0, W, order),
            ],
            axis=1,
        )
        high, low = halves(left)
        h2, l2 = high[:, : 2 * W], low[:, : 2 * W]
        out[:, : 2 * W] = mm(h2, wide[:, : 2 * W]) + mm(h2, wide[:, 2 * W :]) + mm(l2, wide[:, : 2 * W])
        both = mm(high, tip[...])
        out[:, 2 * W :] = both[:, :W] + both[:, W:] + mm(low, tip[:, :W])

    @pl.when(step < count)
    def _():
        rows(mine, mine_next, step * parts)

    @pl.when(step >= count)
    def _():
        rows(theirs, theirs_next, (step - count) * parts)


def basis_of(place, mine, mine_next, theirs, theirs_next, mix):
    half = mine.shape[0] * W
    tall = 512
    count = half // tall
    return pl.pallas_call(
        basis_rows,
        out_shape=jax.ShapeDtypeStruct((2 * half, mix.shape[1]), f32),
        grid_spec=pltpu.PrefetchScalarGridSpec(
            num_scalar_prefetch=1,
            grid=(2 * count,),
            in_specs=[VMEM] * 5,
            out_specs=pl.BlockSpec(
                (tall, mix.shape[1]),
                lambda i, c: (jnp.where(i < count, i + c[1] * count, i - count + (1 - c[1]) * count), 0),
            ),
            scratch_shapes=[pltpu.VMEM((2 * W, 4 * W), bf16), pltpu.VMEM((3 * W, 2 * W), bf16)],
        ),
        compiler_params=room(24),
    )(place, mine, mine_next, theirs, theirs_next, mix)


def scattered(parts, axis):
    return jnp.sum(lax.all_to_all(parts, axis, 0, 0, tiled=True), axis=0)


def gathered(part, axis):
    copies = jnp.broadcast_to(part, (lax.axis_size(axis), *part.shape))
    return lax.all_to_all(copies, axis, 0, 0, tiled=True)


def other_core(value):
    return lax.ppermute(value, CORE, SWAP)


def turned(rows, chips, cores):
    return [
        ((r * chips + a) * cores + b, (a * chips + SLOTS[a][r]) * cores + b)
        for r in range(rows)
        for a in range(chips)
        for b in range(cores)
    ]


def local(covariance, seed_index):
    height, breadth = covariance.shape
    width = seed_index.shape[0]
    rows, chips, cores = (lax.axis_size(a) for a in ALL)
    row, chip, core = (lax.axis_index(a) for a in ALL)
    order = height * rows
    square = (width, width)
    first = core == 0
    turn = turned(rows, chips, cores)
    slots = lax.dynamic_index_in_dim(jnp.array(SLOTS, jnp.int32), row, 0, keepdims=False)
    place = jnp.concatenate([jnp.stack([row, core, chip * cores + core]).astype(jnp.int32), slots])
    start_piece = scattered(picked_rows(place, seed_index, covariance, rows), ROWS).T
    start_turned = lax.ppermute(start_piece, ALL, turn)
    start = gathered(start_piece, ROWS).reshape(breadth, width)
    start, start_turned = lax.optimization_barrier((start, start_turned))
    keep, send = image_of_start(place, seed_index, covariance, start)
    got = other_core(send)
    small = grams_of_start(place, seed_index, start, chips)
    parts = jnp.concatenate([keep + got, small], axis=1)
    mine = gathered(jnp.concatenate([scattered(parts, CHIP), start_turned]), CHIP)
    theirs = other_core(mine)
    (grams,) = kernel(step_grams, [(2 * width, width)], [], place, mine)
    parts, zero_grams = image_of_step(place, covariance, mine, theirs, grams)
    piece = lax.ppermute(scattered(parts, ROWS), ALL, turn)
    (inv0,) = kernel(first_factor, [square], [(width, 2 * width), square], zero_grams)
    mine_next, inv0 = lax.optimization_barrier((gathered(piece, CHIP), inv0))
    keep, send = kernel(next_grams, [(3 * width, width)] * 2, [], place, mine, mine_next)
    got = other_core(send)
    theirs_next = other_core(mine_next)
    totals = gathered(keep[2 * width :] + got[2 * width :], ROWS)
    (pack,) = kernel(
        middle, [(PACK * width, width)], [(width, 2 * width), square, square], zero_grams, inv0, keep, got
    )
    totals, pack = lax.optimization_barrier((totals, pack))
    total = jnp.sum(totals, axis=0)
    rest_total = other_core(total)
    g12, g22 = jnp.where(first, total, rest_total), jnp.where(first, rest_total, total)
    scale = float(order) ** 0.5

    def last_step(*refs):
        last(f32(scale), *refs)

    mix, projection, first_pass = kernel(
        last_step,
        [(3 * width, 3 * width), (3 * width, 2 * width), (3 * width, 2 * width)],
        [(width, 2 * width), square, square],
        pack,
        g12,
        g22,
    )
    basis = basis_of(place, mine, mine_next, theirs, theirs_next, mix)
    return basis, projection, first_pass


def solution(mesh):
    rows, cols = mesh.devices.shape
    fine = Mesh(mesh.devices.reshape(rows, cols // 2, 2), ALL)
    return jax.shard_map(
        local,
        mesh=fine,
        in_specs=(P(ROWS, (CHIP, CORE)), P()),
        out_specs=(P(ROWS, None), P(), P()),
        check_vma=False,
    )
```

```python
import jax
import jax.numpy as jnp
from jax import lax
from jax.experimental import pallas as pl
from jax.experimental.pallas import tpu as pltpu
from jax.sharding import Mesh, PartitionSpec as P

ROWS = "row"
CHIP = "chip"
CORE = "core"
ALL = (ROWS, CHIP, CORE)
SWAP = [(0, 1), (1, 0)]
SLOTS = (
    (2, 6, 0, 5, 1, 4, 3, 7),
    (7, 1, 4, 3, 5, 2, 6, 0),
    (1, 5, 0, 4, 3, 7, 2, 6),
    (4, 2, 5, 1, 6, 0, 7, 3),
    (5, 0, 7, 1, 6, 2, 4, 3),
    (1, 4, 0, 6, 3, 5, 2, 7),
    (4, 3, 7, 2, 6, 1, 5, 0),
    (2, 4, 3, 6, 0, 7, 1, 5),
)
W = 128
f32 = jnp.float32
bf16 = jnp.bfloat16
HI = lax.Precision.HIGHEST


def dot(a, b, dims):
    return lax.dot_general(a, b, (dims, ((), ())), precision=HI, preferred_element_type=f32)


def nn(a, b):
    return dot(a, b, ((1,), (0,)))


def tn(a, b):
    return dot(a, b, ((0,), (0,)))


def nt(a, b):
    return dot(a, b, ((1,), (1,)))


def pieces(x):
    a = x.astype(bf16)
    rest = x - a.astype(f32)
    b = rest.astype(bf16)
    return a, b, (rest - b.astype(f32)).astype(bf16)


def outer(left, panel):
    a0, a1, a2 = pieces(left)
    b0, b1, b2 = pieces(panel)
    return lax.dot_general(
        jnp.concatenate([a0, a0, a1, a0, a2, a1]),
        jnp.concatenate([b0, b1, b0, b2, b0, b1]),
        (((0,), (0,)), ((), ())),
        preferred_element_type=f32,
    )


BAND = 16


def factor(gram, work, upper, inverse):
    sub = lax.broadcasted_iota(jnp.int32, (BAND, W), 0)
    lane = lax.broadcasted_iota(jnp.int32, (BAND, W), 1)
    work[:, :W] = gram
    work[:, W:] = (
        lax.broadcasted_iota(jnp.int32, (W, W), 0) == lax.broadcasted_iota(jnp.int32, (W, W), 1)
    ).astype(f32)

    def step(j, carry):
        base = pl.multiple_of(j * BAND, BAND)
        left = work[pl.ds(base, BAND), :W]
        right = work[pl.ds(base, BAND), W:]
        turned = pltpu.roll(left, (W - base) % W, 1)
        cols = [jnp.broadcast_to(turned[:, k : k + 1], (BAND, W)) for k in range(BAND)]
        scale = jnp.zeros((BAND, W), f32)
        for k in range(BAND):
            top = k // 8 * 8

            def line(v):
                return jnp.broadcast_to(v[k : k + 1, :], (BAND - top, W))

            def below(old, new):
                return new if top == 0 else jnp.concatenate([old[:top], new])

            root = lax.rsqrt(line(cols[k]))
            weight = jnp.where(sub[top:] > k, cols[k][top:] * (root * root), 0.0)
            scale = below(scale, jnp.where(sub[top:] == k, root, scale[top:]))
            for m in range(k + 1, BAND):
                cols[m] = below(cols[m], cols[m][top:] - weight * line(cols[m]))
            left = below(left, left[top:] - weight * line(left))
            right = below(right, right[top:] - weight * line(right))
        left = jnp.where(lane >= base + sub, left * scale, 0.0)
        right = right * scale
        upper[pl.ds(base, BAND), :] = left
        inverse[pl.ds(base, BAND), :] = right
        work[...] = work[...] - outer(left, jnp.concatenate([left, right], axis=1))
        return carry

    lax.fori_loop(0, W // BAND, step, 0)


def blocks_of(ref, start, count):
    return ref[:, start : start + count, :].reshape(ref.shape[0] * count, W)


def turned_blocks(ref, place, start, count, parts):
    return jnp.concatenate([ref[place[3 + place[0] * ref.shape[0] + p], start : start + count, :] for p in parts])


def first_factor(g00, inverse, work, upper):
    factor(g00[:W, :], work, upper, inverse)


def middle(start, inv0, keep, got, pack, work, upper1, inv1):
    g00, cee = start[:W, :], start[W:, :]
    li0 = inv0[...]
    g01, g11 = (keep[i * W : (i + 1) * W, :] + got[i * W : (i + 1) * W, :] for i in range(2))
    x0 = li0.T
    u = nt(cee, li0)
    side = jnp.concatenate([g00, g01], axis=1)
    gram = jnp.concatenate([side, jnp.concatenate([g01.T, g11], axis=1)])
    h = nn(li0, nn(side, jnp.concatenate([u, x0])))
    m00 = nn(li0, nt(g00, li0))
    h_full = h + (h - nn(m00, h))
    comb = jnp.concatenate([u - nn(x0, h_full), x0])
    y = nn(gram, comb)
    factor(tn(comb, y), work, upper1, inv1)
    li1 = inv1[...]
    c1 = nt(comb, li1)
    y1 = nt(y, li1)
    m01 = nn(li0, y1[:W])
    g02 = g11 + tn(cee, g01)
    i1 = jnp.concatenate([nn(cee, c1[:W]), c1])
    s0 = nn(jnp.concatenate([side, g02], axis=1), i1)
    s1 = nn(gram[W:], i1[: 2 * W])
    blocks = (
        [h, h_full, upper1[...], i1[:W], i1[W : 2 * W], i1[2 * W :]]
        + [m00, m01, tn(c1, y1), g02, g00, g01, g11, li0]
        + [nn(li0, s0), tn(c1[:W], s0), s1]
    )
    for i, block in enumerate(blocks):
        pack[i * W : (i + 1) * W, :] = block


PACK = 17


def last(scale, pack, totals, mix, projection, first_pass, work, upper2, inv2):
    first, full, upper1, _, _, c1_low, m00, m01, m11, a02, a00, a01, a11, li0, first0, part1, s1 = (
        pack[i * W : (i + 1) * W, :] for i in range(PACK)
    )
    i1 = pack[3 * W : 6 * W, :]
    c1 = i1[W:]
    a12, a22 = unpacked(totals[...])
    gram = jnp.concatenate(
        [
            jnp.concatenate([a00, a01, a02], axis=1),
            jnp.concatenate([a01.T, a11, a12], axis=1),
            jnp.concatenate([a02.T, a12, a22], axis=1),
        ]
    )
    h = jnp.concatenate([first0, part1 + tn(c1_low, s1 + nn(a12, c1_low))])
    gram_p = jnp.concatenate([jnp.concatenate([m00, m01], axis=1), jnp.concatenate([m01.T, m11], axis=1)])
    h_full = h + (h - nn(gram_p, h))
    zero = jnp.zeros((W, W), f32)
    places = jnp.concatenate([jnp.concatenate([li0.T, zero]), c1], axis=1)
    comb = jnp.concatenate([i1[: 2 * W] - nn(places, h_full), i1[2 * W :]])
    factor(tn(comb, nn(gram, comb)), work, upper2, inv2)
    mix[: 2 * W, : 2 * W] = places * scale
    mix[2 * W :, : 2 * W] = jnp.zeros((W, 2 * W), f32)
    mix[:, 2 * W :] = nt(comb, inv2[...]) * scale
    projection[:W, :W] = full
    projection[W : 2 * W, :W] = upper1
    projection[2 * W :, :W] = zero
    projection[: 2 * W, W:] = h_full
    projection[2 * W :, W:] = upper2[...]
    first_pass[:W, :W] = first
    first_pass[W:, :W] = jnp.zeros((2 * W, W), f32)
    first_pass[: 2 * W, W:] = h
    first_pass[2 * W :, W:] = zero


HBM = pl.BlockSpec(memory_space=pltpu.HBM)
VMEM = pl.BlockSpec(memory_space=pltpu.VMEM)
SMEM = pl.BlockSpec(memory_space=pltpu.SMEM)


def room(mib):
    return pltpu.CompilerParams(vmem_limit_bytes=mib * 2**20)


def kernel(body, shapes, scratch, *args):
    return pl.pallas_call(
        body,
        out_shape=[jax.ShapeDtypeStruct(s, f32) for s in shapes],
        in_specs=[VMEM if a.dtype == f32 else SMEM for a in args],
        out_specs=[VMEM] * len(shapes),
        scratch_shapes=[pltpu.VMEM(s, f32) for s in scratch],
        compiler_params=room(16),
    )(*args)


def halves(x):
    high = x.astype(bf16)
    return high, (x - high.astype(f32)).astype(bf16)


def mm(a, b):
    return lax.dot_general(a, b, (((1,), (0,)), ((), ())), preferred_element_type=f32)


def pick_rows(place, seeds, lanes, covariance, out, buffer, sem):
    count = seeds.shape[0]
    height = covariance.shape[0]
    base = place[0] * height

    def row(line, i):
        return pltpu.make_async_copy(covariance.at[pl.ds(line, 1), :], buffer.at[pl.ds(i, 1), :], sem)

    def body(i, found):
        line = seeds[i] - base
        here = (line >= 0) & (line < height)

        @pl.when(here)
        def _():
            row(line, i).start()

        return found + here.astype(jnp.int32)

    found = lax.fori_loop(0, count, body, 0, unroll=8)
    offsets = jnp.broadcast_to(lanes[...] - base, (count, count))
    held = jnp.where((offsets >= 0) & (offsets < height), 1.0, 0.0).T > 0

    def done(i, carry):
        row(0, 0).wait()
        return carry

    lax.fori_loop(0, found, done, 0)
    for p in range(out.shape[0]):
        out[p] = jnp.where(held, buffer[:, p * W : (p + 1) * W], 0.0)


def picked_rows(place, seeds, covariance, parts):
    count = seeds.shape[0]
    return pl.pallas_call(
        pick_rows,
        out_shape=jax.ShapeDtypeStruct((parts, count, W), f32),
        in_specs=[SMEM, SMEM, VMEM, HBM],
        out_specs=VMEM,
        scratch_shapes=[pltpu.VMEM((count, covariance.shape[1]), f32), pltpu.SemaphoreType.DMA],
    )(place, seeds, seeds.reshape(1, count), covariance)


CHUNKS = 8


def chunks_of(covariance, buffer, sems):
    tall = covariance.shape[0] // CHUNKS
    return [
        pltpu.make_async_copy(covariance.at[pl.ds(i * tall, tall), :], buffer.at[i], sems.at[i]) for i in range(CHUNKS)
    ]


def chunk_scratch(covariance):
    height, breadth = covariance.shape
    return [pltpu.VMEM((CHUNKS, height // CHUNKS, breadth), f32), pltpu.SemaphoreType.DMA((CHUNKS,))]


def first_product(place, lanes, covariance, start, keep, send, buffer, sems):
    height, breadth = covariance.shape
    half = height // 2
    tall = height // CHUNKS
    copies = chunks_of(covariance, buffer, sems)
    for copy in copies:
        copy.start()
    lines = lax.broadcasted_iota(jnp.int32, (breadth, W), 0) + place[2] * breadth
    hot = jnp.where(lines == lanes[...], 1.0, 0.0)
    hit = jnp.max(hot, axis=1, keepdims=True) > 0
    weights = jnp.concatenate(halves(jnp.where(hit, 0.0, start[...])), axis=1)
    first = place[1] == 0
    for i, copy in enumerate(copies):
        copy.wait()
        high, low = halves(buffer[i])
        both = mm(high, weights)
        value = both[:, :W] + both[:, W:] + mm(low, weights[:, :W])
        mine = first if i * tall < half else jnp.logical_not(first)

        def store(out):
            for q in range(tall // W):
                out[i * tall % half // W + q] = value[q * W : (q + 1) * W, :]

        @pl.when(mine)
        def _():
            store(keep)

        @pl.when(jnp.logical_not(mine))
        def _():
            store(send)


def image_of_start(place, seeds, covariance, start):
    height = covariance.shape[0]
    shape = jax.ShapeDtypeStruct((height // 2 // W, W, W), f32)
    return pl.pallas_call(
        first_product,
        out_shape=[shape, shape],
        in_specs=[SMEM, VMEM, HBM, VMEM],
        out_specs=[VMEM] * 2,
        scratch_shapes=chunk_scratch(covariance),
        compiler_params=room(50),
    )(place, seeds.reshape(1, W), covariance, start)


def start_grams(place, lanes, start, out):
    block = start[...]
    lines = lax.broadcasted_iota(jnp.int32, block.shape, 0) + place[2] * block.shape[0]
    hot_t = jnp.where(lines == lanes[...], 1.0, 0.0).T.astype(bf16)
    b0, b1, b2 = pieces(block)
    turned_block = block.T
    high_t, low_t = halves(turned_block)
    both = mm(jnp.concatenate([hot_t, high_t]), jnp.concatenate([b0, b1], axis=1))
    cee = both[:W, :W] + both[:W, W:] + mm(hot_t, b2)
    g00 = both[W:, :W] + both[W:, W:] + mm(low_t, b0)
    parts = out.shape[0]
    bit = W // parts
    for p in range(parts):
        lines = slice(p * bit, (p + 1) * bit)
        out[p, :bit, :] = g00[lines]
        out[p, bit:, :] = cee[lines]


def grams_of_start(place, seeds, start, parts):
    return pl.pallas_call(
        start_grams,
        out_shape=jax.ShapeDtypeStruct((parts, 2 * W // parts, W), f32),
        in_specs=[SMEM, VMEM, VMEM],
        out_specs=VMEM,
        compiler_params=room(16),
    )(place, seeds.reshape(1, W), start)


def cross(a, b):
    right = halves(b)
    high, low = halves(a.T)
    both = mm(high, jnp.concatenate(right, axis=1))
    return both[:, :W] + both[:, W:] + mm(low, right[0])


def step_grams(mine, start, out):
    step = blocks_of(mine, 0, W)
    out[:W, :] = cross(start[...], step)
    out[W:, :] = cross(step, step)


def corner():
    return lax.broadcasted_iota(jnp.int32, (W, W), 0), lax.broadcasted_iota(jnp.int32, (W, W), 1)


SPARE = 8


def next_grams(place, mine, following, out):
    parts = mine.shape[0]
    bit = W // parts
    step = blocks_of(mine, 0, W)
    then, g01, g11 = (
        turned_blocks(following, place, s, n, range(parts)) for s, n in ((0, W), (W, bit), (W + bit, bit))
    )
    g12, g22 = cross(step, then), cross(then, then)
    i, j = corner()
    out[:W, :] = g01
    out[W : 2 * W, :] = g11
    out[2 * W : 3 * W, :] = jnp.where(j >= i, g22, g12)
    diagonal = jnp.sum(jnp.where(i == j, g12, 0.0), axis=0, keepdims=True)
    out[3 * W :, :] = jnp.broadcast_to(diagonal, (SPARE, W))


def unpacked(totals):
    total = jnp.sum(totals, axis=0)
    body = total[:W]
    i, j = corner()
    lower = jnp.where(j < i, body, 0.0)
    g12 = lower + lower.T + jnp.where(i == j, total[W : W + 1], 0.0)
    return g12, jnp.where(j >= i, body, 0.0) + jnp.where(j > i, body, 0.0).T


def second_product(place, covariance, mine, theirs, grams, out, small, buffer, sems, total):
    height, _ = covariance.shape
    half = height // 2
    tall = height // CHUNKS
    copies = chunks_of(covariance, buffer, sems)
    for copy in copies:
        copy.start()
    first = place[1] == 0
    parts = out.shape[0]
    bit = W // parts
    for p in range(parts):
        out[p, W : W + bit, :] = grams[p * bit : (p + 1) * bit, :]
        out[p, W + bit :, :] = grams[W + p * bit : W + (p + 1) * bit, :]
    for i in range(2):
        lines = W + i * bit
        small[i * W : (i + 1) * W, :] = blocks_of(mine, lines, bit) + blocks_of(theirs, lines, bit)
    for i, copy in enumerate(copies):
        lines = slice(i * tall % half // W, (i * tall % half + tall) // W)
        own, other = (mine, theirs) if i * tall < half else (theirs, mine)
        block = jnp.where(first, own[lines, :W, :], other[lines, :W, :]).reshape(tall, W)
        v_high, v_low = halves(block.T)
        copy.wait()
        high, low = halves(buffer[i])
        both = mm(jnp.concatenate([v_high, v_low]), high)
        value = both[:W] + both[W:] + mm(v_high, low)
        if i == 0:
            total[...] = value
        elif i + 1 < CHUNKS:
            total[...] += value
        else:
            value += total[...]
            for p in range(parts):
                out[p, :W, :] = value[:, p * W : (p + 1) * W].T


def image_of_step(place, covariance, mine, theirs, grams):
    breadth = covariance.shape[1]
    parts = breadth // W
    return pl.pallas_call(
        second_product,
        out_shape=[
            jax.ShapeDtypeStruct((parts, W + 2 * (W // parts), W), f32),
            jax.ShapeDtypeStruct((2 * W, W), f32),
        ],
        in_specs=[SMEM, HBM] + [VMEM] * 3,
        out_specs=[VMEM] * 2,
        scratch_shapes=chunk_scratch(covariance) + [pltpu.VMEM((W, breadth), f32)],
        compiler_params=room(50),
    )(place, covariance, mine, theirs, grams)


def basis_rows(place, mine, mine_start, mine_next, theirs, theirs_start, theirs_next, mix, out, wide, tip):
    step = pl.program_id(0)
    count = pl.num_programs(0) // 2
    tall = out.shape[0]
    parts = tall // W

    @pl.when(step == 0)
    def _():
        high, low = halves(mix[: 2 * W, : 2 * W])
        wide[:, : 2 * W] = high
        wide[:, 2 * W :] = low
        high, low = halves(mix[:, 2 * W :])
        tip[:, :W] = high
        tip[:, W:] = low

    def rows(pair, start, following, part):
        order = [part + p for p in range(parts)]
        left = jnp.concatenate(
            [
                start[pl.ds(pl.multiple_of(part * W, tall), tall), :],
                pair[pl.ds(part, parts), :W, :].reshape(tall, W),
                turned_blocks(following, place, 0, W, order),
            ],
            axis=1,
        )
        high, low = halves(left)
        h2, l2 = high[:, : 2 * W], low[:, : 2 * W]
        out[:, : 2 * W] = mm(h2, wide[:, : 2 * W]) + mm(h2, wide[:, 2 * W :]) + mm(l2, wide[:, : 2 * W])
        both = mm(high, tip[...])
        out[:, 2 * W :] = both[:, :W] + both[:, W:] + mm(low, tip[:, :W])

    @pl.when(step < count)
    def _():
        rows(mine, mine_start, mine_next, step * parts)

    @pl.when(step >= count)
    def _():
        rows(theirs, theirs_start, theirs_next, (step - count) * parts)


def basis_of(place, mine, mine_start, mine_next, theirs, theirs_start, theirs_next, mix):
    half = mine.shape[0] * W
    tall = 512
    count = half // tall
    return pl.pallas_call(
        basis_rows,
        out_shape=jax.ShapeDtypeStruct((2 * half, mix.shape[1]), f32),
        grid_spec=pltpu.PrefetchScalarGridSpec(
            num_scalar_prefetch=1,
            grid=(2 * count,),
            in_specs=[VMEM] * 7,
            out_specs=pl.BlockSpec(
                (tall, mix.shape[1]),
                lambda i, c: (jnp.where(i < count, i + c[1] * count, i - count + (1 - c[1]) * count), 0),
            ),
            scratch_shapes=[pltpu.VMEM((2 * W, 4 * W), bf16), pltpu.VMEM((3 * W, 2 * W), bf16)],
        ),
        compiler_params=room(24),
    )(place, mine, mine_start, mine_next, theirs, theirs_start, theirs_next, mix)


def scattered(parts, axis):
    return jnp.sum(lax.all_to_all(parts, axis, 0, 0, tiled=True), axis=0)


def gathered(part, axis):
    copies = jnp.broadcast_to(part, (lax.axis_size(axis), *part.shape))
    return lax.all_to_all(copies, axis, 0, 0, tiled=True)


def other_core(value):
    return lax.ppermute(value, CORE, SWAP)


def turned(rows, chips, cores):
    return [
        ((r * chips + a) * cores + b, (a * chips + SLOTS[a][r]) * cores + b)
        for r in range(rows)
        for a in range(chips)
        for b in range(cores)
    ]


def local(covariance, seed_index):
    height, breadth = covariance.shape
    width = seed_index.shape[0]
    rows, chips, cores = (lax.axis_size(a) for a in ALL)
    row, chip, core = (lax.axis_index(a) for a in ALL)
    order = height * rows
    square = (width, width)
    turn = turned(rows, chips, cores)
    slots = jnp.array(SLOTS, jnp.int32).reshape(-1)
    place = jnp.concatenate([jnp.stack([row, core, chip * cores + core]).astype(jnp.int32), slots])
    start_piece = scattered(picked_rows(place, seed_index, covariance, rows), ROWS).T
    start = gathered(start_piece, ROWS).reshape(breadth, width)
    mine_start = lax.ppermute(start, ALL, turn)
    keep, send = image_of_start(place, seed_index, covariance, start)
    got = other_core(send)
    small = grams_of_start(place, seed_index, start, chips)
    parts = jnp.concatenate([keep + got, small], axis=1)
    step = scattered(parts, CHIP)
    mine = gathered(step, CHIP)
    theirs = other_core(mine)
    (grams,) = kernel(step_grams, [(2 * width, width)], [], mine, mine_start)
    parts, zero_grams = image_of_step(place, covariance, mine, theirs, grams)
    piece = lax.ppermute(scattered(parts, ROWS), ALL, turn)
    (inv0,) = kernel(first_factor, [square], [(width, 2 * width), square], zero_grams)
    mine_next, inv0 = lax.optimization_barrier((gathered(piece, CHIP), inv0))
    (keep,) = kernel(next_grams, [(3 * width + SPARE, width)], [], place, mine, mine_next)
    got = other_core(keep)
    totals = gathered(keep[2 * width :] + got[2 * width :], ROWS)
    theirs_next = other_core(mine_next)
    theirs_start = other_core(mine_start)
    (pack,) = kernel(
        middle, [(PACK * width, width)], [(width, 2 * width), square, square], zero_grams, inv0, keep, got
    )
    totals, pack = lax.optimization_barrier((totals, pack))
    scale = float(order) ** 0.5

    def last_step(*refs):
        last(f32(scale), *refs)

    mix, projection, first_pass = kernel(
        last_step,
        [(3 * width, 3 * width), (3 * width, 2 * width), (3 * width, 2 * width)],
        [(width, 2 * width), square, square],
        pack,
        totals,
    )
    basis = basis_of(place, mine, mine_start, mine_next, theirs, theirs_start, theirs_next, mix)
    return basis, projection, first_pass


def solution(mesh):
    rows, cols = mesh.devices.shape
    fine = Mesh(mesh.devices.reshape(rows, cols // 2, 2), ALL)

    return jax.shard_map(
        local,
        mesh=fine,
        in_specs=(P(ROWS, (CHIP, CORE)), P()),
        out_specs=(P(ROWS, None), P(), P()),
        check_vma=False,
    )
```

```python
import jax
import jax.numpy as jnp
from jax import lax
from jax.experimental import pallas as pl
from jax.experimental.pallas import tpu as pltpu
from jax.sharding import Mesh, PartitionSpec as P

ROWS = "row"
CHIP = "chip"
CORE = "core"
ALL = (ROWS, CHIP, CORE)
SWAP = [(0, 1), (1, 0)]
SLOTS = (
    (2, 6, 0, 5, 1, 4, 3, 7),
    (7, 1, 4, 3, 5, 2, 6, 0),
    (1, 5, 0, 4, 3, 7, 2, 6),
    (4, 2, 5, 1, 6, 0, 7, 3),
    (5, 0, 7, 1, 6, 2, 4, 3),
    (1, 4, 0, 6, 3, 5, 2, 7),
    (4, 3, 7, 2, 6, 1, 5, 0),
    (2, 4, 3, 6, 0, 7, 1, 5),
)
W = 128
f32 = jnp.float32
bf16 = jnp.bfloat16
HI = lax.Precision.HIGHEST


def dot(a, b, dims):
    return lax.dot_general(a, b, (dims, ((), ())), precision=HI, preferred_element_type=f32)


def nn(a, b):
    return dot(a, b, ((1,), (0,)))


def tn(a, b):
    return dot(a, b, ((0,), (0,)))


def nt(a, b):
    return dot(a, b, ((1,), (1,)))


def pieces(x):
    a = x.astype(bf16)
    rest = x - a.astype(f32)
    b = rest.astype(bf16)
    return a, b, (rest - b.astype(f32)).astype(bf16)


def outer(left, panel):
    a0, a1, a2 = pieces(left)
    b0, b1, b2 = pieces(panel)
    return lax.dot_general(
        jnp.concatenate([a0, a0, a1, a0, a2, a1]),
        jnp.concatenate([b0, b1, b0, b2, b0, b1]),
        (((0,), (0,)), ((), ())),
        preferred_element_type=f32,
    )


BAND = 16


def factor(gram):
    sub = lax.broadcasted_iota(jnp.int32, (BAND, W), 0)
    lane = lax.broadcasted_iota(jnp.int32, (BAND, W), 1)
    eye = lax.broadcasted_iota(jnp.int32, (W, W), 0) == lax.broadcasted_iota(jnp.int32, (W, W), 1)
    rest = jnp.concatenate([gram, eye.astype(f32)], axis=1)
    now, rest = rest[:BAND], rest[BAND:]
    upper, inverse = [], []
    for base in range(0, W, BAND):
        left, right = now[:, :W], now[:, W:]
        cols = [jnp.broadcast_to(left[:, base + k : base + k + 1], (BAND, W)) for k in range(BAND)]
        scale = jnp.zeros((BAND, W), f32)
        for k in range(0, BAND, 2):
            top = k // 8 * 8
            here = sub[top:]

            def line(x, i):
                return jnp.broadcast_to(x[i : i + 1, :], (BAND - top, W))

            def below(old, new):
                return new if top == 0 else jnp.concatenate([old[:top], new])

            c, d = cols[k][top:], cols[k + 1][top:]
            p, q, r = line(cols[k], k), line(cols[k + 1], k), line(cols[k + 1], k + 1)
            det = p * r - q * q
            inv_p = 1.0 / p
            inv = 1.0 / det
            later = here > k + 1
            u = jnp.where(later, (c * r - d * q) * inv, jnp.where(here == k + 1, q * inv_p, 0.0))
            v = jnp.where(later, (d * p - c * q) * inv, 0.0)
            last_scale = jnp.where(here == k + 1, lax.rsqrt(det * inv_p), scale[top:])
            scale = below(scale, jnp.where(here == k, lax.rsqrt(p), last_scale))

            def update(x):
                return below(x, x[top:] - u * line(x, k) - v * line(x, k + 1))

            for m in range(k + 2, BAND):
                cols[m] = update(cols[m])
            left = update(left)
            right = update(right)
        left = jnp.where(lane >= base + sub, left * scale, 0.0)
        right = right * scale
        upper.append(left)
        inverse.append(right)
        end = base + BAND
        if end < W:
            panel = jnp.concatenate([left, right], axis=1)
            now = rest[:BAND] - outer(left[:, end : end + BAND], panel)
            if end + BAND < W:
                rest = rest[BAND:] - outer(left[:, end + BAND :], panel)
    return jnp.concatenate(upper), jnp.concatenate(inverse)


def blocks_of(ref, start, count):
    return ref[:, start : start + count, :].reshape(ref.shape[0] * count, W)


def turned_blocks(ref, place, start, count, parts):
    return jnp.concatenate([ref[place[3 + place[0] * ref.shape[0] + p], start : start + count, :] for p in parts])


def first_factor(g00, inverse):
    inverse[...] = factor(g00[:W, :])[1]


def middle(start, inv0, keep, got, pack, stage, sems):
    g00, cee = start[:W, :], start[W:, :]
    li0 = inv0[...]
    g01, g11 = (keep[i * W : (i + 1) * W, :] + got[i * W : (i + 1) * W, :] for i in range(2))
    x0 = li0.T
    u = nt(cee, li0)
    side = jnp.concatenate([g00, g01], axis=1)
    gram = jnp.concatenate([side, jnp.concatenate([g01.T, g11], axis=1)])
    h = nn(li0, nn(side, jnp.concatenate([u, x0])))
    m00 = nn(li0, nt(g00, li0))
    h_full = h + (h - nn(m00, h))
    g02 = g11 + tn(cee, g01)
    for i, block in enumerate([h, h_full, m00, g02, g00, g01, g11, li0]):
        stage[i * W : (i + 1) * W, :] = block
    pack_copy(stage, pack, sems, 0).start()
    comb = jnp.concatenate([u - nn(x0, h_full), x0])
    y = nn(gram, comb)
    upper1, li1 = factor(tn(comb, y))
    c1 = nt(comb, li1)
    y1 = nt(y, li1)
    m01 = nn(li0, y1[:W])
    i1 = jnp.concatenate([nn(cee, c1[:W]), c1])
    s0 = nn(jnp.concatenate([side, g02], axis=1), i1)
    s1 = nn(gram[W:], i1[: 2 * W])
    late = [upper1, i1[:W], i1[W : 2 * W], i1[2 * W :], m01, tn(c1, y1), nn(li0, s0), tn(c1[:W], s0), s1]
    for i, block in enumerate(late):
        stage[EARLY + i * W : EARLY + (i + 1) * W, :] = block
    second = pack_copy(stage, pack, sems, 1)
    second.start()
    pack_copy(stage, pack, sems, 0).wait()
    second.wait()


EARLY = 8 * W
PACK = 17 * W


def pack_copy(source, target, sems, late):
    lines = pl.ds(EARLY, PACK - EARLY) if late else pl.ds(0, EARLY)
    return pltpu.make_async_copy(source.at[lines, :], target.at[lines, :], sems.at[late])


def last(scale, packed, totals, mix, projection, first_pass, pack, sems):
    copies = [pack_copy(packed, pack, sems, i) for i in range(2)]
    for copy in copies:
        copy.start()
    a12, a22 = unpacked(totals[...])
    for copy in copies:
        copy.wait()
    first, full, m00, a02, a00, a01, a11, li0, upper1, _, c1_top, c1_low, m01, m11, first0, part1, s1 = (
        pack[i * W : (i + 1) * W, :] for i in range(PACK // W)
    )
    i1 = pack[EARLY + W : EARLY + 4 * W, :]
    c1 = i1[W:]
    gram = jnp.concatenate(
        [
            jnp.concatenate([a00, a01, a02], axis=1),
            jnp.concatenate([a01.T, a11, a12], axis=1),
            jnp.concatenate([a02.T, a12, a22], axis=1),
        ]
    )
    h = jnp.concatenate([first0, part1 + tn(c1_low, s1 + nn(a12, c1_low))])
    gram_p = jnp.concatenate([jnp.concatenate([m00, m01], axis=1), jnp.concatenate([m01.T, m11], axis=1)])
    h_full = h + (h - nn(gram_p, h))
    zero = jnp.zeros((W, W), f32)
    places = jnp.concatenate([jnp.concatenate([li0.T, zero]), c1], axis=1)
    comb = jnp.concatenate([i1[: 2 * W] - nn(places, h_full), i1[2 * W :]])
    upper2, li2 = factor(tn(comb, nn(gram, comb)))
    mix[: 2 * W, : 2 * W] = places * scale
    mix[2 * W :, : 2 * W] = jnp.zeros((W, 2 * W), f32)
    mix[:, 2 * W :] = nt(comb, li2) * scale
    projection[:W, :W] = full
    projection[W : 2 * W, :W] = upper1
    projection[2 * W :, :W] = zero
    projection[: 2 * W, W:] = h_full
    projection[2 * W :, W:] = upper2
    first_pass[:W, :W] = first
    first_pass[W:, :W] = jnp.zeros((2 * W, W), f32)
    first_pass[: 2 * W, W:] = h
    first_pass[2 * W :, W:] = zero


HBM = pl.BlockSpec(memory_space=pltpu.HBM)
VMEM = pl.BlockSpec(memory_space=pltpu.VMEM)
SMEM = pl.BlockSpec(memory_space=pltpu.SMEM)


def room(mib):
    return pltpu.CompilerParams(vmem_limit_bytes=mib * 2**20)


def kernel(body, shapes, *args):
    return pl.pallas_call(
        body,
        out_shape=[jax.ShapeDtypeStruct(s, f32) for s in shapes],
        in_specs=[VMEM if a.dtype == f32 else SMEM for a in args],
        out_specs=[VMEM] * len(shapes),
        compiler_params=room(16),
    )(*args)


def halves(x):
    high = x.astype(bf16)
    return high, (x - high.astype(f32)).astype(bf16)


def mm(a, b):
    return lax.dot_general(a, b, (((1,), (0,)), ((), ())), preferred_element_type=f32)


def pick_rows(place, seeds, lanes, covariance, out, buffer, sem):
    count = seeds.shape[0]
    height = covariance.shape[0]
    base = place[0] * height

    def row(line, i):
        return pltpu.make_async_copy(covariance.at[pl.ds(line, 1), :], buffer.at[pl.ds(i, 1), :], sem)

    def body(i, found):
        line = seeds[i] - base
        here = (line >= 0) & (line < height)

        @pl.when(here)
        def _():
            row(line, i).start()

        return found + here.astype(jnp.int32)

    found = lax.fori_loop(0, count, body, 0, unroll=8)
    offsets = jnp.broadcast_to(lanes[...] - base, (count, count))
    held = jnp.where((offsets >= 0) & (offsets < height), 1.0, 0.0).T > 0

    def done(i, carry):
        row(0, 0).wait()
        return carry

    lax.fori_loop(0, found, done, 0)
    for p in range(out.shape[0]):
        out[p] = jnp.where(held, buffer[:, p * W : (p + 1) * W], 0.0)


def picked_rows(place, seeds, covariance, parts):
    count = seeds.shape[0]
    return pl.pallas_call(
        pick_rows,
        out_shape=jax.ShapeDtypeStruct((parts, count, W), f32),
        in_specs=[SMEM, SMEM, VMEM, HBM],
        out_specs=VMEM,
        scratch_shapes=[pltpu.VMEM((count, covariance.shape[1]), f32), pltpu.SemaphoreType.DMA],
    )(place, seeds, seeds.reshape(1, count), covariance)


CHUNKS = 8


def chunks_of(covariance, buffer, sems):
    tall = covariance.shape[0] // CHUNKS
    return [
        pltpu.make_async_copy(covariance.at[pl.ds(i * tall, tall), :], buffer.at[i], sems.at[i]) for i in range(CHUNKS)
    ]


def chunk_scratch(covariance):
    height, breadth = covariance.shape
    return [pltpu.VMEM((CHUNKS, height // CHUNKS, breadth), f32), pltpu.SemaphoreType.DMA((CHUNKS,))]


def first_product(place, lanes, covariance, start, keep, send, buffer, sems):
    height, breadth = covariance.shape
    half = height // 2
    tall = height // CHUNKS
    copies = chunks_of(covariance, buffer, sems)
    for copy in copies:
        copy.start()
    lines = lax.broadcasted_iota(jnp.int32, (breadth, W), 0) + place[2] * breadth
    hot = jnp.where(lines == lanes[...], 1.0, 0.0)
    hit = jnp.max(hot, axis=1, keepdims=True) > 0
    weights = jnp.concatenate(halves(jnp.where(hit, 0.0, start[...])), axis=1)
    first = place[1] == 0
    for i, copy in enumerate(copies):
        copy.wait()
        high, low = halves(buffer[i])
        both = mm(high, weights)
        value = both[:, :W] + both[:, W:] + mm(low, weights[:, :W])
        mine = first if i * tall < half else jnp.logical_not(first)

        def store(out):
            for q in range(tall // W):
                out[i * tall % half // W + q] = value[q * W : (q + 1) * W, :]

        @pl.when(mine)
        def _():
            store(keep)

        @pl.when(jnp.logical_not(mine))
        def _():
            store(send)


def image_of_start(place, seeds, covariance, start):
    height = covariance.shape[0]
    shape = jax.ShapeDtypeStruct((height // 2 // W, W, W), f32)
    return pl.pallas_call(
        first_product,
        out_shape=[shape, shape],
        in_specs=[SMEM, VMEM, HBM, VMEM],
        out_specs=[VMEM] * 2,
        scratch_shapes=chunk_scratch(covariance),
        compiler_params=room(50),
    )(place, seeds.reshape(1, W), covariance, start)


def start_grams(place, lanes, start, out):
    block = start[...]
    lines = lax.broadcasted_iota(jnp.int32, block.shape, 0) + place[2] * block.shape[0]
    hot_t = jnp.where(lines == lanes[...], 1.0, 0.0).T.astype(bf16)
    b0, b1, b2 = pieces(block)
    turned_block = block.T
    high_t, low_t = halves(turned_block)
    both = mm(jnp.concatenate([hot_t, high_t]), jnp.concatenate([b0, b1], axis=1))
    cee = both[:W, :W] + both[:W, W:] + mm(hot_t, b2)
    g00 = both[W:, :W] + both[W:, W:] + mm(low_t, b0)
    parts = out.shape[0]
    bit = W // parts
    for p in range(parts):
        lines = slice(p * bit, (p + 1) * bit)
        out[p, :bit, :] = g00[lines]
        out[p, bit:, :] = cee[lines]


def grams_of_start(place, seeds, start, parts):
    return pl.pallas_call(
        start_grams,
        out_shape=jax.ShapeDtypeStruct((parts, 2 * W // parts, W), f32),
        in_specs=[SMEM, VMEM, VMEM],
        out_specs=VMEM,
        compiler_params=room(16),
    )(place, seeds.reshape(1, W), start)


def cross(a, b):
    right = halves(b)
    high, low = halves(a.T)
    both = mm(high, jnp.concatenate(right, axis=1))
    return both[:, :W] + both[:, W:] + mm(low, right[0])


def step_grams(place, mine, out):
    parts = mine.shape[0]
    step, start = blocks_of(mine, 0, W), turned_blocks(mine, place, W + 2 * W // parts, W, range(parts))
    out[:W, :] = cross(start, step)
    out[W:, :] = cross(step, step)


def corner():
    return lax.broadcasted_iota(jnp.int32, (W, W), 0), lax.broadcasted_iota(jnp.int32, (W, W), 1)


SPARE = 8


def next_grams(place, mine, following, out):
    parts = mine.shape[0]
    bit = W // parts
    step = blocks_of(mine, 0, W)
    then, g01, g11 = (
        turned_blocks(following, place, s, n, range(parts)) for s, n in ((0, W), (W, bit), (W + bit, bit))
    )
    g12, g22 = cross(step, then), cross(then, then)
    i, j = corner()
    out[:W, :] = g01
    out[W : 2 * W, :] = g11
    out[2 * W : 3 * W, :] = jnp.where(j >= i, g22, g12)
    diagonal = jnp.sum(jnp.where(i == j, g12, 0.0), axis=0, keepdims=True)
    out[3 * W :, :] = jnp.broadcast_to(diagonal, (SPARE, W))


def unpacked(totals):
    total = jnp.sum(totals, axis=0)
    body = total[:W]
    i, j = corner()
    lower = jnp.where(j < i, body, 0.0)
    g12 = lower + lower.T + jnp.where(i == j, total[W : W + 1], 0.0)
    return g12, jnp.where(j >= i, body, 0.0) + jnp.where(j > i, body, 0.0).T


def second_product(place, covariance, mine, theirs, grams, out, small, buffer, sems, total):
    height, breadth = covariance.shape
    half = height // 2
    tall = height // CHUNKS
    copies = chunks_of(covariance, buffer, sems)
    for copy in copies:
        copy.start()
    first = place[1] == 0
    parts = out.shape[0]
    bit = W // parts
    for p in range(parts):
        out[p, W : W + bit, :] = grams[p * bit : (p + 1) * bit, :]
        out[p, W + bit :, :] = grams[W + p * bit : W + (p + 1) * bit, :]
    for i in range(2):
        lines = W + i * bit
        small[i * W : (i + 1) * W, :] = blocks_of(mine, lines, bit) + blocks_of(theirs, lines, bit)
    for i, copy in enumerate(copies):
        lines = slice(i * tall % half // W, (i * tall % half + tall) // W)
        own, other = (mine, theirs) if i * tall < half else (theirs, mine)
        block = jnp.where(first, own[lines, :W, :], other[lines, :W, :]).reshape(tall, W)
        v_high, v_low = halves(block.T)
        copy.wait()
        high, low = halves(buffer[i])
        both = mm(jnp.concatenate([v_high, v_low]), high)
        value = both[:W] + both[W:] + mm(v_high, low)
        if i == 0:
            total[...] = value
        elif i + 1 < CHUNKS:
            total[...] += value
        else:
            value += total[...]
            for p in range(parts):
                out[p, :W, :] = value[:, p * W : (p + 1) * W].T


def image_of_step(place, covariance, mine, theirs, grams):
    breadth = covariance.shape[1]
    parts = breadth // W
    return pl.pallas_call(
        second_product,
        out_shape=[
            jax.ShapeDtypeStruct((parts, W + 2 * (W // parts), W), f32),
            jax.ShapeDtypeStruct((2 * W, W), f32),
        ],
        in_specs=[SMEM, HBM] + [VMEM] * 3,
        out_specs=[VMEM] * 2,
        scratch_shapes=chunk_scratch(covariance) + [pltpu.VMEM((W, breadth), f32)],
        compiler_params=room(50),
    )(place, covariance, mine, theirs, grams)


def basis_rows(place, mine, mine_next, theirs, theirs_next, mix, out, stage, sems):
    parts = mine.shape[0]
    bit = 2 * W // parts
    count, tall, _ = stage.shape
    half = count * tall // 2
    high, low = halves(mix[: 2 * W, : 2 * W])
    tip_high, tip_low = halves(mix[:, 2 * W :])
    tip = jnp.concatenate([tip_high, tip_low], axis=1)
    copies = []
    for i in range(count):
        line = i * tall % half
        pair, following, side = (mine, mine_next, place[1]) if i * tall < half else (theirs, theirs_next, 1 - place[1])
        order = range(line // W, (line + tall) // W)
        left = jnp.concatenate(
            [
                turned_blocks(pair, place, W + bit, W, order),
                pair[line // W : (line + tall) // W, :W, :].reshape(tall, W),
                turned_blocks(following, place, 0, W, order),
            ],
            axis=1,
        )
        l_high, l_low = halves(left)
        h2, l2 = l_high[:, : 2 * W], l_low[:, : 2 * W]
        stage[i, :, : 2 * W] = mm(h2, high) + mm(h2, low) + mm(l2, high)
        both = mm(l_high, tip)
        stage[i, :, 2 * W :] = both[:, :W] + both[:, W:] + mm(l_low, tip_high)
        rows = pl.ds(pl.multiple_of(side * half + line, tall), tall)
        copies.append(pltpu.make_async_copy(stage.at[i], out.at[rows, :], sems.at[i]))
        copies[-1].start()
    for copy in copies:
        copy.wait()


def basis_of(place, mine, mine_next, theirs, theirs_next, mix):
    height = 2 * mine.shape[0] * W
    tall = 256
    breadth = mix.shape[1]
    return pl.pallas_call(
        basis_rows,
        out_shape=jax.ShapeDtypeStruct((height, breadth), f32),
        in_specs=[SMEM] + [VMEM] * 5,
        out_specs=HBM,
        scratch_shapes=[pltpu.VMEM((height // tall, tall, breadth), f32), pltpu.SemaphoreType.DMA((height // tall,))],
        compiler_params=room(24),
    )(place, mine, mine_next, theirs, theirs_next, mix)


def scattered(parts, axis):
    return jnp.sum(lax.all_to_all(parts, axis, 0, 0, tiled=True), axis=0)


def gathered(part, axis):
    copies = jnp.broadcast_to(part, (lax.axis_size(axis), *part.shape))
    return lax.all_to_all(copies, axis, 0, 0, tiled=True)


def other_core(value):
    return lax.ppermute(value, CORE, SWAP)


def turned(rows, chips, cores):
    return [
        ((r * chips + a) * cores + b, (a * chips + SLOTS[a][r]) * cores + b)
        for r in range(rows)
        for a in range(chips)
        for b in range(cores)
    ]


def local(covariance, seed_index):
    height, breadth = covariance.shape
    width = seed_index.shape[0]
    rows, chips, cores = (lax.axis_size(a) for a in ALL)
    row, chip, core = (lax.axis_index(a) for a in ALL)
    order = height * rows
    square = (width, width)
    turn = turned(rows, chips, cores)
    slots = jnp.array(SLOTS, jnp.int32).reshape(-1)
    place = jnp.concatenate([jnp.stack([row, core, chip * cores + core]).astype(jnp.int32), slots])
    start_piece = scattered(picked_rows(place, seed_index, covariance, rows), ROWS).T
    start_turned = lax.ppermute(start_piece, ALL, turn)
    start = gathered(start_piece, ROWS).reshape(breadth, width)
    start, start_turned = lax.optimization_barrier((start, start_turned))
    keep, send = image_of_start(place, seed_index, covariance, start)
    got = other_core(send)
    small = grams_of_start(place, seed_index, start, chips)
    parts = jnp.concatenate([keep + got, small], axis=1)
    mine = gathered(jnp.concatenate([scattered(parts, CHIP), start_turned]), CHIP)
    theirs = other_core(mine)
    (grams,) = kernel(step_grams, [(2 * width, width)], place, mine)
    parts, zero_grams = image_of_step(place, covariance, mine, theirs, grams)
    piece = lax.ppermute(scattered(parts, ROWS), ALL, turn)
    (inv0,) = kernel(first_factor, [square], zero_grams)
    mine_next, inv0 = lax.optimization_barrier((gathered(piece, CHIP), inv0))
    (keep,) = kernel(next_grams, [(3 * width + SPARE, width)], place, mine, mine_next)
    got = other_core(keep)
    totals = gathered(keep[2 * width :] + got[2 * width :], ROWS)
    theirs_next = other_core(mine_next)
    stage = [pltpu.VMEM((PACK, width), f32), pltpu.SemaphoreType.DMA((2,))]
    pack = pl.pallas_call(
        middle,
        out_shape=jax.ShapeDtypeStruct((PACK, width), f32),
        in_specs=[VMEM] * 4,
        out_specs=HBM,
        scratch_shapes=stage,
        compiler_params=room(60),
    )(zero_grams, inv0, keep, got)
    totals, pack = lax.optimization_barrier((totals, pack))
    scale = float(order) ** 0.5

    def last_step(*refs):
        last(f32(scale), *refs)

    shapes = [(3 * width, 3 * width), (3 * width, 2 * width), (3 * width, 2 * width)]
    mix, projection, first_pass = pl.pallas_call(
        last_step,
        out_shape=[jax.ShapeDtypeStruct(s, f32) for s in shapes],
        in_specs=[HBM, VMEM],
        out_specs=[VMEM] * 3,
        scratch_shapes=stage,
        compiler_params=room(52),
    )(pack, totals)
    basis = basis_of(place, mine, mine_next, theirs, theirs_next, mix)
    return basis, projection, first_pass


def solution(mesh):
    rows, cols = mesh.devices.shape
    fine = Mesh(mesh.devices.reshape(rows, cols // 2, 2), ALL)
    return jax.shard_map(
        local,
        mesh=fine,
        in_specs=(P(ROWS, (CHIP, CORE)), P()),
        out_specs=(P(ROWS, None), P(), P()),
        check_vma=False,
    )
```

```python
import jax
import jax.numpy as jnp
from jax import lax
from jax.experimental import pallas as pl
from jax.experimental.pallas import tpu as pltpu
from jax.sharding import Mesh, PartitionSpec as P

ROWS = "row"
CHIP = "chip"
CORE = "core"
ALL = (ROWS, CHIP, CORE)
SWAP = [(0, 1), (1, 0)]
SLOTS = (
    (
        (2, 6, 3, 5, 0, 4, 1, 7),
        (7, 3, 6, 2, 5, 1, 4, 0),
        (3, 5, 0, 4, 1, 7, 2, 6),
        (4, 0, 5, 1, 6, 2, 7, 3),
        (4, 0, 7, 3, 6, 2, 5, 1),
        (1, 5, 2, 6, 3, 7, 0, 4),
        (7, 3, 6, 2, 5, 1, 4, 0),
        (2, 4, 3, 7, 0, 6, 1, 5),
    ),
    (
        (2, 6, 1, 7, 0, 4, 3, 5),
        (7, 3, 4, 0, 5, 1, 6, 2),
        (3, 7, 0, 4, 1, 5, 2, 6),
        (6, 0, 5, 1, 4, 2, 7, 3),
        (4, 0, 7, 1, 6, 2, 5, 3),
        (1, 5, 0, 6, 3, 7, 2, 4),
        (7, 3, 6, 2, 5, 1, 4, 0),
        (2, 4, 3, 7, 0, 6, 1, 5),
    ),
)
W = 128
f32 = jnp.float32
bf16 = jnp.bfloat16
HI = lax.Precision.HIGHEST


def dot(a, b, dims):
    return lax.dot_general(a, b, (dims, ((), ())), precision=HI, preferred_element_type=f32)


def nn(a, b):
    return dot(a, b, ((1,), (0,)))


def tn(a, b):
    return dot(a, b, ((0,), (0,)))


def nt(a, b):
    return dot(a, b, ((1,), (1,)))


def pieces(x):
    a = x.astype(bf16)
    rest = x - a.astype(f32)
    b = rest.astype(bf16)
    return a, b, (rest - b.astype(f32)).astype(bf16)


def outer(left, panel):
    a0, a1, a2 = pieces(left)
    b0, b1, b2 = pieces(panel)
    return lax.dot_general(
        jnp.concatenate([a0, a0, a1, a0, a2, a1]),
        jnp.concatenate([b0, b1, b0, b2, b0, b1]),
        (((0,), (0,)), ((), ())),
        preferred_element_type=f32,
    )


BAND = 16


def factor(gram):
    sub = lax.broadcasted_iota(jnp.int32, (BAND, W), 0)
    lane = lax.broadcasted_iota(jnp.int32, (BAND, W), 1)
    eye = lax.broadcasted_iota(jnp.int32, (W, W), 0) == lax.broadcasted_iota(jnp.int32, (W, W), 1)
    rest = jnp.concatenate([gram, eye.astype(f32)], axis=1)
    now, rest = rest[:BAND], rest[BAND:]
    upper, inverse = [], []
    for base in range(0, W, BAND):
        left, right = now[:, :W], now[:, W:]
        cols = [jnp.broadcast_to(left[:, base + k : base + k + 1], (BAND, W)) for k in range(BAND)]
        scale = jnp.zeros((BAND, W), f32)
        for k in range(0, BAND, 2):
            top = k // 8 * 8
            here = sub[top:]

            def line(x, i):
                return jnp.broadcast_to(x[i : i + 1, :], (BAND - top, W))

            def below(old, new):
                return new if top == 0 else jnp.concatenate([old[:top], new])

            c, d = cols[k][top:], cols[k + 1][top:]
            p, q, r = line(cols[k], k), line(cols[k + 1], k), line(cols[k + 1], k + 1)
            det = p * r - q * q
            inv_p = 1.0 / p
            inv = 1.0 / det
            later = here > k + 1
            u = jnp.where(later, (c * r - d * q) * inv, jnp.where(here == k + 1, q * inv_p, 0.0))
            v = jnp.where(later, (d * p - c * q) * inv, 0.0)
            last_scale = jnp.where(here == k + 1, lax.rsqrt(det * inv_p), scale[top:])
            scale = below(scale, jnp.where(here == k, lax.rsqrt(p), last_scale))

            def update(x):
                return below(x, x[top:] - u * line(x, k) - v * line(x, k + 1))

            for m in range(k + 2, BAND):
                cols[m] = update(cols[m])
            left = update(left)
            right = update(right)
        left = jnp.where(lane >= base + sub, left * scale, 0.0)
        right = right * scale
        upper.append(left)
        inverse.append(right)
        end = base + BAND
        if end < W:
            panel = jnp.concatenate([left, right], axis=1)
            now = rest[:BAND] - outer(left[:, end : end + BAND], panel)
            if end + BAND < W:
                rest = rest[BAND:] - outer(left[:, end + BAND :], panel)
    return jnp.concatenate(upper), jnp.concatenate(inverse)


def blocks_of(ref, start, count):
    return ref[:, start : start + count, :].reshape(ref.shape[0] * count, W)


def turned_blocks(ref, place, table, start, count, parts, core):
    first = (core * ref.shape[0] + place[0]) * ref.shape[0]
    return jnp.concatenate([ref[table[first + p], start : start + count, :] for p in parts])


def first_factor(start, out):
    g00, cee = start[:W, :], start[W:, :]
    li0 = factor(g00)[1]
    u = nt(cee, li0)
    side = nn(li0, g00)
    for i, block in enumerate([li0, u, nn(side, u), nt(side, li0)]):
        out[i * W : (i + 1) * W, :] = block


def middle(start, ready, keep, got, pack, stage, sems):
    g00, cee = start[:W, :], start[W:, :]
    li0, u, h0, m00 = (ready[i * W : (i + 1) * W, :] for i in range(4))
    g01, g11 = (keep[i * W : (i + 1) * W, :] + got[i * W : (i + 1) * W, :] for i in range(2))
    x0 = li0.T
    side = jnp.concatenate([g00, g01], axis=1)
    gram = jnp.concatenate([side, jnp.concatenate([g01.T, g11], axis=1)])
    h = h0 + nt(nn(li0, g01), li0)
    h_full = h + (h - nn(m00, h))
    g02 = g11 + tn(cee, g01)
    for i, block in enumerate([h, h_full, m00, g02, g00, g01, g11, li0]):
        stage[i * W : (i + 1) * W, :] = block
    pack_copy(stage, pack, sems, 0).start()
    comb = jnp.concatenate([u - nn(x0, h_full), x0])
    y = nn(gram, comb)
    upper1, li1 = factor(tn(comb, y))
    c1 = nt(comb, li1)
    y1 = nt(y, li1)
    m01 = nn(li0, y1[:W])
    i1 = jnp.concatenate([nn(cee, c1[:W]), c1])
    s0 = nn(jnp.concatenate([side, g02], axis=1), i1)
    s1 = nn(gram[W:], i1[: 2 * W])
    late = [upper1, i1[:W], i1[W : 2 * W], i1[2 * W :], m01, tn(c1, y1), nn(li0, s0), tn(c1[:W], s0), s1]
    for i, block in enumerate(late):
        stage[EARLY + i * W : EARLY + (i + 1) * W, :] = block
    second = pack_copy(stage, pack, sems, 1)
    second.start()
    pack_copy(stage, pack, sems, 0).wait()
    second.wait()


EARLY = 8 * W
PACK = 17 * W


def pack_copy(source, target, sems, late):
    lines = pl.ds(EARLY, PACK - EARLY) if late else pl.ds(0, EARLY)
    return pltpu.make_async_copy(source.at[lines, :], target.at[lines, :], sems.at[late])


def last(scale, packed, totals, mix, projection, first_pass, pack, sems):
    copies = [pack_copy(packed, pack, sems, i) for i in range(2)]
    for copy in copies:
        copy.start()
    a12, a22 = unpacked(totals[...])
    for copy in copies:
        copy.wait()
    first, full, m00, a02, a00, a01, a11, li0, upper1, _, c1_top, c1_low, m01, m11, first0, part1, s1 = (
        pack[i * W : (i + 1) * W, :] for i in range(PACK // W)
    )
    i1 = pack[EARLY + W : EARLY + 4 * W, :]
    c1 = i1[W:]
    gram = jnp.concatenate(
        [
            jnp.concatenate([a00, a01, a02], axis=1),
            jnp.concatenate([a01.T, a11, a12], axis=1),
            jnp.concatenate([a02.T, a12, a22], axis=1),
        ]
    )
    h = jnp.concatenate([first0, part1 + tn(c1_low, s1 + nn(a12, c1_low))])
    gram_p = jnp.concatenate([jnp.concatenate([m00, m01], axis=1), jnp.concatenate([m01.T, m11], axis=1)])
    h_full = h + (h - nn(gram_p, h))
    zero = jnp.zeros((W, W), f32)
    places = jnp.concatenate([jnp.concatenate([li0.T, zero]), c1], axis=1)
    comb = jnp.concatenate([i1[: 2 * W] - nn(places, h_full), i1[2 * W :]])
    upper2, li2 = factor(tn(comb, nn(gram, comb)))
    mix[: 2 * W, : 2 * W] = places * scale
    mix[2 * W :, : 2 * W] = jnp.zeros((W, 2 * W), f32)
    mix[:, 2 * W :] = nt(comb, li2) * scale
    projection[:W, :W] = full
    projection[W : 2 * W, :W] = upper1
    projection[2 * W :, :W] = zero
    projection[: 2 * W, W:] = h_full
    projection[2 * W :, W:] = upper2
    first_pass[:W, :W] = first
    first_pass[W:, :W] = jnp.zeros((2 * W, W), f32)
    first_pass[: 2 * W, W:] = h
    first_pass[2 * W :, W:] = zero


HBM = pl.BlockSpec(memory_space=pltpu.HBM)
VMEM = pl.BlockSpec(memory_space=pltpu.VMEM)
SMEM = pl.BlockSpec(memory_space=pltpu.SMEM)


def room(mib):
    return pltpu.CompilerParams(vmem_limit_bytes=mib * 2**20)


def kernel(body, shapes, *args):
    return pl.pallas_call(
        body,
        out_shape=[jax.ShapeDtypeStruct(s, f32) for s in shapes],
        in_specs=[VMEM if a.dtype == f32 else SMEM for a in args],
        out_specs=[VMEM] * len(shapes),
        compiler_params=room(16),
    )(*args)


def halves(x):
    high = x.astype(bf16)
    return high, (x - high.astype(f32)).astype(bf16)


def mm(a, b):
    return lax.dot_general(a, b, (((1,), (0,)), ((), ())), preferred_element_type=f32)


def pick_rows(place, seeds, lanes, covariance, out, buffer, sem):
    count = seeds.shape[0]
    height = covariance.shape[0]
    base = place[0] * height

    def row(line, i):
        return pltpu.make_async_copy(covariance.at[pl.ds(line, 1), :], buffer.at[pl.ds(i, 1), :], sem)

    def body(i, found):
        line = seeds[i] - base
        here = (line >= 0) & (line < height)

        @pl.when(here)
        def _():
            row(line, i).start()

        return found + here.astype(jnp.int32)

    found = lax.fori_loop(0, count, body, 0, unroll=8)
    offsets = jnp.broadcast_to(lanes[...] - base, (count, count))
    held = jnp.where((offsets >= 0) & (offsets < height), 1.0, 0.0).T > 0

    def done(i, carry):
        row(0, 0).wait()
        return carry

    lax.fori_loop(0, found, done, 0)
    for p in range(out.shape[0]):
        out[p] = jnp.where(held, buffer[:, p * W : (p + 1) * W], 0.0)


def picked_rows(place, seeds, covariance, parts):
    count = seeds.shape[0]
    return pl.pallas_call(
        pick_rows,
        out_shape=jax.ShapeDtypeStruct((parts, count, W), f32),
        in_specs=[SMEM, SMEM, VMEM, HBM],
        out_specs=VMEM,
        scratch_shapes=[pltpu.VMEM((count, covariance.shape[1]), f32), pltpu.SemaphoreType.DMA],
    )(place, seeds, seeds.reshape(1, count), covariance)


CHUNKS = 8


def chunks_of(covariance, buffer, sems):
    tall = covariance.shape[0] // CHUNKS
    return [
        pltpu.make_async_copy(covariance.at[pl.ds(i * tall, tall), :], buffer.at[i], sems.at[i]) for i in range(CHUNKS)
    ]


def chunk_scratch(covariance):
    height, breadth = covariance.shape
    return [pltpu.VMEM((CHUNKS, height // CHUNKS, breadth), f32), pltpu.SemaphoreType.DMA((CHUNKS,))]


def first_product(place, lanes, covariance, start, keep, send, buffer, sems):
    height, breadth = covariance.shape
    half = height // 2
    tall = height // CHUNKS
    copies = chunks_of(covariance, buffer, sems)
    for copy in copies:
        copy.start()
    lines = lax.broadcasted_iota(jnp.int32, (breadth, W), 0) + place[2] * breadth
    hot = jnp.where(lines == lanes[...], 1.0, 0.0)
    hit = jnp.max(hot, axis=1, keepdims=True) > 0
    weights = jnp.concatenate(halves(jnp.where(hit, 0.0, start[...])), axis=1)
    first = place[1] == 0
    for i, copy in enumerate(copies):
        copy.wait()
        high, low = halves(buffer[i])
        both = mm(high, weights)
        value = both[:, :W] + both[:, W:] + mm(low, weights[:, :W])
        mine = first if i * tall < half else jnp.logical_not(first)

        def store(out):
            for q in range(tall // W):
                out[i * tall % half // W + q] = value[q * W : (q + 1) * W, :]

        @pl.when(mine)
        def _():
            store(keep)

        @pl.when(jnp.logical_not(mine))
        def _():
            store(send)


def image_of_start(place, seeds, covariance, start):
    height = covariance.shape[0]
    shape = jax.ShapeDtypeStruct((height // 2 // W, W, W), f32)
    return pl.pallas_call(
        first_product,
        out_shape=[shape, shape],
        in_specs=[SMEM, VMEM, HBM, VMEM],
        out_specs=[VMEM] * 2,
        scratch_shapes=chunk_scratch(covariance),
        compiler_params=room(50),
    )(place, seeds.reshape(1, W), covariance, start)


def start_grams(place, lanes, start, out):
    block = start[...]
    lines = lax.broadcasted_iota(jnp.int32, block.shape, 0) + place[2] * block.shape[0]
    hot_t = jnp.where(lines == lanes[...], 1.0, 0.0).T.astype(bf16)
    b0, b1, b2 = pieces(block)
    turned_block = block.T
    high_t, low_t = halves(turned_block)
    both = mm(jnp.concatenate([hot_t, high_t]), jnp.concatenate([b0, b1], axis=1))
    cee = both[:W, :W] + both[:W, W:] + mm(hot_t, b2)
    g00 = both[W:, :W] + both[W:, W:] + mm(low_t, b0)
    parts = out.shape[0]
    bit = W // parts
    for p in range(parts):
        lines = slice(p * bit, (p + 1) * bit)
        out[p, :bit, :] = g00[lines]
        out[p, bit:, :] = cee[lines]


def grams_of_start(place, seeds, start, parts):
    return pl.pallas_call(
        start_grams,
        out_shape=jax.ShapeDtypeStruct((parts, 2 * W // parts, W), f32),
        in_specs=[SMEM, VMEM, VMEM],
        out_specs=VMEM,
        compiler_params=room(16),
    )(place, seeds.reshape(1, W), start)


def cross(a, b):
    right = halves(b)
    high, low = halves(a.T)
    both = mm(high, jnp.concatenate(right, axis=1))
    return both[:, :W] + both[:, W:] + mm(low, right[0])


def step_grams(place, table, mine, out):
    parts = mine.shape[0]
    step = blocks_of(mine, 0, W)
    start = turned_blocks(mine, place, table, W + 2 * W // parts, W, range(parts), place[1])
    out[:W, :] = cross(start, step)
    out[W:, :] = cross(step, step)


def corner():
    return lax.broadcasted_iota(jnp.int32, (W, W), 0), lax.broadcasted_iota(jnp.int32, (W, W), 1)


SPARE = 8


def next_grams(place, table, mine, following, out):
    parts = mine.shape[0]
    bit = W // parts
    step = blocks_of(mine, 0, W)
    then, g01, g11 = (
        turned_blocks(following, place, table, s, n, range(parts), place[1])
        for s, n in ((0, W), (W, bit), (W + bit, bit))
    )
    g12, g22 = cross(step, then), cross(then, then)
    i, j = corner()
    out[:W, :] = g01
    out[W : 2 * W, :] = g11
    out[2 * W : 3 * W, :] = jnp.where(j >= i, g22, g12)
    diagonal = jnp.sum(jnp.where(i == j, g12, 0.0), axis=0, keepdims=True)
    out[3 * W :, :] = jnp.broadcast_to(diagonal, (SPARE, W))


def unpacked(totals):
    total = jnp.sum(totals, axis=0)
    body = total[:W]
    i, j = corner()
    lower = jnp.where(j < i, body, 0.0)
    g12 = lower + lower.T + jnp.where(i == j, total[W : W + 1], 0.0)
    return g12, jnp.where(j >= i, body, 0.0) + jnp.where(j > i, body, 0.0).T


def second_product(place, covariance, mine, theirs, grams, out, small, buffer, sems, total):
    height, breadth = covariance.shape
    half = height // 2
    tall = height // CHUNKS
    copies = chunks_of(covariance, buffer, sems)
    for copy in copies:
        copy.start()
    first = place[1] == 0
    parts = out.shape[0]
    bit = W // parts
    for p in range(parts):
        out[p, W : W + bit, :] = grams[p * bit : (p + 1) * bit, :]
        out[p, W + bit :, :] = grams[W + p * bit : W + (p + 1) * bit, :]
    for i in range(2):
        lines = W + i * bit
        small[i * W : (i + 1) * W, :] = blocks_of(mine, lines, bit) + blocks_of(theirs, lines, bit)
    for i, copy in enumerate(copies):
        lines = slice(i * tall % half // W, (i * tall % half + tall) // W)
        own, other = (mine, theirs) if i * tall < half else (theirs, mine)
        block = jnp.where(first, own[lines, :W, :], other[lines, :W, :]).reshape(tall, W)
        v_high, v_low = halves(block.T)
        copy.wait()
        high, low = halves(buffer[i])
        both = mm(jnp.concatenate([v_high, v_low]), high)
        value = both[:W] + both[W:] + mm(v_high, low)
        if i == 0:
            total[...] = value
        elif i + 1 < CHUNKS:
            total[...] += value
        else:
            value += total[...]
            for p in range(parts):
                out[p, :W, :] = value[:, p * W : (p + 1) * W].T


def image_of_step(place, covariance, mine, theirs, grams):
    breadth = covariance.shape[1]
    parts = breadth // W
    return pl.pallas_call(
        second_product,
        out_shape=[
            jax.ShapeDtypeStruct((parts, W + 2 * (W // parts), W), f32),
            jax.ShapeDtypeStruct((2 * W, W), f32),
        ],
        in_specs=[SMEM, HBM] + [VMEM] * 3,
        out_specs=[VMEM] * 2,
        scratch_shapes=chunk_scratch(covariance) + [pltpu.VMEM((W, breadth), f32)],
        compiler_params=room(50),
    )(place, covariance, mine, theirs, grams)


def basis_rows(place, table, mine, mine_next, theirs, theirs_next, mix, out, stage, sems):
    parts = mine.shape[0]
    bit = 2 * W // parts
    count, tall, _ = stage.shape
    half = count * tall // 2
    high, low = halves(mix[: 2 * W, : 2 * W])
    tip_high, tip_low = halves(mix[:, 2 * W :])
    tip = jnp.concatenate([tip_high, tip_low], axis=1)
    copies = []
    for i in range(count):
        line = i * tall % half
        pair, following, side = (mine, mine_next, place[1]) if i * tall < half else (theirs, theirs_next, 1 - place[1])
        order = range(line // W, (line + tall) // W)
        left = jnp.concatenate(
            [
                turned_blocks(pair, place, table, W + bit, W, order, side),
                pair[line // W : (line + tall) // W, :W, :].reshape(tall, W),
                turned_blocks(following, place, table, 0, W, order, side),
            ],
            axis=1,
        )
        l_high, l_low = halves(left)
        h2, l2 = l_high[:, : 2 * W], l_low[:, : 2 * W]
        stage[i, :, : 2 * W] = mm(h2, high) + mm(h2, low) + mm(l2, high)
        both = mm(l_high, tip)
        stage[i, :, 2 * W :] = both[:, :W] + both[:, W:] + mm(l_low, tip_high)
        rows = pl.ds(pl.multiple_of(side * half + line, tall), tall)
        copies.append(pltpu.make_async_copy(stage.at[i], out.at[rows, :], sems.at[i]))
        copies[-1].start()
    for copy in copies:
        copy.wait()


def basis_of(place, table, mine, mine_next, theirs, theirs_next, mix):
    height = 2 * mine.shape[0] * W
    tall = 256
    breadth = mix.shape[1]
    return pl.pallas_call(
        basis_rows,
        out_shape=jax.ShapeDtypeStruct((height, breadth), f32),
        in_specs=[SMEM] * 2 + [VMEM] * 5,
        out_specs=HBM,
        scratch_shapes=[pltpu.VMEM((height // tall, tall, breadth), f32), pltpu.SemaphoreType.DMA((height // tall,))],
        compiler_params=room(24),
    )(place, table, mine, mine_next, theirs, theirs_next, mix)


def scattered(parts, axis):
    return jnp.sum(lax.all_to_all(parts, axis, 0, 0, tiled=True), axis=0)


def gathered(part, axis):
    copies = jnp.broadcast_to(part, (lax.axis_size(axis), *part.shape))
    return lax.all_to_all(copies, axis, 0, 0, tiled=True)


def other_core(value):
    return lax.ppermute(value, CORE, SWAP)


def turned(rows, chips, cores):
    return [
        ((r * chips + a) * cores + b, (a * chips + SLOTS[b][a][r]) * cores + b)
        for r in range(rows)
        for a in range(chips)
        for b in range(cores)
    ]


def local(covariance, seed_index):
    height, breadth = covariance.shape
    width = seed_index.shape[0]
    rows, chips, cores = (lax.axis_size(a) for a in ALL)
    row, chip, core = (lax.axis_index(a) for a in ALL)
    order = height * rows
    turn = turned(rows, chips, cores)
    table = jnp.array(SLOTS, jnp.int32).reshape(-1)
    place = jnp.stack([row, core, chip * cores + core]).astype(jnp.int32)
    start_piece = scattered(picked_rows(place, seed_index, covariance, rows), ROWS).T
    start_turned = lax.ppermute(start_piece, ALL, turn)
    start = gathered(start_piece, ROWS).reshape(breadth, width)
    start, start_turned = lax.optimization_barrier((start, start_turned))
    keep, send = image_of_start(place, seed_index, covariance, start)
    got = other_core(send)
    small = grams_of_start(place, seed_index, start, chips)
    parts = jnp.concatenate([keep + got, small], axis=1)
    mine = gathered(jnp.concatenate([scattered(parts, CHIP), start_turned]), CHIP)
    theirs = other_core(mine)
    (grams,) = kernel(step_grams, [(2 * width, width)], place, table, mine)
    parts, zero_grams = image_of_step(place, covariance, mine, theirs, grams)
    piece = lax.ppermute(scattered(parts, ROWS), ALL, turn)
    (ready,) = kernel(first_factor, [(4 * width, width)], zero_grams)
    mine_next, ready = lax.optimization_barrier((gathered(piece, CHIP), ready))
    (keep,) = kernel(next_grams, [(3 * width + SPARE, width)], place, table, mine, mine_next)
    got = other_core(keep)
    totals = gathered(keep[2 * width :] + got[2 * width :], ROWS)
    theirs_next = other_core(mine_next)
    stage = [pltpu.VMEM((PACK, width), f32), pltpu.SemaphoreType.DMA((2,))]
    pack = pl.pallas_call(
        middle,
        out_shape=jax.ShapeDtypeStruct((PACK, width), f32),
        in_specs=[VMEM] * 4,
        out_specs=HBM,
        scratch_shapes=stage,
        compiler_params=room(60),
    )(zero_grams, ready, keep, got)
    totals, pack = lax.optimization_barrier((totals, pack))
    scale = float(order) ** 0.5

    def last_step(*refs):
        last(f32(scale), *refs)

    shapes = [(3 * width, 3 * width), (3 * width, 2 * width), (3 * width, 2 * width)]
    mix, projection, first_pass = pl.pallas_call(
        last_step,
        out_shape=[jax.ShapeDtypeStruct(s, f32) for s in shapes],
        in_specs=[HBM, VMEM],
        out_specs=[VMEM] * 3,
        scratch_shapes=stage,
        compiler_params=room(52),
    )(pack, totals)
    basis = basis_of(place, table, mine, mine_next, theirs, theirs_next, mix)
    return basis, projection, first_pass


def solution(mesh):
    rows, cols = mesh.devices.shape
    fine = Mesh(mesh.devices.reshape(rows, cols // 2, 2), ALL)
    return jax.shard_map(
        local,
        mesh=fine,
        in_specs=(P(ROWS, (CHIP, CORE)), P()),
        out_specs=(P(ROWS, None), P(), P()),
        check_vma=False,
    )
```

```python
import jax
import jax.numpy as jnp
from jax import lax
from jax.experimental import pallas as pl
from jax.experimental.pallas import tpu as pltpu
from jax.sharding import Mesh, PartitionSpec as P

ROWS = "row"
CHIP = "chip"
CORE = "core"
ALL = (ROWS, CHIP, CORE)
SWAP = [(0, 1), (1, 0)]
SLOTS = (
    (
        (2, 6, 3, 5, 0, 4, 1, 7),
        (7, 3, 6, 2, 5, 1, 4, 0),
        (3, 5, 0, 4, 1, 7, 2, 6),
        (4, 0, 5, 1, 6, 2, 7, 3),
        (4, 0, 7, 3, 6, 2, 5, 1),
        (1, 5, 2, 6, 3, 7, 0, 4),
        (7, 3, 6, 2, 5, 1, 4, 0),
        (2, 4, 3, 7, 0, 6, 1, 5),
    ),
    (
        (2, 6, 1, 7, 0, 4, 3, 5),
        (7, 3, 4, 0, 5, 1, 6, 2),
        (3, 7, 0, 4, 1, 5, 2, 6),
        (6, 0, 5, 1, 4, 2, 7, 3),
        (4, 0, 7, 1, 6, 2, 5, 3),
        (1, 5, 0, 6, 3, 7, 2, 4),
        (7, 3, 6, 2, 5, 1, 4, 0),
        (2, 4, 3, 7, 0, 6, 1, 5),
    ),
)
W = 128
f32 = jnp.float32
bf16 = jnp.bfloat16
HI = lax.Precision.HIGHEST


def dot(a, b, dims):
    return lax.dot_general(a, b, (dims, ((), ())), precision=HI, preferred_element_type=f32)


def nn(a, b):
    return dot(a, b, ((1,), (0,)))


def tn(a, b):
    return dot(a, b, ((0,), (0,)))


def nt(a, b):
    return dot(a, b, ((1,), (1,)))


def pieces(x):
    a = x.astype(bf16)
    rest = x - a.astype(f32)
    b = rest.astype(bf16)
    return a, b, (rest - b.astype(f32)).astype(bf16)


def outer(left, panel):
    a0, a1, a2 = pieces(left)
    b0, b1, b2 = pieces(panel)
    return lax.dot_general(
        jnp.concatenate([a0, a0, a1, a0, a2, a1]),
        jnp.concatenate([b0, b1, b0, b2, b0, b1]),
        (((0,), (0,)), ((), ())),
        preferred_element_type=f32,
    )


BAND = 16


def factor(gram):
    sub = lax.broadcasted_iota(jnp.int32, (BAND, W), 0)
    lane = lax.broadcasted_iota(jnp.int32, (BAND, W), 1)
    eye = lax.broadcasted_iota(jnp.int32, (W, W), 0) == lax.broadcasted_iota(jnp.int32, (W, W), 1)
    rest = jnp.concatenate([gram, eye.astype(f32)], axis=1)
    now, rest = rest[:BAND], rest[BAND:]
    upper, inverse = [], []
    for base in range(0, W, BAND):
        left, right = now[:, :W], now[:, W:]
        cols = [jnp.broadcast_to(left[:, base + k : base + k + 1], (BAND, W)) for k in range(BAND)]
        scale = jnp.zeros((BAND, W), f32)
        for k in range(0, BAND, 2):
            top = k // 8 * 8
            here = sub[top:]

            def line(x, i):
                return jnp.broadcast_to(x[i : i + 1, :], (BAND - top, W))

            def below(old, new):
                return new if top == 0 else jnp.concatenate([old[:top], new])

            c, d = cols[k][top:], cols[k + 1][top:]
            p, q, r = line(cols[k], k), line(cols[k + 1], k), line(cols[k + 1], k + 1)
            det = p * r - q * q
            inv_p = 1.0 / p
            inv = 1.0 / det
            later = here > k + 1
            u = jnp.where(later, (c * r - d * q) * inv, jnp.where(here == k + 1, q * inv_p, 0.0))
            v = jnp.where(later, (d * p - c * q) * inv, 0.0)
            last_scale = jnp.where(here == k + 1, lax.rsqrt(det * inv_p), scale[top:])
            scale = below(scale, jnp.where(here == k, lax.rsqrt(p), last_scale))

            def update(x):
                return below(x, x[top:] - u * line(x, k) - v * line(x, k + 1))

            for m in range(k + 2, BAND):
                cols[m] = update(cols[m])
            left = update(left)
            right = update(right)
        left = jnp.where(lane >= base + sub, left * scale, 0.0)
        right = right * scale
        upper.append(left)
        inverse.append(right)
        end = base + BAND
        if end < W:
            panel = jnp.concatenate([left, right], axis=1)
            now = rest[:BAND] - outer(left[:, end : end + BAND], panel)
            if end + BAND < W:
                rest = rest[BAND:] - outer(left[:, end + BAND :], panel)
    return jnp.concatenate(upper), jnp.concatenate(inverse)


def blocks_of(ref, start, count):
    return ref[:, start : start + count, :].reshape(ref.shape[0] * count, W)


def turned_blocks(ref, place, table, start, count, parts, core):
    first = (core * ref.shape[0] + place[0]) * ref.shape[0]
    return jnp.concatenate([ref[table[first + p], start : start + count, :] for p in parts])


def first_factor(start, out):
    g00, cee = start[:W, :], start[W:, :]
    li0 = factor(g00)[1]
    u = nt(cee, li0)
    side = nn(li0, g00)
    for i, block in enumerate([li0, u, nn(side, u), nt(side, li0)]):
        out[i * W : (i + 1) * W, :] = block


def middle(start, ready, keep, got, pack, stage, sems):
    g00, cee = start[:W, :], start[W:, :]
    li0, u, h0, m00 = (ready[i * W : (i + 1) * W, :] for i in range(4))
    g01, g11 = (keep[i * W : (i + 1) * W, :] + got[i * W : (i + 1) * W, :] for i in range(2))
    x0 = li0.T
    side = jnp.concatenate([g00, g01], axis=1)
    gram = jnp.concatenate([side, jnp.concatenate([g01.T, g11], axis=1)])
    h = h0 + nt(nn(li0, g01), li0)
    h_full = h + (h - nn(m00, h))
    g02 = g11 + tn(cee, g01)
    for i, block in enumerate([h, h_full, m00, g02, li0]):
        stage[i * W : (i + 1) * W, :] = block
    pack_copy(stage, pack, sems, 0).start()
    comb = jnp.concatenate([u - nn(x0, h_full), x0])
    y = nn(gram, comb)
    upper1, li1 = factor(tn(comb, y))
    c1 = nt(comb, li1)
    y1 = nt(y, li1)
    m01 = nn(li0, y1[:W])
    i1 = jnp.concatenate([nn(cee, c1[:W]), c1])
    s0 = nn(jnp.concatenate([side, g02], axis=1), i1)
    s1 = nn(gram[W:], i1[: 2 * W])
    late = [upper1, i1[:W], i1[W : 2 * W], i1[2 * W :], m01, tn(c1, y1), nn(li0, s0), tn(c1[:W], s0), s1]
    late.append(tn(i1[:W], s0))
    for i, block in enumerate(late):
        stage[EARLY + i * W : EARLY + (i + 1) * W, :] = block
    second = pack_copy(stage, pack, sems, 1)
    second.start()
    pack_copy(stage, pack, sems, 0).wait()
    second.wait()


EARLY = 5 * W
PACK = 15 * W


def pack_copy(source, target, sems, late):
    lines = pl.ds(EARLY, PACK - EARLY) if late else pl.ds(0, EARLY)
    return pltpu.make_async_copy(source.at[lines, :], target.at[lines, :], sems.at[late])


def last(scale, packed, totals, mix, projection, first_pass, pack, sems):
    copies = [pack_copy(packed, pack, sems, i) for i in range(2)]
    for copy in copies:
        copy.start()
    a12, a22 = unpacked(totals[...])
    for copy in copies:
        copy.wait()
    first, full, m00, a02, li0, upper1, _, c1_top, c1_low, m01, m11, first0, part1, s1, square = (
        pack[i * W : (i + 1) * W, :] for i in range(PACK // W)
    )
    i1 = pack[EARLY + W : EARLY + 4 * W, :]
    c1 = i1[W:]
    s1 = s1 + nn(a12, c1_low)
    s2 = nn(jnp.concatenate([a02.T, a12, a22], axis=1), i1)
    square = square + tn(c1, jnp.concatenate([s1, s2]))
    h = jnp.concatenate([first0, part1 + tn(c1_low, s1)])
    gram_p = jnp.concatenate([jnp.concatenate([m00, m01], axis=1), jnp.concatenate([m01.T, m11], axis=1)])
    h_full = h + (h - nn(gram_p, h))
    inner = tn(h, h_full)
    upper2, li2 = factor(square - inner - inner.T + tn(h_full, nn(gram_p, h_full)))
    zero = jnp.zeros((W, W), f32)
    places = jnp.concatenate([jnp.concatenate([li0.T, zero]), c1], axis=1)
    comb = jnp.concatenate([i1[: 2 * W] - nn(places, h_full), i1[2 * W :]])
    mix[: 2 * W, : 2 * W] = places * scale
    mix[2 * W :, : 2 * W] = jnp.zeros((W, 2 * W), f32)
    mix[:, 2 * W :] = nt(comb, li2) * scale
    projection[:W, :W] = full
    projection[W : 2 * W, :W] = upper1
    projection[2 * W :, :W] = zero
    projection[: 2 * W, W:] = h_full
    projection[2 * W :, W:] = upper2
    first_pass[:W, :W] = first
    first_pass[W:, :W] = jnp.zeros((2 * W, W), f32)
    first_pass[: 2 * W, W:] = h
    first_pass[2 * W :, W:] = zero


HBM = pl.BlockSpec(memory_space=pltpu.HBM)
VMEM = pl.BlockSpec(memory_space=pltpu.VMEM)
SMEM = pl.BlockSpec(memory_space=pltpu.SMEM)


def room(mib):
    return pltpu.CompilerParams(vmem_limit_bytes=mib * 2**20)


def kernel(body, shapes, *args):
    return pl.pallas_call(
        body,
        out_shape=[jax.ShapeDtypeStruct(s, f32) for s in shapes],
        in_specs=[VMEM if a.dtype == f32 else SMEM for a in args],
        out_specs=[VMEM] * len(shapes),
        compiler_params=room(16),
    )(*args)


def halves(x):
    high = x.astype(bf16)
    return high, (x - high.astype(f32)).astype(bf16)


def mm(a, b):
    return lax.dot_general(a, b, (((1,), (0,)), ((), ())), preferred_element_type=f32)


def pick_rows(place, seeds, lanes, covariance, out, buffer, sem):
    count = seeds.shape[0]
    height = covariance.shape[0]
    base = place[0] * height

    def row(line, i):
        return pltpu.make_async_copy(covariance.at[pl.ds(line, 1), :], buffer.at[pl.ds(i, 1), :], sem)

    def body(i, found):
        line = seeds[i] - base
        here = (line >= 0) & (line < height)

        @pl.when(here)
        def _():
            row(line, i).start()

        return found + here.astype(jnp.int32)

    found = lax.fori_loop(0, count, body, 0, unroll=8)
    offsets = jnp.broadcast_to(lanes[...] - base, (count, count))
    held = jnp.where((offsets >= 0) & (offsets < height), 1.0, 0.0).T > 0

    def done(i, carry):
        row(0, 0).wait()
        return carry

    lax.fori_loop(0, found, done, 0)
    for p in range(out.shape[0]):
        out[p] = jnp.where(held, buffer[:, p * W : (p + 1) * W], 0.0)


def picked_rows(place, seeds, covariance, parts):
    count = seeds.shape[0]
    return pl.pallas_call(
        pick_rows,
        out_shape=jax.ShapeDtypeStruct((parts, count, W), f32),
        in_specs=[SMEM, SMEM, VMEM, HBM],
        out_specs=VMEM,
        scratch_shapes=[pltpu.VMEM((count, covariance.shape[1]), f32), pltpu.SemaphoreType.DMA],
        compiler_params=room(50),
    )(place, seeds, seeds.reshape(1, count), covariance)


CHUNKS = 8


def chunks_of(covariance, buffer, sems):
    tall = covariance.shape[0] // CHUNKS
    return [
        pltpu.make_async_copy(covariance.at[pl.ds(i * tall, tall), :], buffer.at[i], sems.at[i]) for i in range(CHUNKS)
    ]


def chunk_scratch(covariance):
    height, breadth = covariance.shape
    return [pltpu.VMEM((CHUNKS, height // CHUNKS, breadth), f32), pltpu.SemaphoreType.DMA((CHUNKS,))]


def first_product(place, lanes, covariance, start, keep, send, buffer, sems):
    height, breadth = covariance.shape
    half = height // 2
    tall = height // CHUNKS
    copies = chunks_of(covariance, buffer, sems)
    for copy in copies:
        copy.start()
    lines = lax.broadcasted_iota(jnp.int32, (breadth, W), 0) + place[2] * breadth
    hot = jnp.where(lines == lanes[...], 1.0, 0.0)
    hit = jnp.max(hot, axis=1, keepdims=True) > 0
    weights = jnp.concatenate(halves(jnp.where(hit, 0.0, start[...])), axis=1)
    first = place[1] == 0
    for i, copy in enumerate(copies):
        copy.wait()
        high, low = halves(buffer[i])
        both = mm(high, weights)
        value = both[:, :W] + both[:, W:] + mm(low, weights[:, :W])
        mine = first if i * tall < half else jnp.logical_not(first)

        def store(out):
            for q in range(tall // W):
                out[i * tall % half // W + q] = value[q * W : (q + 1) * W, :]

        @pl.when(mine)
        def _():
            store(keep)

        @pl.when(jnp.logical_not(mine))
        def _():
            store(send)


def image_of_start(place, seeds, covariance, start):
    height = covariance.shape[0]
    shape = jax.ShapeDtypeStruct((height // 2 // W, W, W), f32)
    return pl.pallas_call(
        first_product,
        out_shape=[shape, shape],
        in_specs=[SMEM, VMEM, HBM, VMEM],
        out_specs=[VMEM] * 2,
        scratch_shapes=chunk_scratch(covariance),
        compiler_params=room(50),
    )(place, seeds.reshape(1, W), covariance, start)


def start_grams(place, lanes, start, out):
    block = start[...]
    lines = lax.broadcasted_iota(jnp.int32, block.shape, 0) + place[2] * block.shape[0]
    hot_t = jnp.where(lines == lanes[...], 1.0, 0.0).T.astype(bf16)
    b0, b1, b2 = pieces(block)
    turned_block = block.T
    high_t, low_t = halves(turned_block)
    both = mm(jnp.concatenate([hot_t, high_t]), jnp.concatenate([b0, b1], axis=1))
    cee = both[:W, :W] + both[:W, W:] + mm(hot_t, b2)
    g00 = both[W:, :W] + both[W:, W:] + mm(low_t, b0)
    parts = out.shape[0]
    bit = W // parts
    for p in range(parts):
        lines = slice(p * bit, (p + 1) * bit)
        out[p, :bit, :] = g00[lines]
        out[p, bit:, :] = cee[lines]


def grams_of_start(place, seeds, start, parts):
    return pl.pallas_call(
        start_grams,
        out_shape=jax.ShapeDtypeStruct((parts, 2 * W // parts, W), f32),
        in_specs=[SMEM, VMEM, VMEM],
        out_specs=VMEM,
        compiler_params=room(16),
    )(place, seeds.reshape(1, W), start)


def cross(a, b):
    right = halves(b)
    high, low = halves(a.T)
    both = mm(high, jnp.concatenate(right, axis=1))
    return both[:, :W] + both[:, W:] + mm(low, right[0])


def step_grams(place, table, mine, out):
    parts = mine.shape[0]
    step = blocks_of(mine, 0, W)
    start = turned_blocks(mine, place, table, W + 2 * W // parts, W, range(parts), place[1])
    out[:W, :] = cross(start, step)
    out[W:, :] = cross(step, step)


def corner():
    return lax.broadcasted_iota(jnp.int32, (W, W), 0), lax.broadcasted_iota(jnp.int32, (W, W), 1)


SPARE = 8


def next_grams(place, table, mine, following, out):
    parts = mine.shape[0]
    bit = W // parts
    step = blocks_of(mine, 0, W)
    then, g01, g11 = (
        turned_blocks(following, place, table, s, n, range(parts), place[1])
        for s, n in ((0, W), (W, bit), (W + bit, bit))
    )
    g12, g22 = cross(step, then), cross(then, then)
    i, j = corner()
    out[:W, :] = g01
    out[W : 2 * W, :] = g11
    out[2 * W : 3 * W, :] = jnp.where(j >= i, g22, g12)
    diagonal = jnp.sum(jnp.where(i == j, g12, 0.0), axis=0, keepdims=True)
    out[3 * W :, :] = jnp.broadcast_to(diagonal, (SPARE, W))


def unpacked(totals):
    total = jnp.sum(totals, axis=0)
    body = total[:W]
    i, j = corner()
    lower = jnp.where(j < i, body, 0.0)
    g12 = lower + lower.T + jnp.where(i == j, total[W : W + 1], 0.0)
    return g12, jnp.where(j >= i, body, 0.0) + jnp.where(j > i, body, 0.0).T


def second_product(place, covariance, mine, theirs, grams, out, small, buffer, sems, total):
    height, breadth = covariance.shape
    half = height // 2
    tall = height // CHUNKS
    copies = chunks_of(covariance, buffer, sems)
    for copy in copies:
        copy.start()
    first = place[1] == 0
    parts = out.shape[0]
    bit = W // parts
    for p in range(parts):
        out[p, W : W + bit, :] = grams[p * bit : (p + 1) * bit, :]
        out[p, W + bit :, :] = grams[W + p * bit : W + (p + 1) * bit, :]
    for i in range(2):
        lines = W + i * bit
        small[i * W : (i + 1) * W, :] = blocks_of(mine, lines, bit) + blocks_of(theirs, lines, bit)
    for i, copy in enumerate(copies):
        lines = slice(i * tall % half // W, (i * tall % half + tall) // W)
        own, other = (mine, theirs) if i * tall < half else (theirs, mine)
        block = jnp.where(first, own[lines, :W, :], other[lines, :W, :]).reshape(tall, W)
        v_high, v_low = halves(block.T)
        copy.wait()
        high, low = halves(buffer[i])
        both = mm(jnp.concatenate([v_high, v_low]), high)
        value = both[:W] + both[W:] + mm(v_high, low)
        if i == 0:
            total[...] = value
        elif i + 1 < CHUNKS:
            total[...] += value
        else:
            value += total[...]
            for p in range(parts):
                out[p, :W, :] = value[:, p * W : (p + 1) * W].T


def image_of_step(place, covariance, mine, theirs, grams):
    breadth = covariance.shape[1]
    parts = breadth // W
    return pl.pallas_call(
        second_product,
        out_shape=[
            jax.ShapeDtypeStruct((parts, W + 2 * (W // parts), W), f32),
            jax.ShapeDtypeStruct((2 * W, W), f32),
        ],
        in_specs=[SMEM, HBM] + [VMEM] * 3,
        out_specs=[VMEM] * 2,
        scratch_shapes=chunk_scratch(covariance) + [pltpu.VMEM((W, breadth), f32)],
        compiler_params=room(50),
    )(place, covariance, mine, theirs, grams)


def basis_rows(place, table, mine, mine_next, theirs, theirs_next, mix, out, stage, sems):
    parts = mine.shape[0]
    bit = 2 * W // parts
    count, tall, _ = stage.shape
    half = count * tall // 2
    high, low = halves(mix[: 2 * W, : 2 * W])
    tip_high, tip_low = halves(mix[:, 2 * W :])
    tip = jnp.concatenate([tip_high, tip_low], axis=1)
    copies = []
    for i in range(count):
        line = i * tall % half
        pair, following, side = (mine, mine_next, place[1]) if i * tall < half else (theirs, theirs_next, 1 - place[1])
        order = range(line // W, (line + tall) // W)
        left = jnp.concatenate(
            [
                turned_blocks(pair, place, table, W + bit, W, order, side),
                pair[line // W : (line + tall) // W, :W, :].reshape(tall, W),
                turned_blocks(following, place, table, 0, W, order, side),
            ],
            axis=1,
        )
        l_high, l_low = halves(left)
        h2, l2 = l_high[:, : 2 * W], l_low[:, : 2 * W]
        stage[i, :, : 2 * W] = mm(h2, high) + mm(h2, low) + mm(l2, high)
        both = mm(l_high, tip)
        stage[i, :, 2 * W :] = both[:, :W] + both[:, W:] + mm(l_low, tip_high)
        rows = pl.ds(pl.multiple_of(side * half + line, tall), tall)
        copies.append(pltpu.make_async_copy(stage.at[i], out.at[rows, :], sems.at[i]))
        copies[-1].start()
    for copy in copies:
        copy.wait()


def basis_of(place, table, mine, mine_next, theirs, theirs_next, mix):
    height = 2 * mine.shape[0] * W
    tall = 256
    breadth = mix.shape[1]
    return pl.pallas_call(
        basis_rows,
        out_shape=jax.ShapeDtypeStruct((height, breadth), f32),
        in_specs=[SMEM] * 2 + [VMEM] * 5,
        out_specs=HBM,
        scratch_shapes=[pltpu.VMEM((height // tall, tall, breadth), f32), pltpu.SemaphoreType.DMA((height // tall,))],
        compiler_params=room(24),
    )(place, table, mine, mine_next, theirs, theirs_next, mix)


def scattered(parts, axis):
    return jnp.sum(lax.all_to_all(parts, axis, 0, 0, tiled=True), axis=0)


def gathered(part, axis):
    copies = jnp.broadcast_to(part, (lax.axis_size(axis), *part.shape))
    return lax.all_to_all(copies, axis, 0, 0, tiled=True)


def other_core(value):
    return lax.ppermute(value, CORE, SWAP)


def turned(rows, chips, cores):
    return [
        ((r * chips + a) * cores + b, (a * chips + SLOTS[b][a][r]) * cores + b)
        for r in range(rows)
        for a in range(chips)
        for b in range(cores)
    ]


def local(covariance, seed_index):
    height, breadth = covariance.shape
    width = seed_index.shape[0]
    rows, chips, cores = (lax.axis_size(a) for a in ALL)
    row, chip, core = (lax.axis_index(a) for a in ALL)
    order = height * rows
    turn = turned(rows, chips, cores)
    table = jnp.array(SLOTS, jnp.int32).reshape(-1)
    place = jnp.stack([row, core, chip * cores + core]).astype(jnp.int32)
    start_piece = scattered(picked_rows(place, seed_index, covariance, rows), ROWS).T
    start_turned = lax.ppermute(start_piece, ALL, turn)
    start = gathered(start_piece, ROWS).reshape(breadth, width)
    start, start_turned = lax.optimization_barrier((start, start_turned))
    keep, send = image_of_start(place, seed_index, covariance, start)
    got = other_core(send)
    small = grams_of_start(place, seed_index, start, chips)
    parts = jnp.concatenate([keep + got, small], axis=1)
    mine = gathered(jnp.concatenate([scattered(parts, CHIP), start_turned]), CHIP)
    theirs = other_core(mine)
    (grams,) = kernel(step_grams, [(2 * width, width)], place, table, mine)
    parts, zero_grams = image_of_step(place, covariance, mine, theirs, grams)
    piece = lax.ppermute(scattered(parts, ROWS), ALL, turn)
    (ready,) = kernel(first_factor, [(4 * width, width)], zero_grams)
    mine_next, ready = lax.optimization_barrier((gathered(piece, CHIP), ready))
    (keep,) = kernel(next_grams, [(3 * width + SPARE, width)], place, table, mine, mine_next)
    got = other_core(keep)
    totals = gathered(keep[2 * width :] + got[2 * width :], ROWS)
    theirs_next = other_core(mine_next)
    stage = [pltpu.VMEM((PACK, width), f32), pltpu.SemaphoreType.DMA((2,))]
    pack = pl.pallas_call(
        middle,
        out_shape=jax.ShapeDtypeStruct((PACK, width), f32),
        in_specs=[VMEM] * 4,
        out_specs=HBM,
        scratch_shapes=stage,
        compiler_params=room(60),
    )(zero_grams, ready, keep, got)
    totals, pack = lax.optimization_barrier((totals, pack))
    scale = float(order) ** 0.5

    def last_step(*refs):
        last(f32(scale), *refs)

    shapes = [(3 * width, 3 * width), (3 * width, 2 * width), (3 * width, 2 * width)]
    mix, projection, first_pass = pl.pallas_call(
        last_step,
        out_shape=[jax.ShapeDtypeStruct(s, f32) for s in shapes],
        in_specs=[HBM, VMEM],
        out_specs=[VMEM] * 3,
        scratch_shapes=stage,
        compiler_params=room(52),
    )(pack, totals)
    basis = basis_of(place, table, mine, mine_next, theirs, theirs_next, mix)
    return basis, projection, first_pass


def solution(mesh):
    rows, cols = mesh.devices.shape
    fine = Mesh(mesh.devices.reshape(rows, cols // 2, 2), ALL)
    return jax.shard_map(
        local,
        mesh=fine,
        in_specs=(P(ROWS, (CHIP, CORE)), P()),
        out_specs=(P(ROWS, None), P(), P()),
        check_vma=False,
    )
```

```python
import jax
import jax.numpy as jnp
from jax import lax
from jax.experimental import pallas as pl
from jax.experimental.pallas import tpu as pltpu
from jax.sharding import Mesh, PartitionSpec as P

ROWS = "row"
CHIP = "chip"
CORE = "core"
ALL = (ROWS, CHIP, CORE)
SWAP = [(0, 1), (1, 0)]
SLOTS = (
    (
        (2, 6, 3, 5, 0, 4, 1, 7),
        (7, 3, 6, 2, 5, 1, 4, 0),
        (3, 5, 0, 4, 1, 7, 2, 6),
        (4, 0, 5, 1, 6, 2, 7, 3),
        (4, 0, 7, 3, 6, 2, 5, 1),
        (1, 5, 2, 6, 3, 7, 0, 4),
        (7, 3, 6, 2, 5, 1, 4, 0),
        (2, 4, 3, 7, 0, 6, 1, 5),
    ),
    (
        (2, 6, 1, 7, 0, 4, 3, 5),
        (7, 3, 4, 0, 5, 1, 6, 2),
        (3, 7, 0, 4, 1, 5, 2, 6),
        (6, 0, 5, 1, 4, 2, 7, 3),
        (4, 0, 7, 1, 6, 2, 5, 3),
        (1, 5, 0, 6, 3, 7, 2, 4),
        (7, 3, 6, 2, 5, 1, 4, 0),
        (2, 4, 3, 7, 0, 6, 1, 5),
    ),
)
W = 128
f32 = jnp.float32
bf16 = jnp.bfloat16
HI = lax.Precision.HIGHEST


def dot(a, b, dims):
    return lax.dot_general(a, b, (dims, ((), ())), precision=HI, preferred_element_type=f32)


def nn(a, b):
    return dot(a, b, ((1,), (0,)))


def tn(a, b):
    return dot(a, b, ((0,), (0,)))


def nt(a, b):
    return dot(a, b, ((1,), (1,)))


def pieces(x):
    a = x.astype(bf16)
    rest = x - a.astype(f32)
    b = rest.astype(bf16)
    return a, b, (rest - b.astype(f32)).astype(bf16)


def outer(left, panel):
    a0, a1, a2 = pieces(left)
    b0, b1, b2 = pieces(panel)
    return lax.dot_general(
        jnp.concatenate([a0, a0, a1, a0, a2, a1]),
        jnp.concatenate([b0, b1, b0, b2, b0, b1]),
        (((0,), (0,)), ((), ())),
        preferred_element_type=f32,
    )


BAND = 16


def factor(gram):
    sub = lax.broadcasted_iota(jnp.int32, (BAND, W), 0)
    lane = lax.broadcasted_iota(jnp.int32, (BAND, W), 1)
    eye = lax.broadcasted_iota(jnp.int32, (W, W), 0) == lax.broadcasted_iota(jnp.int32, (W, W), 1)
    rest = jnp.concatenate([gram, eye.astype(f32)], axis=1)
    now, rest = rest[:BAND], rest[BAND:]
    upper, inverse = [], []
    for base in range(0, W, BAND):
        left, right = now[:, :W], now[:, W:]
        cols = [jnp.broadcast_to(left[:, base + k : base + k + 1], (BAND, W)) for k in range(BAND)]
        scale = jnp.zeros((BAND, W), f32)
        for k in range(0, BAND, 2):
            top = k // 8 * 8
            here = sub[top:]

            def line(x, i):
                return jnp.broadcast_to(x[i : i + 1, :], (BAND - top, W))

            def below(old, new):
                return new if top == 0 else jnp.concatenate([old[:top], new])

            c, d = cols[k][top:], cols[k + 1][top:]
            p, q, r = line(cols[k], k), line(cols[k + 1], k), line(cols[k + 1], k + 1)
            det = p * r - q * q
            inv_p = 1.0 / p
            inv = 1.0 / det
            later = here > k + 1
            u = jnp.where(later, (c * r - d * q) * inv, jnp.where(here == k + 1, q * inv_p, 0.0))
            v = jnp.where(later, (d * p - c * q) * inv, 0.0)
            last_scale = jnp.where(here == k + 1, lax.rsqrt(det * inv_p), scale[top:])
            scale = below(scale, jnp.where(here == k, lax.rsqrt(p), last_scale))

            def update(x):
                return below(x, x[top:] - u * line(x, k) - v * line(x, k + 1))

            for m in range(k + 2, BAND):
                cols[m] = update(cols[m])
            left = update(left)
            right = update(right)
        left = jnp.where(lane >= base + sub, left * scale, 0.0)
        right = right * scale
        upper.append(left)
        inverse.append(right)
        end = base + BAND
        if end < W:
            panel = jnp.concatenate([left, right], axis=1)
            now = rest[:BAND] - outer(left[:, end : end + BAND], panel)
            if end + BAND < W:
                rest = rest[BAND:] - outer(left[:, end + BAND :], panel)
    return jnp.concatenate(upper), jnp.concatenate(inverse)


def blocks_of(ref, start, count):
    return ref[:, start : start + count, :].reshape(ref.shape[0] * count, W)


def turned_blocks(ref, place, table, start, count, parts, core):
    first = (core * ref.shape[0] + place[0]) * ref.shape[0]
    return jnp.concatenate([ref[table[first + p], start : start + count, :] for p in parts])


def first_factor(start, out):
    g00, cee = start[:W, :], start[W:, :]
    li0 = factor(g00)[1]
    u = nt(cee, li0)
    side = nn(li0, g00)
    for i, block in enumerate([li0, u, nn(side, u), nt(side, li0)]):
        out[i * W : (i + 1) * W, :] = block


def middle(start, ready, keep, got, pack, stage, sems):
    g00, cee = start[:W, :], start[W:, :]
    li0, u, h0, m00 = (ready[i * W : (i + 1) * W, :] for i in range(4))
    g01, g11 = (keep[i * W : (i + 1) * W, :] + got[i * W : (i + 1) * W, :] for i in range(2))
    x0 = li0.T
    side = jnp.concatenate([g00, g01], axis=1)
    gram = jnp.concatenate([side, jnp.concatenate([g01.T, g11], axis=1)])
    h = h0 + nt(nn(li0, g01), li0)
    h_full = h + (h - nn(m00, h))
    g02 = g11 + tn(cee, g01)
    for i, block in enumerate([h, h_full, m00, g02, li0]):
        stage[i * W : (i + 1) * W, :] = block
    pack_copy(stage, pack, sems, 0).start()
    comb = jnp.concatenate([u - nn(x0, h_full), x0])
    y = nn(gram, comb)
    upper1, li1 = factor(tn(comb, y))
    scaled = nt(jnp.concatenate([comb, y]), li1)
    c1, y1 = scaled[: 2 * W], scaled[2 * W :]
    m01 = nn(li0, y1[:W])
    i1 = jnp.concatenate([nn(cee, c1[:W]), c1])
    s0 = nn(jnp.concatenate([side, g02], axis=1), i1)
    s1 = nn(gram[W:], i1[: 2 * W])
    crossed = nn(jnp.concatenate([li0, c1[:W].T, i1[:W].T]), s0)
    late = [upper1, i1[:W], i1[W : 2 * W], i1[2 * W :], m01, tn(c1, y1), crossed[:W], crossed[W : 2 * W], s1]
    late.append(crossed[2 * W :])
    for i, block in enumerate(late):
        stage[EARLY + i * W : EARLY + (i + 1) * W, :] = block
    second = pack_copy(stage, pack, sems, 1)
    second.start()
    pack_copy(stage, pack, sems, 0).wait()
    second.wait()


EARLY = 5 * W
PACK = 15 * W


def pack_copy(source, target, sems, late):
    lines = pl.ds(EARLY, PACK - EARLY) if late else pl.ds(0, EARLY)
    return pltpu.make_async_copy(source.at[lines, :], target.at[lines, :], sems.at[late])


def last(scale, packed, totals, mix, projection, first_pass, pack, sems, parts, total_sem):
    copies = [pack_copy(packed, pack, sems, i) for i in range(2)]
    summands = pltpu.make_async_copy(totals, parts, total_sem)
    summands.start()
    for copy in copies:
        copy.start()
    summands.wait()
    a12, a22 = unpacked(parts[...])
    for copy in copies:
        copy.wait()
    first, full, m00, a02, li0, upper1, _, c1_top, c1_low, m01, m11, first0, part1, s1, square = (
        pack[i * W : (i + 1) * W, :] for i in range(PACK // W)
    )
    i1 = pack[EARLY + W : EARLY + 4 * W, :]
    c1 = i1[W:]
    s1 = s1 + nn(a12, c1_low)
    s2 = nn(jnp.concatenate([a02.T, a12, a22], axis=1), i1)
    square = square + tn(c1, jnp.concatenate([s1, s2]))
    h = jnp.concatenate([first0, part1 + tn(c1_low, s1)])
    gram_p = jnp.concatenate([jnp.concatenate([m00, m01], axis=1), jnp.concatenate([m01.T, m11], axis=1)])
    h_full = h + (h - nn(gram_p, h))
    inner = tn(h, h_full)
    upper2, li2 = factor(square - inner - inner.T + tn(h_full, nn(gram_p, h_full)))
    zero = jnp.zeros((W, W), f32)
    places = jnp.concatenate([jnp.concatenate([li0.T, zero]), c1], axis=1)
    comb = jnp.concatenate([i1[: 2 * W] - nn(places, h_full), i1[2 * W :]])
    mix[: 2 * W, : 2 * W] = places * scale
    mix[2 * W :, : 2 * W] = jnp.zeros((W, 2 * W), f32)
    mix[:, 2 * W :] = nt(comb, li2) * scale
    projection[:W, :W] = full
    projection[W : 2 * W, :W] = upper1
    projection[2 * W :, :W] = zero
    projection[: 2 * W, W:] = h_full
    projection[2 * W :, W:] = upper2
    first_pass[:W, :W] = first
    first_pass[W:, :W] = jnp.zeros((2 * W, W), f32)
    first_pass[: 2 * W, W:] = h
    first_pass[2 * W :, W:] = zero


HBM = pl.BlockSpec(memory_space=pltpu.HBM)
VMEM = pl.BlockSpec(memory_space=pltpu.VMEM)
SMEM = pl.BlockSpec(memory_space=pltpu.SMEM)


def room(mib):
    return pltpu.CompilerParams(vmem_limit_bytes=mib * 2**20)


def kernel(body, shapes, *args):
    return pl.pallas_call(
        body,
        out_shape=[jax.ShapeDtypeStruct(s, f32) for s in shapes],
        in_specs=[VMEM if a.dtype == f32 else SMEM for a in args],
        out_specs=[VMEM] * len(shapes),
        compiler_params=room(16),
    )(*args)


def halves(x):
    high = x.astype(bf16)
    return high, (x - high.astype(f32)).astype(bf16)


def mm(a, b):
    return lax.dot_general(a, b, (((1,), (0,)), ((), ())), preferred_element_type=f32)


def pick_rows(place, seeds, lanes, covariance, out, buffer, sem):
    count = seeds.shape[0]
    height = covariance.shape[0]
    base = place[0] * height

    def row(line, i):
        return pltpu.make_async_copy(covariance.at[pl.ds(line, 1), :], buffer.at[pl.ds(i, 1), :], sem)

    def body(i, found):
        line = seeds[i] - base
        here = (line >= 0) & (line < height)

        @pl.when(here)
        def _():
            row(line, i).start()

        return found + here.astype(jnp.int32)

    found = lax.fori_loop(0, count, body, 0, unroll=8)
    offsets = jnp.broadcast_to(lanes[...] - base, (count, count))
    held = jnp.where((offsets >= 0) & (offsets < height), 1.0, 0.0).T > 0

    def done(i, carry):
        row(0, 0).wait()
        return carry

    lax.fori_loop(0, found, done, 0)
    for p in range(out.shape[0]):
        out[p] = jnp.where(held, buffer[:, p * W : (p + 1) * W], 0.0)


def picked_rows(place, seeds, covariance, parts):
    count = seeds.shape[0]
    return pl.pallas_call(
        pick_rows,
        out_shape=jax.ShapeDtypeStruct((parts, count, W), f32),
        in_specs=[SMEM, SMEM, VMEM, HBM],
        out_specs=VMEM,
        scratch_shapes=[pltpu.VMEM((count, covariance.shape[1]), f32), pltpu.SemaphoreType.DMA],
        compiler_params=room(50),
    )(place, seeds, seeds.reshape(1, count), covariance)


CHUNKS = 8


def chunks_of(covariance, buffer, sems):
    tall = covariance.shape[0] // CHUNKS
    return [
        pltpu.make_async_copy(covariance.at[pl.ds(i * tall, tall), :], buffer.at[i], sems.at[i]) for i in range(CHUNKS)
    ]


def chunk_scratch(covariance):
    height, breadth = covariance.shape
    return [pltpu.VMEM((CHUNKS, height // CHUNKS, breadth), f32), pltpu.SemaphoreType.DMA((CHUNKS,))]


def first_product(place, lanes, covariance, start, keep, send, buffer, sems):
    height, breadth = covariance.shape
    half = height // 2
    tall = height // CHUNKS
    copies = chunks_of(covariance, buffer, sems)
    for copy in copies:
        copy.start()
    lines = lax.broadcasted_iota(jnp.int32, (breadth, W), 0) + place[2] * breadth
    hot = jnp.where(lines == lanes[...], 1.0, 0.0)
    hit = jnp.max(hot, axis=1, keepdims=True) > 0
    weights = jnp.concatenate(halves(jnp.where(hit, 0.0, start[...])), axis=1)
    first = place[1] == 0
    for i, copy in enumerate(copies):
        copy.wait()
        high, low = halves(buffer[i])
        both = mm(high, weights)
        value = both[:, :W] + both[:, W:] + mm(low, weights[:, :W])
        mine = first if i * tall < half else jnp.logical_not(first)

        def store(out):
            for q in range(tall // W):
                out[i * tall % half // W + q] = value[q * W : (q + 1) * W, :]

        @pl.when(mine)
        def _():
            store(keep)

        @pl.when(jnp.logical_not(mine))
        def _():
            store(send)


def image_of_start(place, seeds, covariance, start):
    height = covariance.shape[0]
    shape = jax.ShapeDtypeStruct((height // 2 // W, W, W), f32)
    return pl.pallas_call(
        first_product,
        out_shape=[shape, shape],
        in_specs=[SMEM, VMEM, HBM, VMEM],
        out_specs=[VMEM] * 2,
        scratch_shapes=chunk_scratch(covariance),
        compiler_params=room(50),
    )(place, seeds.reshape(1, W), covariance, start)


def start_grams(place, lanes, start, out):
    block = start[...]
    lines = lax.broadcasted_iota(jnp.int32, block.shape, 0) + place[2] * block.shape[0]
    hot_t = jnp.where(lines == lanes[...], 1.0, 0.0).T.astype(bf16)
    b0, b1, b2 = pieces(block)
    turned_block = block.T
    high_t, low_t = halves(turned_block)
    both = mm(jnp.concatenate([hot_t, high_t]), jnp.concatenate([b0, b1], axis=1))
    cee = both[:W, :W] + both[:W, W:] + mm(hot_t, b2)
    g00 = both[W:, :W] + both[W:, W:] + mm(low_t, b0)
    parts = out.shape[0]
    bit = W // parts
    for p in range(parts):
        lines = slice(p * bit, (p + 1) * bit)
        out[p, :bit, :] = g00[lines]
        out[p, bit:, :] = cee[lines]


def grams_of_start(place, seeds, start, parts):
    return pl.pallas_call(
        start_grams,
        out_shape=jax.ShapeDtypeStruct((parts, 2 * W // parts, W), f32),
        in_specs=[SMEM, VMEM, VMEM],
        out_specs=VMEM,
        compiler_params=room(16),
    )(place, seeds.reshape(1, W), start)


def cross(a, b):
    right = halves(b)
    high, low = halves(a.T)
    both = mm(high, jnp.concatenate(right, axis=1))
    return both[:, :W] + both[:, W:] + mm(low, right[0])


def step_grams(place, table, mine, out):
    parts = mine.shape[0]
    step = blocks_of(mine, 0, W)
    start = turned_blocks(mine, place, table, W + 2 * W // parts, W, range(parts), place[1])
    out[:W, :] = cross(start, step)
    out[W:, :] = cross(step, step)


def corner():
    return lax.broadcasted_iota(jnp.int32, (W, W), 0), lax.broadcasted_iota(jnp.int32, (W, W), 1)


SPARE = 8


def next_grams(place, table, mine, following, out):
    parts = mine.shape[0]
    bit = W // parts
    step = blocks_of(mine, 0, W)
    then, g01, g11 = (
        turned_blocks(following, place, table, s, n, range(parts), place[1])
        for s, n in ((0, W), (W, bit), (W + bit, bit))
    )
    g12, g22 = cross(step, then), cross(then, then)
    i, j = corner()
    out[:W, :] = g01
    out[W : 2 * W, :] = g11
    out[2 * W : 3 * W, :] = jnp.where(j >= i, g22, g12)
    diagonal = jnp.sum(jnp.where(i == j, g12, 0.0), axis=0, keepdims=True)
    out[3 * W :, :] = jnp.broadcast_to(diagonal, (SPARE, W))


def unpacked(totals):
    total = jnp.sum(totals, axis=0)
    body = total[:W]
    i, j = corner()
    lower = jnp.where(j < i, body, 0.0)
    g12 = lower + lower.T + jnp.where(i == j, total[W : W + 1], 0.0)
    return g12, jnp.where(j >= i, body, 0.0) + jnp.where(j > i, body, 0.0).T


def second_product(place, covariance, mine, theirs, grams, out, small, buffer, sems, total):
    height, breadth = covariance.shape
    half = height // 2
    tall = height // CHUNKS
    copies = chunks_of(covariance, buffer, sems)
    for copy in copies:
        copy.start()
    first = place[1] == 0
    parts = out.shape[0]
    bit = W // parts
    for p in range(parts):
        out[p, W : W + bit, :] = grams[p * bit : (p + 1) * bit, :]
        out[p, W + bit :, :] = grams[W + p * bit : W + (p + 1) * bit, :]
    for i in range(2):
        lines = W + i * bit
        small[i * W : (i + 1) * W, :] = blocks_of(mine, lines, bit) + blocks_of(theirs, lines, bit)
    for i, copy in enumerate(copies):
        lines = slice(i * tall % half // W, (i * tall % half + tall) // W)
        own, other = (mine, theirs) if i * tall < half else (theirs, mine)
        block = jnp.where(first, own[lines, :W, :], other[lines, :W, :]).reshape(tall, W)
        v_high, v_low = halves(block.T)
        copy.wait()
        high, low = halves(buffer[i])
        both = mm(jnp.concatenate([v_high, v_low]), high)
        value = both[:W] + both[W:] + mm(v_high, low)
        if i == 0:
            total[...] = value
        elif i + 1 < CHUNKS:
            total[...] += value
        else:
            value += total[...]
            for p in range(parts):
                out[p, :W, :] = value[:, p * W : (p + 1) * W].T


def image_of_step(place, covariance, mine, theirs, grams):
    breadth = covariance.shape[1]
    parts = breadth // W
    return pl.pallas_call(
        second_product,
        out_shape=[
            jax.ShapeDtypeStruct((parts, W + 2 * (W // parts), W), f32),
            jax.ShapeDtypeStruct((2 * W, W), f32),
        ],
        in_specs=[SMEM, HBM] + [VMEM] * 3,
        out_specs=[VMEM] * 2,
        scratch_shapes=chunk_scratch(covariance) + [pltpu.VMEM((W, breadth), f32)],
        compiler_params=room(50),
    )(place, covariance, mine, theirs, grams)


def basis_rows(place, table, mine, mine_next, theirs, theirs_next, mix, out, stage, sems):
    parts = mine.shape[0]
    bit = 2 * W // parts
    count, tall, _ = stage.shape
    half = count * tall // 2
    high, low = halves(mix[: 2 * W, : 2 * W])
    tip_high, tip_low = halves(mix[:, 2 * W :])
    tip = jnp.concatenate([tip_high, tip_low], axis=1)
    copies = []
    for i in range(count):
        line = i * tall % half
        pair, following, side = (mine, mine_next, place[1]) if i * tall < half else (theirs, theirs_next, 1 - place[1])
        order = range(line // W, (line + tall) // W)
        left = jnp.concatenate(
            [
                turned_blocks(pair, place, table, W + bit, W, order, side),
                pair[line // W : (line + tall) // W, :W, :].reshape(tall, W),
                turned_blocks(following, place, table, 0, W, order, side),
            ],
            axis=1,
        )
        l_high, l_low = halves(left)
        h2, l2 = l_high[:, : 2 * W], l_low[:, : 2 * W]
        stage[i, :, : 2 * W] = mm(h2, high) + mm(h2, low) + mm(l2, high)
        both = mm(l_high, tip)
        stage[i, :, 2 * W :] = both[:, :W] + both[:, W:] + mm(l_low, tip_high)
        rows = pl.ds(pl.multiple_of(side * half + line, tall), tall)
        copies.append(pltpu.make_async_copy(stage.at[i], out.at[rows, :], sems.at[i]))
        copies[-1].start()
    for copy in copies:
        copy.wait()


def basis_of(place, table, mine, mine_next, theirs, theirs_next, mix):
    height = 2 * mine.shape[0] * W
    tall = 256
    breadth = mix.shape[1]
    return pl.pallas_call(
        basis_rows,
        out_shape=jax.ShapeDtypeStruct((height, breadth), f32),
        in_specs=[SMEM] * 2 + [VMEM] * 5,
        out_specs=HBM,
        scratch_shapes=[pltpu.VMEM((height // tall, tall, breadth), f32), pltpu.SemaphoreType.DMA((height // tall,))],
        compiler_params=room(24),
    )(place, table, mine, mine_next, theirs, theirs_next, mix)


def scattered(parts, axis):
    return jnp.sum(lax.all_to_all(parts, axis, 0, 0, tiled=True), axis=0)


def gathered(part, axis):
    copies = jnp.broadcast_to(part, (lax.axis_size(axis), *part.shape))
    return lax.all_to_all(copies, axis, 0, 0, tiled=True)


def other_core(value):
    return lax.ppermute(value, CORE, SWAP)


def turned(rows, chips, cores):
    return [
        ((r * chips + a) * cores + b, (a * chips + SLOTS[b][a][r]) * cores + b)
        for r in range(rows)
        for a in range(chips)
        for b in range(cores)
    ]


def local(covariance, seed_index):
    height, breadth = covariance.shape
    width = seed_index.shape[0]
    rows, chips, cores = (lax.axis_size(a) for a in ALL)
    row, chip, core = (lax.axis_index(a) for a in ALL)
    order = height * rows
    turn = turned(rows, chips, cores)
    table = jnp.array(SLOTS, jnp.int32).reshape(-1)
    place = jnp.stack([row, core, chip * cores + core]).astype(jnp.int32)
    start_piece = scattered(picked_rows(place, seed_index, covariance, rows), ROWS).T
    start_turned = lax.ppermute(start_piece, ALL, turn)
    start = gathered(start_piece, ROWS).reshape(breadth, width)
    start, start_turned = lax.optimization_barrier((start, start_turned))
    keep, send = image_of_start(place, seed_index, covariance, start)
    got = other_core(send)
    small = grams_of_start(place, seed_index, start, chips)
    parts = jnp.concatenate([keep + got, small], axis=1)
    mine = gathered(jnp.concatenate([scattered(parts, CHIP), start_turned]), CHIP)
    theirs = other_core(mine)
    (grams,) = kernel(step_grams, [(2 * width, width)], place, table, mine)
    parts, zero_grams = image_of_step(place, covariance, mine, theirs, grams)
    piece = lax.ppermute(scattered(parts, ROWS), ALL, turn)
    (ready,) = kernel(first_factor, [(4 * width, width)], zero_grams)
    mine_next, ready = lax.optimization_barrier((gathered(piece, CHIP), ready))
    (keep,) = kernel(next_grams, [(3 * width + SPARE, width)], place, table, mine, mine_next)
    got = other_core(keep)
    totals = gathered(keep[2 * width :] + got[2 * width :], ROWS)
    theirs_next = other_core(mine_next)
    stage = [pltpu.VMEM((PACK, width), f32), pltpu.SemaphoreType.DMA((2,))]
    pack = pl.pallas_call(
        middle,
        out_shape=jax.ShapeDtypeStruct((PACK, width), f32),
        in_specs=[VMEM] * 4,
        out_specs=HBM,
        scratch_shapes=stage,
        compiler_params=room(60),
    )(zero_grams, ready, keep, got)
    totals, pack = lax.optimization_barrier((totals, pack))
    scale = float(order) ** 0.5

    def last_step(*refs):
        last(f32(scale), *refs)

    shapes = [(3 * width, 3 * width), (3 * width, 2 * width), (3 * width, 2 * width)]
    mix, projection, first_pass = pl.pallas_call(
        last_step,
        out_shape=[jax.ShapeDtypeStruct(s, f32) for s in shapes],
        in_specs=[HBM, HBM],
        out_specs=[VMEM] * 3,
        scratch_shapes=stage + [pltpu.VMEM(totals.shape, f32), pltpu.SemaphoreType.DMA],
        compiler_params=room(52),
    )(pack, totals)
    basis = basis_of(place, table, mine, mine_next, theirs, theirs_next, mix)
    return basis, projection, first_pass


def solution(mesh):
    rows, cols = mesh.devices.shape
    fine = Mesh(mesh.devices.reshape(rows, cols // 2, 2), ALL)
    return jax.shard_map(
        local,
        mesh=fine,
        in_specs=(P(ROWS, (CHIP, CORE)), P()),
        out_specs=(P(ROWS, None), P(), P()),
        check_vma=False,
    )
```

```python
import jax
import jax.numpy as jnp
from jax import lax
from jax.experimental import pallas as pl
from jax.experimental.pallas import tpu as pltpu
from jax.sharding import Mesh, PartitionSpec as P

ROWS = "row"
CHIP = "chip"
CORE = "core"
ALL = (ROWS, CHIP, CORE)
SWAP = [(0, 1), (1, 0)]
SLOTS = (
    (
        (2, 6, 3, 5, 0, 4, 1, 7),
        (7, 3, 6, 2, 5, 1, 4, 0),
        (3, 5, 0, 4, 1, 7, 2, 6),
        (4, 0, 5, 1, 6, 2, 7, 3),
        (4, 0, 7, 3, 6, 2, 5, 1),
        (1, 5, 2, 6, 3, 7, 0, 4),
        (7, 3, 6, 2, 5, 1, 4, 0),
        (2, 4, 3, 7, 0, 6, 1, 5),
    ),
    (
        (2, 6, 1, 7, 0, 4, 3, 5),
        (7, 3, 4, 0, 5, 1, 6, 2),
        (3, 7, 0, 4, 1, 5, 2, 6),
        (6, 0, 5, 1, 4, 2, 7, 3),
        (4, 0, 7, 1, 6, 2, 5, 3),
        (1, 5, 0, 6, 3, 7, 2, 4),
        (7, 3, 6, 2, 5, 1, 4, 0),
        (2, 4, 3, 7, 0, 6, 1, 5),
    ),
)
W = 128
f32 = jnp.float32
bf16 = jnp.bfloat16
HI = lax.Precision.HIGHEST


def dot(a, b, dims):
    return lax.dot_general(a, b, (dims, ((), ())), precision=HI, preferred_element_type=f32)


def nn(a, b):
    return dot(a, b, ((1,), (0,)))


def tn(a, b):
    return dot(a, b, ((0,), (0,)))


def nt(a, b):
    return dot(a, b, ((1,), (1,)))


def pieces(x):
    a = x.astype(bf16)
    rest = x - a.astype(f32)
    b = rest.astype(bf16)
    return a, b, (rest - b.astype(f32)).astype(bf16)


def outer(left, panel):
    a0, a1, a2 = pieces(left)
    b0, b1, b2 = pieces(panel)
    return lax.dot_general(
        jnp.concatenate([a0, a0, a1, a0, a2, a1]),
        jnp.concatenate([b0, b1, b0, b2, b0, b1]),
        (((0,), (0,)), ((), ())),
        preferred_element_type=f32,
    )


BAND = 16


def factor(gram):
    sub = lax.broadcasted_iota(jnp.int32, (BAND, W), 0)
    lane = lax.broadcasted_iota(jnp.int32, (BAND, W), 1)
    eye = lax.broadcasted_iota(jnp.int32, (W, W), 0) == lax.broadcasted_iota(jnp.int32, (W, W), 1)
    rest = jnp.concatenate([gram, eye.astype(f32)], axis=1)
    now, rest = rest[:BAND], rest[BAND:]
    upper, inverse = [], []
    for base in range(0, W, BAND):
        left, right = now[:, :W], now[:, W:]
        cols = [jnp.broadcast_to(left[:, base + k : base + k + 1], (BAND, W)) for k in range(BAND)]
        scale = jnp.zeros((BAND, W), f32)
        for k in range(0, BAND, 2):
            top = k // 8 * 8
            here = sub[top:]

            def line(x, i):
                return jnp.broadcast_to(x[i : i + 1, :], (BAND - top, W))

            def below(old, new):
                return new if top == 0 else jnp.concatenate([old[:top], new])

            c, d = cols[k][top:], cols[k + 1][top:]
            p, q, r = line(cols[k], k), line(cols[k + 1], k), line(cols[k + 1], k + 1)
            det = p * r - q * q
            inv_p = 1.0 / p
            inv = 1.0 / det
            later = here > k + 1
            u = jnp.where(later, (c * r - d * q) * inv, jnp.where(here == k + 1, q * inv_p, 0.0))
            v = jnp.where(later, (d * p - c * q) * inv, 0.0)
            last_scale = jnp.where(here == k + 1, lax.rsqrt(det * inv_p), scale[top:])
            scale = below(scale, jnp.where(here == k, lax.rsqrt(p), last_scale))

            def update(x):
                return below(x, x[top:] - u * line(x, k) - v * line(x, k + 1))

            for m in range(k + 2, BAND):
                cols[m] = update(cols[m])
            left = update(left)
            right = update(right)
        left = jnp.where(lane >= base + sub, left * scale, 0.0)
        right = right * scale
        upper.append(left)
        inverse.append(right)
        end = base + BAND
        if end < W:
            panel = jnp.concatenate([left, right], axis=1)
            now = rest[:BAND] - outer(left[:, end : end + BAND], panel)
            if end + BAND < W:
                rest = rest[BAND:] - outer(left[:, end + BAND :], panel)
    return jnp.concatenate(upper), jnp.concatenate(inverse)


def blocks_of(ref, start, count):
    return ref[:, start : start + count, :].reshape(ref.shape[0] * count, W)


def turned_blocks(ref, place, table, start, count, parts, core):
    first = (core * ref.shape[0] + place[0]) * ref.shape[0]
    return jnp.concatenate([ref[table[first + p], start : start + count, :] for p in parts])


def first_factor(start, out):
    g00, cee = start[:W, :], start[W:, :]
    li0 = factor(g00)[1]
    u = nt(cee, li0)
    side = nn(li0, g00)
    for i, block in enumerate([li0, u, nn(side, u), nt(side, li0)]):
        out[i * W : (i + 1) * W, :] = block


def middle(start, ready, keep, got, pack, stage, sems):
    g00, cee = start[:W, :], start[W:, :]
    li0, u, h0, m00 = (ready[i * W : (i + 1) * W, :] for i in range(4))
    g01, g11 = (keep[i * W : (i + 1) * W, :] + got[i * W : (i + 1) * W, :] for i in range(2))
    x0 = li0.T
    side = jnp.concatenate([g00, g01], axis=1)
    gram = jnp.concatenate([side, jnp.concatenate([g01.T, g11], axis=1)])
    h = h0 + nt(nn(li0, g01), li0)
    h_full = h + (h - nn(m00, h))
    g02 = g11 + tn(cee, g01)
    for i, block in enumerate([h, h_full, m00, g02, li0]):
        stage[i * W : (i + 1) * W, :] = block
    pack_copy(stage, pack, sems, 0).start()
    comb = jnp.concatenate([u - nn(x0, h_full), x0])
    y = nn(gram, comb)
    upper1, li1 = factor(tn(comb, y))
    c1 = nt(comb, li1)
    y1 = nt(y, li1)
    m01 = nn(li0, y1[:W])
    i1 = jnp.concatenate([nn(cee, c1[:W]), c1])
    s0 = nn(jnp.concatenate([side, g02], axis=1), i1)
    s1 = nn(gram[W:], i1[: 2 * W])
    late = [upper1, i1[:W], i1[W : 2 * W], i1[2 * W :], m01, tn(c1, y1), nn(li0, s0), tn(c1[:W], s0), s1]
    late.append(tn(i1[:W], s0))
    for i, block in enumerate(late):
        stage[EARLY + i * W : EARLY + (i + 1) * W, :] = block
    second = pack_copy(stage, pack, sems, 1)
    second.start()
    pack_copy(stage, pack, sems, 0).wait()
    second.wait()


EARLY = 5 * W
PACK = 15 * W


def pack_copy(source, target, sems, late):
    lines = pl.ds(EARLY, PACK - EARLY) if late else pl.ds(0, EARLY)
    return pltpu.make_async_copy(source.at[lines, :], target.at[lines, :], sems.at[late])


def last(scale, packed, totals, mix, projection, first_pass, pack, sems, parts, total_sem):
    copies = [pack_copy(packed, pack, sems, i) for i in range(2)]
    summands = pltpu.make_async_copy(totals, parts, total_sem)
    summands.start()
    for copy in copies:
        copy.start()
    summands.wait()
    a12, a22 = unpacked(parts[...])
    for copy in copies:
        copy.wait()
    first, full, m00, a02, li0, upper1, _, c1_top, c1_low, m01, m11, first0, part1, s1, square = (
        pack[i * W : (i + 1) * W, :] for i in range(PACK // W)
    )
    i1 = pack[EARLY + W : EARLY + 4 * W, :]
    c1 = i1[W:]
    s1 = s1 + nn(a12, c1_low)
    s2 = nn(jnp.concatenate([a02.T, a12, a22], axis=1), i1)
    square = square + tn(c1, jnp.concatenate([s1, s2]))
    h = jnp.concatenate([first0, part1 + tn(c1_low, s1)])
    gram_p = jnp.concatenate([jnp.concatenate([m00, m01], axis=1), jnp.concatenate([m01.T, m11], axis=1)])
    h_full = h + (h - nn(gram_p, h))
    inner = tn(h, h_full)
    upper2, li2 = factor(square - inner - inner.T + tn(h_full, nn(gram_p, h_full)))
    zero = jnp.zeros((W, W), f32)
    places = jnp.concatenate([jnp.concatenate([li0.T, zero]), c1], axis=1)
    comb = jnp.concatenate([i1[: 2 * W] - nn(places, h_full), i1[2 * W :]])
    mix[: 2 * W, : 2 * W] = places * scale
    mix[2 * W :, : 2 * W] = jnp.zeros((W, 2 * W), f32)
    mix[:, 2 * W :] = nt(comb, li2) * scale
    projection[:W, :W] = full
    projection[W : 2 * W, :W] = upper1
    projection[2 * W :, :W] = zero
    projection[: 2 * W, W:] = h_full
    projection[2 * W :, W:] = upper2
    first_pass[:W, :W] = first
    first_pass[W:, :W] = jnp.zeros((2 * W, W), f32)
    first_pass[: 2 * W, W:] = h
    first_pass[2 * W :, W:] = zero


HBM = pl.BlockSpec(memory_space=pltpu.HBM)
VMEM = pl.BlockSpec(memory_space=pltpu.VMEM)
SMEM = pl.BlockSpec(memory_space=pltpu.SMEM)


def room(mib):
    return pltpu.CompilerParams(vmem_limit_bytes=mib * 2**20)


def kernel(body, shapes, *args):
    return pl.pallas_call(
        body,
        out_shape=[jax.ShapeDtypeStruct(s, f32) for s in shapes],
        in_specs=[VMEM if a.dtype == f32 else SMEM for a in args],
        out_specs=[VMEM] * len(shapes),
        compiler_params=room(16),
    )(*args)


def halves(x):
    high = x.astype(bf16)
    return high, (x - high.astype(f32)).astype(bf16)


def mm(a, b):
    return lax.dot_general(a, b, (((1,), (0,)), ((), ())), preferred_element_type=f32)


def pick_rows(place, seeds, lanes, covariance, out, buffer, sem):
    count = seeds.shape[0]
    height = covariance.shape[0]
    base = place[0] * height

    def row(line, i):
        return pltpu.make_async_copy(covariance.at[pl.ds(line, 1), :], buffer.at[pl.ds(i, 1), :], sem)

    def body(i, found):
        line = seeds[i] - base
        here = (line >= 0) & (line < height)

        @pl.when(here)
        def _():
            row(line, i).start()

        return found + here.astype(jnp.int32)

    found = lax.fori_loop(0, count, body, 0, unroll=8)
    offsets = jnp.broadcast_to(lanes[...] - base, (count, count))
    held = jnp.where((offsets >= 0) & (offsets < height), 1.0, 0.0).T > 0

    def done(i, carry):
        row(0, 0).wait()
        return carry

    lax.fori_loop(0, found, done, 0)
    for p in range(out.shape[0]):
        out[p] = jnp.where(held, buffer[:, p * W : (p + 1) * W], 0.0)


def picked_rows(place, seeds, covariance, parts):
    count = seeds.shape[0]
    return pl.pallas_call(
        pick_rows,
        out_shape=jax.ShapeDtypeStruct((parts, count, W), f32),
        in_specs=[SMEM, SMEM, VMEM, HBM],
        out_specs=VMEM,
        scratch_shapes=[pltpu.VMEM((count, covariance.shape[1]), f32), pltpu.SemaphoreType.DMA],
        compiler_params=room(50),
    )(place, seeds, seeds.reshape(1, count), covariance)


CHUNKS = 8


def hold_rows(covariance, out, sem):
    tall = out.shape[0]
    copy = pltpu.make_async_copy(covariance.at[pl.ds(covariance.shape[0] - tall, tall), :], out, sem)
    copy.start()
    copy.wait()


def held_rows(covariance, chunks):
    height, breadth = covariance.shape
    return pl.pallas_call(
        hold_rows,
        out_shape=pltpu.VMEM((height // CHUNKS * chunks, breadth), f32),
        in_specs=[HBM],
        out_specs=VMEM,
        scratch_shapes=[pltpu.SemaphoreType.DMA],
        compiler_params=room(57),
    )(covariance)


def chunks_of(covariance, held, buffer, sems):
    tall = covariance.shape[0] // CHUNKS
    streamed = buffer.shape[0]
    copies = [
        pltpu.make_async_copy(covariance.at[pl.ds(i * tall, tall), :], buffer.at[i], sems.at[i]) for i in range(streamed)
    ]
    for copy in copies:
        copy.start()
    chunks = [(streamed + i, lambda i=i: held[i * tall : (i + 1) * tall, :]) for i in range(CHUNKS - streamed)]

    def arrived(i):
        copies[i].wait()
        return buffer[i]

    return chunks + [(i, lambda i=i: arrived(i)) for i in range(streamed)]


def chunk_scratch(covariance, held):
    height, breadth = covariance.shape
    streamed = CHUNKS - held.shape[0] * CHUNKS // height
    return [pltpu.VMEM((streamed, height // CHUNKS, breadth), f32), pltpu.SemaphoreType.DMA((streamed,))]


def first_product(place, lanes, covariance, held, start, keep, send, buffer, sems):
    height, breadth = covariance.shape
    half = height // 2
    tall = height // CHUNKS
    chunks = chunks_of(covariance, held, buffer, sems)
    lines = lax.broadcasted_iota(jnp.int32, (breadth, W), 0) + place[2] * breadth
    hot = jnp.where(lines == lanes[...], 1.0, 0.0)
    hit = jnp.max(hot, axis=1, keepdims=True) > 0
    weights = jnp.concatenate(halves(jnp.where(hit, 0.0, start[...])), axis=1)
    first = place[1] == 0
    for i, read in chunks:
        high, low = halves(read())
        both = mm(high, weights)
        value = both[:, :W] + both[:, W:] + mm(low, weights[:, :W])
        mine = first if i * tall < half else jnp.logical_not(first)

        def store(out):
            for q in range(tall // W):
                out[i * tall % half // W + q] = value[q * W : (q + 1) * W, :]

        @pl.when(mine)
        def _():
            store(keep)

        @pl.when(jnp.logical_not(mine))
        def _():
            store(send)


def image_of_start(place, seeds, covariance, held, start):
    height = covariance.shape[0]
    shape = jax.ShapeDtypeStruct((height // 2 // W, W, W), f32)
    return pl.pallas_call(
        first_product,
        out_shape=[shape, shape],
        in_specs=[SMEM, VMEM, HBM, VMEM, VMEM],
        out_specs=[VMEM] * 2,
        scratch_shapes=chunk_scratch(covariance, held),
        compiler_params=room(50),
    )(place, seeds.reshape(1, W), covariance, held, start)


def start_grams(place, lanes, start, out):
    block = start[...]
    lines = lax.broadcasted_iota(jnp.int32, block.shape, 0) + place[2] * block.shape[0]
    hot_t = jnp.where(lines == lanes[...], 1.0, 0.0).T.astype(bf16)
    b0, b1, b2 = pieces(block)
    turned_block = block.T
    high_t, low_t = halves(turned_block)
    both = mm(jnp.concatenate([hot_t, high_t]), jnp.concatenate([b0, b1], axis=1))
    cee = both[:W, :W] + both[:W, W:] + mm(hot_t, b2)
    g00 = both[W:, :W] + both[W:, W:] + mm(low_t, b0)
    parts = out.shape[0]
    bit = W // parts
    for p in range(parts):
        lines = slice(p * bit, (p + 1) * bit)
        out[p, :bit, :] = g00[lines]
        out[p, bit:, :] = cee[lines]


def grams_of_start(place, seeds, start, parts):
    return pl.pallas_call(
        start_grams,
        out_shape=jax.ShapeDtypeStruct((parts, 2 * W // parts, W), f32),
        in_specs=[SMEM, VMEM, VMEM],
        out_specs=VMEM,
        compiler_params=room(16),
    )(place, seeds.reshape(1, W), start)


def cross(a, b):
    right = halves(b)
    high, low = halves(a.T)
    both = mm(high, jnp.concatenate(right, axis=1))
    return both[:, :W] + both[:, W:] + mm(low, right[0])


def step_grams(place, table, mine, out):
    parts = mine.shape[0]
    step = blocks_of(mine, 0, W)
    start = turned_blocks(mine, place, table, W + 2 * W // parts, W, range(parts), place[1])
    out[:W, :] = cross(start, step)
    out[W:, :] = cross(step, step)


def corner():
    return lax.broadcasted_iota(jnp.int32, (W, W), 0), lax.broadcasted_iota(jnp.int32, (W, W), 1)


SPARE = 8


def next_grams(place, table, mine, following, out):
    parts = mine.shape[0]
    bit = W // parts
    step = blocks_of(mine, 0, W)
    then, g01, g11 = (
        turned_blocks(following, place, table, s, n, range(parts), place[1])
        for s, n in ((0, W), (W, bit), (W + bit, bit))
    )
    g12, g22 = cross(step, then), cross(then, then)
    i, j = corner()
    out[:W, :] = g01
    out[W : 2 * W, :] = g11
    out[2 * W : 3 * W, :] = jnp.where(j >= i, g22, g12)
    diagonal = jnp.sum(jnp.where(i == j, g12, 0.0), axis=0, keepdims=True)
    out[3 * W :, :] = jnp.broadcast_to(diagonal, (SPARE, W))


def unpacked(totals):
    total = jnp.sum(totals, axis=0)
    body = total[:W]
    i, j = corner()
    lower = jnp.where(j < i, body, 0.0)
    g12 = lower + lower.T + jnp.where(i == j, total[W : W + 1], 0.0)
    return g12, jnp.where(j >= i, body, 0.0) + jnp.where(j > i, body, 0.0).T


def second_product(place, covariance, held, mine, theirs, grams, out, small, buffer, sems, total):
    height, breadth = covariance.shape
    half = height // 2
    tall = height // CHUNKS
    chunks = chunks_of(covariance, held, buffer, sems)
    first = place[1] == 0
    parts = out.shape[0]
    bit = W // parts
    for p in range(parts):
        out[p, W : W + bit, :] = grams[p * bit : (p + 1) * bit, :]
        out[p, W + bit :, :] = grams[W + p * bit : W + (p + 1) * bit, :]
    for i in range(2):
        lines = W + i * bit
        small[i * W : (i + 1) * W, :] = blocks_of(mine, lines, bit) + blocks_of(theirs, lines, bit)
    for i, read in chunks:
        lines = slice(i * tall % half // W, (i * tall % half + tall) // W)
        own, other = (mine, theirs) if i * tall < half else (theirs, mine)
        block = jnp.where(first, own[lines, :W, :], other[lines, :W, :]).reshape(tall, W)
        v_high, v_low = halves(block.T)
        high, low = halves(read())
        both = mm(jnp.concatenate([v_high, v_low]), high)
        value = both[:W] + both[W:] + mm(v_high, low)
        if i == chunks[0][0]:
            total[...] = value
        elif i != chunks[-1][0]:
            total[...] += value
        else:
            value += total[...]
            for p in range(parts):
                out[p, :W, :] = value[:, p * W : (p + 1) * W].T


def image_of_step(place, covariance, held, mine, theirs, grams):
    breadth = covariance.shape[1]
    parts = breadth // W
    return pl.pallas_call(
        second_product,
        out_shape=[
            jax.ShapeDtypeStruct((parts, W + 2 * (W // parts), W), f32),
            jax.ShapeDtypeStruct((2 * W, W), f32),
        ],
        in_specs=[SMEM, HBM] + [VMEM] * 4,
        out_specs=[VMEM] * 2,
        scratch_shapes=chunk_scratch(covariance, held) + [pltpu.VMEM((W, breadth), f32)],
        compiler_params=room(50),
    )(place, covariance, held, mine, theirs, grams)


def basis_rows(place, table, mine, mine_next, theirs, theirs_next, mix, out, stage, sems):
    parts = mine.shape[0]
    bit = 2 * W // parts
    count, tall, _ = stage.shape
    half = count * tall // 2
    high, low = halves(mix[: 2 * W, : 2 * W])
    tip_high, tip_low = halves(mix[:, 2 * W :])
    tip = jnp.concatenate([tip_high, tip_low], axis=1)
    copies = []
    for i in range(count):
        line = i * tall % half
        pair, following, side = (mine, mine_next, place[1]) if i * tall < half else (theirs, theirs_next, 1 - place[1])
        order = range(line // W, (line + tall) // W)
        left = jnp.concatenate(
            [
                turned_blocks(pair, place, table, W + bit, W, order, side),
                pair[line // W : (line + tall) // W, :W, :].reshape(tall, W),
                turned_blocks(following, place, table, 0, W, order, side),
            ],
            axis=1,
        )
        l_high, l_low = halves(left)
        h2, l2 = l_high[:, : 2 * W], l_low[:, : 2 * W]
        stage[i, :, : 2 * W] = mm(h2, high) + mm(h2, low) + mm(l2, high)
        both = mm(l_high, tip)
        stage[i, :, 2 * W :] = both[:, :W] + both[:, W:] + mm(l_low, tip_high)
        rows = pl.ds(pl.multiple_of(side * half + line, tall), tall)
        copies.append(pltpu.make_async_copy(stage.at[i], out.at[rows, :], sems.at[i]))
        copies[-1].start()
    for copy in copies:
        copy.wait()


def basis_of(place, table, mine, mine_next, theirs, theirs_next, mix):
    height = 2 * mine.shape[0] * W
    tall = 256
    breadth = mix.shape[1]
    return pl.pallas_call(
        basis_rows,
        out_shape=jax.ShapeDtypeStruct((height, breadth), f32),
        in_specs=[SMEM] * 2 + [VMEM] * 5,
        out_specs=HBM,
        scratch_shapes=[pltpu.VMEM((height // tall, tall, breadth), f32), pltpu.SemaphoreType.DMA((height // tall,))],
        compiler_params=room(24),
    )(place, table, mine, mine_next, theirs, theirs_next, mix)


def scattered(parts, axis):
    return jnp.sum(lax.all_to_all(parts, axis, 0, 0, tiled=True), axis=0)


def gathered(part, axis):
    copies = jnp.broadcast_to(part, (lax.axis_size(axis), *part.shape))
    return lax.all_to_all(copies, axis, 0, 0, tiled=True)


def other_core(value):
    return lax.ppermute(value, CORE, SWAP)


def turned(rows, chips, cores):
    return [
        ((r * chips + a) * cores + b, (a * chips + SLOTS[b][a][r]) * cores + b)
        for r in range(rows)
        for a in range(chips)
        for b in range(cores)
    ]


def local(covariance, seed_index):
    height, breadth = covariance.shape
    width = seed_index.shape[0]
    rows, chips, cores = (lax.axis_size(a) for a in ALL)
    row, chip, core = (lax.axis_index(a) for a in ALL)
    order = height * rows
    turn = turned(rows, chips, cores)
    table = jnp.array(SLOTS, jnp.int32).reshape(-1)
    place = jnp.stack([row, core, chip * cores + core]).astype(jnp.int32)
    start_piece = scattered(picked_rows(place, seed_index, covariance, rows), ROWS).T
    block, start_piece = lax.optimization_barrier((covariance, start_piece))
    held = held_rows(block, 2)
    start_turned = lax.ppermute(start_piece, ALL, turn)
    start = gathered(start_piece, ROWS).reshape(breadth, width)
    start, start_turned, held = lax.optimization_barrier((start, start_turned, held))
    keep, send = image_of_start(place, seed_index, covariance, held, start)
    got = other_core(send)
    small = grams_of_start(place, seed_index, start, chips)
    parts = jnp.concatenate([keep + got, small], axis=1)
    block, parts = lax.optimization_barrier((covariance, parts))
    held = held_rows(block, 1)
    step, held = lax.optimization_barrier((lax.all_to_all(parts, CHIP, 0, 0, tiled=True), held))
    mine = gathered(jnp.concatenate([jnp.sum(step, axis=0), start_turned]), CHIP)
    theirs = other_core(mine)
    (grams,) = kernel(step_grams, [(2 * width, width)], place, table, mine)
    parts, zero_grams = image_of_step(place, covariance, held, mine, theirs, grams)
    piece = lax.ppermute(scattered(parts, ROWS), ALL, turn)
    (ready,) = kernel(first_factor, [(4 * width, width)], zero_grams)
    mine_next, ready = lax.optimization_barrier((gathered(piece, CHIP), ready))
    (keep,) = kernel(next_grams, [(3 * width + SPARE, width)], place, table, mine, mine_next)
    got = other_core(keep)
    totals = gathered(keep[2 * width :] + got[2 * width :], ROWS)
    theirs_next = other_core(mine_next)
    stage = [pltpu.VMEM((PACK, width), f32), pltpu.SemaphoreType.DMA((2,))]
    pack = pl.pallas_call(
        middle,
        out_shape=jax.ShapeDtypeStruct((PACK, width), f32),
        in_specs=[VMEM] * 4,
        out_specs=HBM,
        scratch_shapes=stage,
        compiler_params=room(60),
    )(zero_grams, ready, keep, got)
    totals, pack = lax.optimization_barrier((totals, pack))
    scale = float(order) ** 0.5

    def last_step(*refs):
        last(f32(scale), *refs)

    shapes = [(3 * width, 3 * width), (3 * width, 2 * width), (3 * width, 2 * width)]
    mix, projection, first_pass = pl.pallas_call(
        last_step,
        out_shape=[jax.ShapeDtypeStruct(s, f32) for s in shapes],
        in_specs=[HBM, HBM],
        out_specs=[VMEM] * 3,
        scratch_shapes=stage + [pltpu.VMEM(totals.shape, f32), pltpu.SemaphoreType.DMA],
        compiler_params=room(52),
    )(pack, totals)
    basis = basis_of(place, table, mine, mine_next, theirs, theirs_next, mix)
    return basis, projection, first_pass


def solution(mesh):
    rows, cols = mesh.devices.shape
    fine = Mesh(mesh.devices.reshape(rows, cols // 2, 2), ALL)
    return jax.shard_map(
        local,
        mesh=fine,
        in_specs=(P(ROWS, (CHIP, CORE)), P()),
        out_specs=(P(ROWS, None), P(), P()),
        check_vma=False,
    )
```

```python
import jax
import jax.numpy as jnp
from jax import lax
from jax.experimental import pallas as pl
from jax.experimental.pallas import tpu as pltpu
from jax.sharding import Mesh, PartitionSpec as P

ROWS = "row"
CHIP = "chip"
CORE = "core"
ALL = (ROWS, CHIP, CORE)
SWAP = [(0, 1), (1, 0)]
SLOTS = (
    (
        (2, 6, 3, 5, 0, 4, 1, 7),
        (7, 3, 6, 2, 5, 1, 4, 0),
        (3, 5, 0, 4, 1, 7, 2, 6),
        (4, 0, 5, 1, 6, 2, 7, 3),
        (4, 0, 7, 3, 6, 2, 5, 1),
        (1, 5, 2, 6, 3, 7, 0, 4),
        (7, 3, 6, 2, 5, 1, 4, 0),
        (2, 4, 3, 7, 0, 6, 1, 5),
    ),
    (
        (2, 6, 1, 7, 0, 4, 3, 5),
        (7, 3, 4, 0, 5, 1, 6, 2),
        (3, 7, 0, 4, 1, 5, 2, 6),
        (6, 0, 5, 1, 4, 2, 7, 3),
        (4, 0, 7, 1, 6, 2, 5, 3),
        (1, 5, 0, 6, 3, 7, 2, 4),
        (7, 3, 6, 2, 5, 1, 4, 0),
        (2, 4, 3, 7, 0, 6, 1, 5),
    ),
)
W = 128
f32 = jnp.float32
bf16 = jnp.bfloat16
HI = lax.Precision.HIGHEST


def dot(a, b, dims):
    return lax.dot_general(a, b, (dims, ((), ())), precision=HI, preferred_element_type=f32)


def nn(a, b):
    return dot(a, b, ((1,), (0,)))


def tn(a, b):
    return dot(a, b, ((0,), (0,)))


def nt(a, b):
    return dot(a, b, ((1,), (1,)))


def pieces(x):
    a = x.astype(bf16)
    rest = x - a.astype(f32)
    b = rest.astype(bf16)
    return a, b, (rest - b.astype(f32)).astype(bf16)


def outer(left, panel):
    a0, a1, a2 = pieces(left)
    b0, b1, b2 = pieces(panel)
    return lax.dot_general(
        jnp.concatenate([a0, a0, a1, a0, a2, a1]),
        jnp.concatenate([b0, b1, b0, b2, b0, b1]),
        (((0,), (0,)), ((), ())),
        preferred_element_type=f32,
    )


BAND = 16


def factor(gram):
    sub = lax.broadcasted_iota(jnp.int32, (BAND, W), 0)
    lane = lax.broadcasted_iota(jnp.int32, (BAND, W), 1)
    eye = lax.broadcasted_iota(jnp.int32, (W, W), 0) == lax.broadcasted_iota(jnp.int32, (W, W), 1)
    rest = jnp.concatenate([gram, eye.astype(f32)], axis=1)
    now, rest = rest[:BAND], rest[BAND:]
    upper, inverse = [], []
    for base in range(0, W, BAND):
        left, right = now[:, :W], now[:, W:]
        cols = [jnp.broadcast_to(left[:, base + k : base + k + 1], (BAND, W)) for k in range(BAND)]
        scale = jnp.zeros((BAND, W), f32)
        for k in range(0, BAND, 2):
            top = k // 8 * 8
            here = sub[top:]

            def line(x, i):
                return jnp.broadcast_to(x[i : i + 1, :], (BAND - top, W))

            def below(old, new):
                return new if top == 0 else jnp.concatenate([old[:top], new])

            c, d = cols[k][top:], cols[k + 1][top:]
            p, q, r = line(cols[k], k), line(cols[k + 1], k), line(cols[k + 1], k + 1)
            det = p * r - q * q
            inv_p = 1.0 / p
            inv = 1.0 / det
            later = here > k + 1
            u = jnp.where(later, (c * r - d * q) * inv, jnp.where(here == k + 1, q * inv_p, 0.0))
            v = jnp.where(later, (d * p - c * q) * inv, 0.0)
            last_scale = jnp.where(here == k + 1, lax.rsqrt(det * inv_p), scale[top:])
            scale = below(scale, jnp.where(here == k, lax.rsqrt(p), last_scale))

            def update(x):
                return below(x, x[top:] - u * line(x, k) - v * line(x, k + 1))

            for m in range(k + 2, BAND):
                cols[m] = update(cols[m])
            left = update(left)
            right = update(right)
        left = jnp.where(lane >= base + sub, left * scale, 0.0)
        right = right * scale
        upper.append(left)
        inverse.append(right)
        end = base + BAND
        if end < W:
            panel = jnp.concatenate([left, right], axis=1)
            now = rest[:BAND] - outer(left[:, end : end + BAND], panel)
            if end + BAND < W:
                rest = rest[BAND:] - outer(left[:, end + BAND :], panel)
    return jnp.concatenate(upper), jnp.concatenate(inverse)


def blocks_of(ref, start, count):
    return ref[:, start : start + count, :].reshape(ref.shape[0] * count, W)


def turned_blocks(ref, place, table, start, count, parts, core):
    first = (core * ref.shape[0] + place[0]) * ref.shape[0]
    return jnp.concatenate([ref[table[first + p], start : start + count, :] for p in parts])


def first_factor(start, out):
    g00, cee = start[:W, :], start[W:, :]
    li0 = factor(g00)[1]
    u = nt(cee, li0)
    side = nn(li0, g00)
    for i, block in enumerate([li0, u, nn(side, u), nt(side, li0)]):
        out[i * W : (i + 1) * W, :] = block


def middle(start, ready, keep, got, pack, stage, sems):
    g00, cee = start[:W, :], start[W:, :]
    li0, u, h0, m00 = (ready[i * W : (i + 1) * W, :] for i in range(4))
    g01, g11 = (keep[i * W : (i + 1) * W, :] + got[i * W : (i + 1) * W, :] for i in range(2))
    x0 = li0.T
    side = jnp.concatenate([g00, g01], axis=1)
    gram = jnp.concatenate([side, jnp.concatenate([g01.T, g11], axis=1)])
    h = h0 + nt(nn(li0, g01), li0)
    h_full = h + (h - nn(m00, h))
    g02 = g11 + tn(cee, g01)
    for i, block in enumerate([h, h_full, m00, g02, li0]):
        stage[i * W : (i + 1) * W, :] = block
    pack_copy(stage, pack, sems, 0).start()
    comb = jnp.concatenate([u - nn(x0, h_full), x0])
    y = nn(gram, comb)
    upper1, li1 = factor(tn(comb, y))
    c1 = nt(comb, li1)
    y1 = nt(y, li1)
    m01 = nn(li0, y1[:W])
    i1 = jnp.concatenate([nn(cee, c1[:W]), c1])
    s0 = nn(jnp.concatenate([side, g02], axis=1), i1)
    s1 = nn(gram[W:], i1[: 2 * W])
    late = [upper1, i1[:W], i1[W : 2 * W], i1[2 * W :], m01, tn(c1, y1), nn(li0, s0), tn(c1[:W], s0), s1]
    late.append(tn(i1[:W], s0))
    for i, block in enumerate(late):
        stage[EARLY + i * W : EARLY + (i + 1) * W, :] = block
    second = pack_copy(stage, pack, sems, 1)
    second.start()
    pack_copy(stage, pack, sems, 0).wait()
    second.wait()


EARLY = 5 * W
PACK = 15 * W


def pack_copy(source, target, sems, late):
    lines = pl.ds(EARLY, PACK - EARLY) if late else pl.ds(0, EARLY)
    return pltpu.make_async_copy(source.at[lines, :], target.at[lines, :], sems.at[late])


def last(scale, packed, totals, mix, projection, first_pass, pack, sems, parts, total_sem):
    copies = [pack_copy(packed, pack, sems, i) for i in range(2)]
    summands = pltpu.make_async_copy(totals, parts, total_sem)
    summands.start()
    for copy in copies:
        copy.start()
    summands.wait()
    a12, a22 = unpacked(parts[...])
    for copy in copies:
        copy.wait()
    first, full, m00, a02, li0, upper1, _, c1_top, c1_low, m01, m11, first0, part1, s1, square = (
        pack[i * W : (i + 1) * W, :] for i in range(PACK // W)
    )
    i1 = pack[EARLY + W : EARLY + 4 * W, :]
    c1 = i1[W:]
    s1 = s1 + nn(a12, c1_low)
    s2 = nn(jnp.concatenate([a02.T, a12, a22], axis=1), i1)
    square = square + tn(c1, jnp.concatenate([s1, s2]))
    h = jnp.concatenate([first0, part1 + tn(c1_low, s1)])
    gram_p = jnp.concatenate([jnp.concatenate([m00, m01], axis=1), jnp.concatenate([m01.T, m11], axis=1)])
    h_full = h + (h - nn(gram_p, h))
    inner = tn(h, h_full)
    upper2, li2 = factor(square - inner - inner.T + tn(h_full, nn(gram_p, h_full)))
    zero = jnp.zeros((W, W), f32)
    places = jnp.concatenate([jnp.concatenate([li0.T, zero]), c1], axis=1)
    comb = jnp.concatenate([i1[: 2 * W] - nn(places, h_full), i1[2 * W :]])
    mix[: 2 * W, : 2 * W] = places * scale
    mix[2 * W :, : 2 * W] = jnp.zeros((W, 2 * W), f32)
    mix[:, 2 * W :] = nt(comb, li2) * scale
    projection[:W, :W] = full
    projection[W : 2 * W, :W] = upper1
    projection[2 * W :, :W] = zero
    projection[: 2 * W, W:] = h_full
    projection[2 * W :, W:] = upper2
    first_pass[:W, :W] = first
    first_pass[W:, :W] = jnp.zeros((2 * W, W), f32)
    first_pass[: 2 * W, W:] = h
    first_pass[2 * W :, W:] = zero


HBM = pl.BlockSpec(memory_space=pltpu.HBM)
VMEM = pl.BlockSpec(memory_space=pltpu.VMEM)
SMEM = pl.BlockSpec(memory_space=pltpu.SMEM)


def room(mib):
    return pltpu.CompilerParams(vmem_limit_bytes=mib * 2**20)


def kernel(body, shapes, *args):
    return pl.pallas_call(
        body,
        out_shape=[jax.ShapeDtypeStruct(s, f32) for s in shapes],
        in_specs=[VMEM if a.dtype == f32 else SMEM for a in args],
        out_specs=[VMEM] * len(shapes),
        compiler_params=room(16),
    )(*args)


def halves(x):
    high = x.astype(bf16)
    return high, (x - high.astype(f32)).astype(bf16)


def mm(a, b):
    return lax.dot_general(a, b, (((1,), (0,)), ((), ())), preferred_element_type=f32)


def pick_rows(place, seeds, lanes, covariance, out, buffer, sem):
    count = seeds.shape[0]
    height = covariance.shape[0]
    base = place[0] * height

    def row(line, i):
        return pltpu.make_async_copy(covariance.at[pl.ds(line, 1), :], buffer.at[pl.ds(i, 1), :], sem)

    def body(i, found):
        line = seeds[i] - base
        here = (line >= 0) & (line < height)

        @pl.when(here)
        def _():
            row(line, i).start()

        return found + here.astype(jnp.int32)

    found = lax.fori_loop(0, count, body, 0, unroll=8)
    offsets = jnp.broadcast_to(lanes[...] - base, (count, count))
    held = jnp.where((offsets >= 0) & (offsets < height), 1.0, 0.0).T > 0

    def done(i, carry):
        row(0, 0).wait()
        return carry

    lax.fori_loop(0, found, done, 0)
    for p in range(out.shape[0]):
        out[p] = jnp.where(held, buffer[:, p * W : (p + 1) * W], 0.0)


def picked_rows(place, seeds, covariance, parts):
    count = seeds.shape[0]
    return pl.pallas_call(
        pick_rows,
        out_shape=jax.ShapeDtypeStruct((parts, count, W), f32),
        in_specs=[SMEM, SMEM, VMEM, HBM],
        out_specs=VMEM,
        scratch_shapes=[pltpu.VMEM((count, covariance.shape[1]), f32), pltpu.SemaphoreType.DMA],
        compiler_params=room(50),
    )(place, seeds, seeds.reshape(1, count), covariance)


CHUNKS = 8


def hold_rows(covariance, out, sem):
    tall = out.shape[0]
    copy = pltpu.make_async_copy(covariance.at[pl.ds(covariance.shape[0] - tall, tall), :], out, sem)
    copy.start()
    copy.wait()


def held_rows(covariance, chunks):
    height, breadth = covariance.shape
    return pl.pallas_call(
        hold_rows,
        out_shape=pltpu.VMEM((height // CHUNKS * chunks, breadth), f32),
        in_specs=[HBM],
        out_specs=VMEM,
        scratch_shapes=[pltpu.SemaphoreType.DMA],
        compiler_params=room(57),
    )(covariance)


def chunks_of(covariance, held, buffer, sems):
    tall = covariance.shape[0] // CHUNKS
    streamed = buffer.shape[0]
    copies = [
        pltpu.make_async_copy(covariance.at[pl.ds(i * tall, tall), :], buffer.at[i], sems.at[i]) for i in range(streamed)
    ]
    for copy in copies:
        copy.start()
    chunks = [(streamed + i, lambda i=i: held[i * tall : (i + 1) * tall, :]) for i in range(CHUNKS - streamed)]

    def arrived(i):
        copies[i].wait()
        return buffer[i]

    return chunks + [(i, lambda i=i: arrived(i)) for i in range(streamed)]


def chunk_scratch(covariance, held):
    height, breadth = covariance.shape
    streamed = CHUNKS - held * CHUNKS // height
    return [pltpu.VMEM((streamed, height // CHUNKS, breadth), f32), pltpu.SemaphoreType.DMA((streamed,))]


def first_product(place, lanes, covariance, held, start, keep, send, buffer, sems):
    height, breadth = covariance.shape
    half = height // 2
    tall = height // CHUNKS
    chunks = chunks_of(covariance, held, buffer, sems)
    lines = lax.broadcasted_iota(jnp.int32, (breadth, W), 0) + place[2] * breadth
    hot = jnp.where(lines == lanes[...], 1.0, 0.0)
    hit = jnp.max(hot, axis=1, keepdims=True) > 0
    weights = jnp.concatenate(halves(jnp.where(hit, 0.0, start[...])), axis=1)
    first = place[1] == 0
    for i, read in chunks:
        high, low = halves(read())
        both = mm(high, weights)
        value = both[:, :W] + both[:, W:] + mm(low, weights[:, :W])
        mine = first if i * tall < half else jnp.logical_not(first)

        def store(out):
            for q in range(tall // W):
                out[i * tall % half // W + q] = value[q * W : (q + 1) * W, :]

        @pl.when(mine)
        def _():
            store(keep)

        @pl.when(jnp.logical_not(mine))
        def _():
            store(send)


def image_of_start(place, seeds, covariance, held, start):
    height = covariance.shape[0]
    shape = jax.ShapeDtypeStruct((height // 2 // W, W, W), f32)
    return pl.pallas_call(
        first_product,
        out_shape=[shape, shape],
        in_specs=[SMEM, VMEM, HBM, VMEM, VMEM],
        out_specs=[VMEM] * 2,
        scratch_shapes=chunk_scratch(covariance, held.shape[0]),
        compiler_params=room(50),
    )(place, seeds.reshape(1, W), covariance, held, start)


def start_grams(place, lanes, start, out):
    block = start[...]
    lines = lax.broadcasted_iota(jnp.int32, block.shape, 0) + place[2] * block.shape[0]
    hot_t = jnp.where(lines == lanes[...], 1.0, 0.0).T.astype(bf16)
    b0, b1, b2 = pieces(block)
    turned_block = block.T
    high_t, low_t = halves(turned_block)
    both = mm(jnp.concatenate([hot_t, high_t]), jnp.concatenate([b0, b1], axis=1))
    cee = both[:W, :W] + both[:W, W:] + mm(hot_t, b2)
    g00 = both[W:, :W] + both[W:, W:] + mm(low_t, b0)
    parts = out.shape[0]
    bit = W // parts
    for p in range(parts):
        lines = slice(p * bit, (p + 1) * bit)
        out[p, :bit, :] = g00[lines]
        out[p, bit:, :] = cee[lines]


def grams_of_start(place, seeds, start, parts):
    return pl.pallas_call(
        start_grams,
        out_shape=jax.ShapeDtypeStruct((parts, 2 * W // parts, W), f32),
        in_specs=[SMEM, VMEM, VMEM],
        out_specs=VMEM,
        compiler_params=room(16),
    )(place, seeds.reshape(1, W), start)


def cross(a, b):
    right = halves(b)
    high, low = halves(a.T)
    both = mm(high, jnp.concatenate(right, axis=1))
    return both[:, :W] + both[:, W:] + mm(low, right[0])


def fold(parts, out):
    out[...] = jnp.sum(parts[...], axis=0)


def step_grams(place, table, mine, out):
    parts = mine.shape[0]
    step = blocks_of(mine, 0, W)
    start = turned_blocks(mine, place, table, W + 2 * W // parts, W, range(parts), place[1])
    out[:W, :] = cross(start, step)
    out[W:, :] = cross(step, step)


def corner():
    return lax.broadcasted_iota(jnp.int32, (W, W), 0), lax.broadcasted_iota(jnp.int32, (W, W), 1)


SPARE = 8


def next_grams(place, table, mine, following, out):
    parts = mine.shape[0]
    bit = W // parts
    step = blocks_of(mine, 0, W)
    then, g01, g11 = (
        turned_blocks(following, place, table, s, n, range(parts), place[1])
        for s, n in ((0, W), (W, bit), (W + bit, bit))
    )
    g12, g22 = cross(step, then), cross(then, then)
    i, j = corner()
    out[:W, :] = g01
    out[W : 2 * W, :] = g11
    out[2 * W : 3 * W, :] = jnp.where(j >= i, g22, g12)
    diagonal = jnp.sum(jnp.where(i == j, g12, 0.0), axis=0, keepdims=True)
    out[3 * W :, :] = jnp.broadcast_to(diagonal, (SPARE, W))


def unpacked(totals):
    total = jnp.sum(totals, axis=0)
    body = total[:W]
    i, j = corner()
    lower = jnp.where(j < i, body, 0.0)
    g12 = lower + lower.T + jnp.where(i == j, total[W : W + 1], 0.0)
    return g12, jnp.where(j >= i, body, 0.0) + jnp.where(j > i, body, 0.0).T


def second_product(place, covariance, mine, theirs, grams, out, small, buffer, sems, total):
    height, breadth = covariance.shape
    half = height // 2
    tall = height // CHUNKS
    chunks = chunks_of(covariance, None, buffer, sems)
    first = place[1] == 0
    parts = out.shape[0]
    bit = W // parts
    for p in range(parts):
        out[p, W : W + bit, :] = grams[p * bit : (p + 1) * bit, :]
        out[p, W + bit :, :] = grams[W + p * bit : W + (p + 1) * bit, :]
    for i in range(2):
        lines = W + i * bit
        small[i * W : (i + 1) * W, :] = blocks_of(mine, lines, bit) + blocks_of(theirs, lines, bit)
    for i, read in chunks:
        lines = slice(i * tall % half // W, (i * tall % half + tall) // W)
        own, other = (mine, theirs) if i * tall < half else (theirs, mine)
        block = jnp.where(first, own[lines, :W, :], other[lines, :W, :]).reshape(tall, W)
        v_high, v_low = halves(block.T)
        high, low = halves(read())
        both = mm(jnp.concatenate([v_high, v_low]), high)
        value = both[:W] + both[W:] + mm(v_high, low)
        if i == chunks[0][0]:
            total[...] = value
        elif i != chunks[-1][0]:
            total[...] += value
        else:
            value += total[...]
            for p in range(parts):
                out[p, :W, :] = value[:, p * W : (p + 1) * W].T


def image_of_step(place, covariance, mine, theirs, grams):
    breadth = covariance.shape[1]
    parts = breadth // W
    return pl.pallas_call(
        second_product,
        out_shape=[
            jax.ShapeDtypeStruct((parts, W + 2 * (W // parts), W), f32),
            jax.ShapeDtypeStruct((2 * W, W), f32),
        ],
        in_specs=[SMEM, HBM] + [VMEM] * 3,
        out_specs=[VMEM] * 2,
        scratch_shapes=chunk_scratch(covariance, 0) + [pltpu.VMEM((W, breadth), f32)],
        compiler_params=room(50),
    )(place, covariance, mine, theirs, grams)


def basis_rows(place, table, mine, mine_next, theirs, theirs_next, mix, out, stage, sems):
    parts = mine.shape[0]
    bit = 2 * W // parts
    count, tall, _ = stage.shape
    half = count * tall // 2
    high, low = halves(mix[: 2 * W, : 2 * W])
    tip_high, tip_low = halves(mix[:, 2 * W :])
    tip = jnp.concatenate([tip_high, tip_low], axis=1)
    copies = []
    for i in range(count):
        line = i * tall % half
        pair, following, side = (mine, mine_next, place[1]) if i * tall < half else (theirs, theirs_next, 1 - place[1])
        order = range(line // W, (line + tall) // W)
        left = jnp.concatenate(
            [
                turned_blocks(pair, place, table, W + bit, W, order, side),
                pair[line // W : (line + tall) // W, :W, :].reshape(tall, W),
                turned_blocks(following, place, table, 0, W, order, side),
            ],
            axis=1,
        )
        l_high, l_low = halves(left)
        h2, l2 = l_high[:, : 2 * W], l_low[:, : 2 * W]
        stage[i, :, : 2 * W] = mm(h2, high) + mm(h2, low) + mm(l2, high)
        both = mm(l_high, tip)
        stage[i, :, 2 * W :] = both[:, :W] + both[:, W:] + mm(l_low, tip_high)
        rows = pl.ds(pl.multiple_of(side * half + line, tall), tall)
        copies.append(pltpu.make_async_copy(stage.at[i], out.at[rows, :], sems.at[i]))
        copies[-1].start()
    for copy in copies:
        copy.wait()


def basis_of(place, table, mine, mine_next, theirs, theirs_next, mix):
    height = 2 * mine.shape[0] * W
    tall = 256
    breadth = mix.shape[1]
    return pl.pallas_call(
        basis_rows,
        out_shape=jax.ShapeDtypeStruct((height, breadth), f32),
        in_specs=[SMEM] * 2 + [VMEM] * 5,
        out_specs=HBM,
        scratch_shapes=[pltpu.VMEM((height // tall, tall, breadth), f32), pltpu.SemaphoreType.DMA((height // tall,))],
        compiler_params=room(24),
    )(place, table, mine, mine_next, theirs, theirs_next, mix)


def scattered(parts, axis):
    return jnp.sum(lax.all_to_all(parts, axis, 0, 0, tiled=True), axis=0)


def gathered(part, axis):
    copies = jnp.broadcast_to(part, (lax.axis_size(axis), *part.shape))
    return lax.all_to_all(copies, axis, 0, 0, tiled=True)


def other_core(value):
    return lax.ppermute(value, CORE, SWAP)


def turned(rows, chips, cores):
    return [
        ((r * chips + a) * cores + b, (a * chips + SLOTS[b][a][r]) * cores + b)
        for r in range(rows)
        for a in range(chips)
        for b in range(cores)
    ]


def local(covariance, seed_index):
    height, breadth = covariance.shape
    width = seed_index.shape[0]
    rows, chips, cores = (lax.axis_size(a) for a in ALL)
    row, chip, core = (lax.axis_index(a) for a in ALL)
    order = height * rows
    turn = turned(rows, chips, cores)
    table = jnp.array(SLOTS, jnp.int32).reshape(-1)
    place = jnp.stack([row, core, chip * cores + core]).astype(jnp.int32)
    start_piece = scattered(picked_rows(place, seed_index, covariance, rows), ROWS).T
    block, start_piece = lax.optimization_barrier((covariance, start_piece))
    held = held_rows(block, 2)
    start_turned = lax.ppermute(start_piece, ALL, turn)
    start = gathered(start_piece, ROWS).reshape(breadth, width)
    start, start_turned, held = lax.optimization_barrier((start, start_turned, held))
    keep, send = image_of_start(place, seed_index, covariance, held, start)
    got = other_core(send)
    small = grams_of_start(place, seed_index, start, chips)
    parts = jnp.concatenate([keep + got, small], axis=1)
    mine = gathered(jnp.concatenate([scattered(parts, CHIP), start_turned]), CHIP)
    theirs = other_core(mine)
    (grams,) = kernel(step_grams, [(2 * width, width)], place, table, mine)
    parts, zero_grams = image_of_step(place, covariance, mine, theirs, grams)
    (piece,) = kernel(fold, [parts.shape[1:]], lax.all_to_all(parts, ROWS, 0, 0, tiled=True))
    piece = lax.ppermute(piece, ALL, turn)
    (ready,) = kernel(first_factor, [(4 * width, width)], zero_grams)
    mine_next, ready = lax.optimization_barrier((gathered(piece, CHIP), ready))
    (keep,) = kernel(next_grams, [(3 * width + SPARE, width)], place, table, mine, mine_next)
    got = other_core(keep)
    totals = gathered(keep[2 * width :] + got[2 * width :], ROWS)
    theirs_next = other_core(mine_next)
    stage = [pltpu.VMEM((PACK, width), f32), pltpu.SemaphoreType.DMA((2,))]
    pack = pl.pallas_call(
        middle,
        out_shape=jax.ShapeDtypeStruct((PACK, width), f32),
        in_specs=[VMEM] * 4,
        out_specs=HBM,
        scratch_shapes=stage,
        compiler_params=room(60),
    )(zero_grams, ready, keep, got)
    totals, pack = lax.optimization_barrier((totals, pack))
    scale = float(order) ** 0.5

    def last_step(*refs):
        last(f32(scale), *refs)

    shapes = [(3 * width, 3 * width), (3 * width, 2 * width), (3 * width, 2 * width)]
    mix, projection, first_pass = pl.pallas_call(
        last_step,
        out_shape=[jax.ShapeDtypeStruct(s, f32) for s in shapes],
        in_specs=[HBM, HBM],
        out_specs=[VMEM] * 3,
        scratch_shapes=stage + [pltpu.VMEM(totals.shape, f32), pltpu.SemaphoreType.DMA],
        compiler_params=room(52),
    )(pack, totals)
    basis = basis_of(place, table, mine, mine_next, theirs, theirs_next, mix)
    return basis, projection, first_pass


def solution(mesh):
    rows, cols = mesh.devices.shape
    fine = Mesh(mesh.devices.reshape(rows, cols // 2, 2), ALL)
    return jax.shard_map(
        local,
        mesh=fine,
        in_specs=(P(ROWS, (CHIP, CORE)), P()),
        out_specs=(P(ROWS, None), P(), P()),
        check_vma=False,
    )
```

```python
import jax
import jax.numpy as jnp
from jax import lax
from jax.experimental import pallas as pl
from jax.experimental.pallas import tpu as pltpu
from jax.sharding import Mesh, PartitionSpec as P

ROWS = "row"
CHIP = "chip"
CORE = "core"
ALL = (ROWS, CHIP, CORE)
SWAP = [(0, 1), (1, 0)]
SLOTS = (
    (
        (2, 6, 3, 5, 0, 4, 1, 7),
        (7, 3, 6, 2, 5, 1, 4, 0),
        (3, 5, 0, 4, 1, 7, 2, 6),
        (4, 0, 5, 1, 6, 2, 7, 3),
        (4, 0, 7, 3, 6, 2, 5, 1),
        (1, 5, 2, 6, 3, 7, 0, 4),
        (7, 3, 6, 2, 5, 1, 4, 0),
        (2, 4, 3, 7, 0, 6, 1, 5),
    ),
    (
        (2, 6, 1, 7, 0, 4, 3, 5),
        (7, 3, 4, 0, 5, 1, 6, 2),
        (3, 7, 0, 4, 1, 5, 2, 6),
        (6, 0, 5, 1, 4, 2, 7, 3),
        (4, 0, 7, 1, 6, 2, 5, 3),
        (1, 5, 0, 6, 3, 7, 2, 4),
        (7, 3, 6, 2, 5, 1, 4, 0),
        (2, 4, 3, 7, 0, 6, 1, 5),
    ),
)
W = 128
f32 = jnp.float32
bf16 = jnp.bfloat16
HI = lax.Precision.HIGHEST


def dot(a, b, dims):
    return lax.dot_general(a, b, (dims, ((), ())), precision=HI, preferred_element_type=f32)


def nn(a, b):
    return dot(a, b, ((1,), (0,)))


def tn(a, b):
    return dot(a, b, ((0,), (0,)))


def nt(a, b):
    return dot(a, b, ((1,), (1,)))


def pieces(x):
    a = x.astype(bf16)
    rest = x - a.astype(f32)
    b = rest.astype(bf16)
    return a, b, (rest - b.astype(f32)).astype(bf16)


def outer(left, panel):
    a0, a1, a2 = pieces(left)
    b0, b1, b2 = pieces(panel)
    return lax.dot_general(
        jnp.concatenate([a0, a0, a1, a0, a2, a1]),
        jnp.concatenate([b0, b1, b0, b2, b0, b1]),
        (((0,), (0,)), ((), ())),
        preferred_element_type=f32,
    )


BAND = 16


def factor(gram):
    sub = lax.broadcasted_iota(jnp.int32, (BAND, W), 0)
    lane = lax.broadcasted_iota(jnp.int32, (BAND, W), 1)
    eye = lax.broadcasted_iota(jnp.int32, (W, W), 0) == lax.broadcasted_iota(jnp.int32, (W, W), 1)
    rest = jnp.concatenate([gram, eye.astype(f32)], axis=1)
    now, rest = rest[:BAND], rest[BAND:]
    upper, inverse = [], []
    for base in range(0, W, BAND):
        left, right = now[:, :W], now[:, W:]
        cols = [jnp.broadcast_to(left[:, base + k : base + k + 1], (BAND, W)) for k in range(BAND)]
        scale = jnp.zeros((BAND, W), f32)
        for k in range(0, BAND, 2):
            top = k // 8 * 8
            here = sub[top:]

            def line(x, i):
                return jnp.broadcast_to(x[i : i + 1, :], (BAND - top, W))

            def below(old, new):
                return new if top == 0 else jnp.concatenate([old[:top], new])

            c, d = cols[k][top:], cols[k + 1][top:]
            p, q, r = line(cols[k], k), line(cols[k + 1], k), line(cols[k + 1], k + 1)
            det = p * r - q * q
            inv_p = 1.0 / p
            inv = 1.0 / det
            later = here > k + 1
            u = jnp.where(later, (c * r - d * q) * inv, jnp.where(here == k + 1, q * inv_p, 0.0))
            v = jnp.where(later, (d * p - c * q) * inv, 0.0)
            last_scale = jnp.where(here == k + 1, lax.rsqrt(det * inv_p), scale[top:])
            scale = below(scale, jnp.where(here == k, lax.rsqrt(p), last_scale))

            def update(x):
                return below(x, x[top:] - u * line(x, k) - v * line(x, k + 1))

            for m in range(k + 2, BAND):
                cols[m] = update(cols[m])
            left = update(left)
            right = update(right)
        left = jnp.where(lane >= base + sub, left * scale, 0.0)
        right = right * scale
        upper.append(left)
        inverse.append(right)
        end = base + BAND
        if end < W:
            panel = jnp.concatenate([left, right], axis=1)
            now = rest[:BAND] - outer(left[:, end : end + BAND], panel)
            if end + BAND < W:
                rest = rest[BAND:] - outer(left[:, end + BAND :], panel)
    return jnp.concatenate(upper), jnp.concatenate(inverse)


def blocks_of(ref, start, count):
    return ref[:, start : start + count, :].reshape(ref.shape[0] * count, W)


def turned_blocks(ref, place, table, start, count, parts, core):
    first = (core * ref.shape[0] + place[0]) * ref.shape[0]
    return jnp.concatenate([ref[table[first + p], start : start + count, :] for p in parts])


def first_factor(start, out):
    g00, cee = start[:W, :], start[W:, :]
    li0 = factor(g00)[1]
    u = nt(cee, li0)
    side = nn(li0, g00)
    for i, block in enumerate([li0, u, nn(side, u), nt(side, li0)]):
        out[i * W : (i + 1) * W, :] = block


def middle(start, ready, keep, got, pack, stage, sems):
    g00, cee = start[:W, :], start[W:, :]
    li0, u, h0, m00 = (ready[i * W : (i + 1) * W, :] for i in range(4))
    g01, g11 = (keep[i * W : (i + 1) * W, :] + got[i * W : (i + 1) * W, :] for i in range(2))
    x0 = li0.T
    side = jnp.concatenate([g00, g01], axis=1)
    gram = jnp.concatenate([side, jnp.concatenate([g01.T, g11], axis=1)])
    h = h0 + nt(nn(li0, g01), li0)
    h_full = h + (h - nn(m00, h))
    g02 = g11 + tn(cee, g01)
    for i, block in enumerate([h, h_full, m00, g02, li0]):
        stage[i * W : (i + 1) * W, :] = block
    pack_copy(stage, pack, sems, 0).start()
    comb = jnp.concatenate([u - nn(x0, h_full), x0])
    y = nn(gram, comb)
    upper1, li1 = factor(tn(comb, y))
    c1 = nt(comb, li1)
    y1 = nt(y, li1)
    m01 = nn(li0, y1[:W])
    i1 = jnp.concatenate([nn(cee, c1[:W]), c1])
    s0 = nn(jnp.concatenate([side, g02], axis=1), i1)
    s1 = nn(gram[W:], i1[: 2 * W])
    late = [upper1, i1[:W], i1[W : 2 * W], i1[2 * W :], m01, tn(c1, y1), nn(li0, s0), tn(c1[:W], s0), s1]
    late.append(tn(i1[:W], s0))
    for i, block in enumerate(late):
        stage[EARLY + i * W : EARLY + (i + 1) * W, :] = block
    second = pack_copy(stage, pack, sems, 1)
    second.start()
    pack_copy(stage, pack, sems, 0).wait()
    second.wait()


EARLY = 5 * W
PACK = 15 * W


def pack_copy(source, target, sems, late):
    lines = pl.ds(EARLY, PACK - EARLY) if late else pl.ds(0, EARLY)
    return pltpu.make_async_copy(source.at[lines, :], target.at[lines, :], sems.at[late])


def last(scale, packed, totals, mix, projection, first_pass, pack, sems, parts, total_sem):
    copies = [pack_copy(packed, pack, sems, i) for i in range(2)]
    summands = pltpu.make_async_copy(totals, parts, total_sem)
    summands.start()
    for copy in copies:
        copy.start()
    summands.wait()
    a12, a22 = unpacked(parts[...])
    for copy in copies:
        copy.wait()
    first, full, m00, a02, li0, upper1, _, c1_top, c1_low, m01, m11, first0, part1, s1, square = (
        pack[i * W : (i + 1) * W, :] for i in range(PACK // W)
    )
    i1 = pack[EARLY + W : EARLY + 4 * W, :]
    c1 = i1[W:]
    s1 = s1 + nn(a12, c1_low)
    s2 = nn(jnp.concatenate([a02.T, a12, a22], axis=1), i1)
    square = square + tn(c1, jnp.concatenate([s1, s2]))
    h = jnp.concatenate([first0, part1 + tn(c1_low, s1)])
    gram_p = jnp.concatenate([jnp.concatenate([m00, m01], axis=1), jnp.concatenate([m01.T, m11], axis=1)])
    h_full = h + (h - nn(gram_p, h))
    inner = tn(h, h_full)
    upper2, li2 = factor(square - inner - inner.T + tn(h_full, nn(gram_p, h_full)))
    zero = jnp.zeros((W, W), f32)
    places = jnp.concatenate([jnp.concatenate([li0.T, zero]), c1], axis=1)
    comb = jnp.concatenate([i1[: 2 * W] - nn(places, h_full), i1[2 * W :]])
    mix[: 2 * W, : 2 * W] = places * scale
    mix[2 * W :, : 2 * W] = jnp.zeros((W, 2 * W), f32)
    mix[:, 2 * W :] = nt(comb, li2) * scale
    projection[:W, :W] = full
    projection[W : 2 * W, :W] = upper1
    projection[2 * W :, :W] = zero
    projection[: 2 * W, W:] = h_full
    projection[2 * W :, W:] = upper2
    first_pass[:W, :W] = first
    first_pass[W:, :W] = jnp.zeros((2 * W, W), f32)
    first_pass[: 2 * W, W:] = h
    first_pass[2 * W :, W:] = zero


HBM = pl.BlockSpec(memory_space=pltpu.HBM)
VMEM = pl.BlockSpec(memory_space=pltpu.VMEM)
SMEM = pl.BlockSpec(memory_space=pltpu.SMEM)


def room(mib):
    return pltpu.CompilerParams(vmem_limit_bytes=mib * 2**20)


def kernel(body, shapes, *args):
    return pl.pallas_call(
        body,
        out_shape=[jax.ShapeDtypeStruct(s, f32) for s in shapes],
        in_specs=[VMEM if a.dtype == f32 else SMEM for a in args],
        out_specs=[VMEM] * len(shapes),
        compiler_params=room(16),
    )(*args)


def halves(x):
    high = x.astype(bf16)
    return high, (x - high.astype(f32)).astype(bf16)


def mm(a, b):
    return lax.dot_general(a, b, (((1,), (0,)), ((), ())), preferred_element_type=f32)


def pick_rows(place, seeds, lanes, covariance, out, buffer, sem):
    count = seeds.shape[0]
    height = covariance.shape[0]
    base = place[0] * height

    def row(line, i):
        return pltpu.make_async_copy(covariance.at[pl.ds(line, 1), :], buffer.at[pl.ds(i, 1), :], sem)

    def body(i, found):
        line = seeds[i] - base
        here = (line >= 0) & (line < height)

        @pl.when(here)
        def _():
            row(line, i).start()

        return found + here.astype(jnp.int32)

    found = lax.fori_loop(0, count, body, 0, unroll=8)
    offsets = jnp.broadcast_to(lanes[...] - base, (count, count))
    held = jnp.where((offsets >= 0) & (offsets < height), 1.0, 0.0).T > 0

    def done(i, carry):
        row(0, 0).wait()
        return carry

    lax.fori_loop(0, found, done, 0)
    for p in range(out.shape[0]):
        out[p] = jnp.where(held, buffer[:, p * W : (p + 1) * W], 0.0)


def picked_rows(place, seeds, covariance, parts):
    count = seeds.shape[0]
    return pl.pallas_call(
        pick_rows,
        out_shape=jax.ShapeDtypeStruct((parts, count, W), f32),
        in_specs=[SMEM, SMEM, VMEM, HBM],
        out_specs=VMEM,
        scratch_shapes=[pltpu.VMEM((count, covariance.shape[1]), f32), pltpu.SemaphoreType.DMA],
        compiler_params=room(50),
    )(place, seeds, seeds.reshape(1, count), covariance)


CHUNKS = 8


def hold_rows(covariance, out, sem):
    tall = out.shape[0]
    copy = pltpu.make_async_copy(covariance.at[pl.ds(covariance.shape[0] - tall, tall), :], out, sem)
    copy.start()
    copy.wait()


def held_rows(covariance, chunks):
    height, breadth = covariance.shape
    return pl.pallas_call(
        hold_rows,
        out_shape=pltpu.VMEM((height // CHUNKS * chunks, breadth), f32),
        in_specs=[HBM],
        out_specs=VMEM,
        scratch_shapes=[pltpu.SemaphoreType.DMA],
        compiler_params=room(57),
    )(covariance)


def chunks_of(covariance, held, buffer, sems):
    tall = covariance.shape[0] // CHUNKS
    streamed = buffer.shape[0]
    copies = [
        pltpu.make_async_copy(covariance.at[pl.ds(i * tall, tall), :], buffer.at[i], sems.at[i]) for i in range(streamed)
    ]
    for copy in copies:
        copy.start()
    chunks = [(streamed + i, lambda i=i: held[i * tall : (i + 1) * tall, :]) for i in range(CHUNKS - streamed)]

    def arrived(i):
        copies[i].wait()
        return buffer[i]

    return chunks + [(i, lambda i=i: arrived(i)) for i in range(streamed)]


def chunk_scratch(covariance, held):
    height, breadth = covariance.shape
    streamed = CHUNKS - held * CHUNKS // height
    return [pltpu.VMEM((streamed, height // CHUNKS, breadth), f32), pltpu.SemaphoreType.DMA((streamed,))]


def first_product(place, lanes, covariance, held, start, keep, send, buffer, sems):
    height, breadth = covariance.shape
    half = height // 2
    tall = height // CHUNKS
    chunks = chunks_of(covariance, held, buffer, sems)
    lines = lax.broadcasted_iota(jnp.int32, (breadth, W), 0) + place[2] * breadth
    hot = jnp.where(lines == lanes[...], 1.0, 0.0)
    hit = jnp.max(hot, axis=1, keepdims=True) > 0
    weights = jnp.concatenate(halves(jnp.where(hit, 0.0, start[...])), axis=1)
    first = place[1] == 0
    for i, read in chunks:
        high, low = halves(read())
        both = mm(high, weights)
        value = both[:, :W] + both[:, W:] + mm(low, weights[:, :W])
        mine = first if i * tall < half else jnp.logical_not(first)

        def store(out):
            for q in range(tall // W):
                out[i * tall % half // W + q] = value[q * W : (q + 1) * W, :]

        @pl.when(mine)
        def _():
            store(keep)

        @pl.when(jnp.logical_not(mine))
        def _():
            store(send)


def image_of_start(place, seeds, covariance, held, start):
    height = covariance.shape[0]
    shape = jax.ShapeDtypeStruct((height // 2 // W, W, W), f32)
    return pl.pallas_call(
        first_product,
        out_shape=[shape, shape],
        in_specs=[SMEM, VMEM, HBM, VMEM, VMEM],
        out_specs=[VMEM] * 2,
        scratch_shapes=chunk_scratch(covariance, held.shape[0]),
        compiler_params=room(50),
    )(place, seeds.reshape(1, W), covariance, held, start)


def start_grams(place, lanes, start, out):
    block = start[...]
    lines = lax.broadcasted_iota(jnp.int32, block.shape, 0) + place[2] * block.shape[0]
    hot_t = jnp.where(lines == lanes[...], 1.0, 0.0).T.astype(bf16)
    b0, b1, b2 = pieces(block)
    turned_block = block.T
    high_t, low_t = halves(turned_block)
    both = mm(jnp.concatenate([hot_t, high_t]), jnp.concatenate([b0, b1], axis=1))
    cee = both[:W, :W] + both[:W, W:] + mm(hot_t, b2)
    g00 = both[W:, :W] + both[W:, W:] + mm(low_t, b0)
    parts = out.shape[0]
    bit = W // parts
    for p in range(parts):
        lines = slice(p * bit, (p + 1) * bit)
        out[p, :bit, :] = g00[lines]
        out[p, bit:, :] = cee[lines]


def grams_of_start(place, seeds, start, parts):
    return pl.pallas_call(
        start_grams,
        out_shape=jax.ShapeDtypeStruct((parts, 2 * W // parts, W), f32),
        in_specs=[SMEM, VMEM, VMEM],
        out_specs=VMEM,
        compiler_params=room(16),
    )(place, seeds.reshape(1, W), start)


def cross(a, b):
    right = halves(b)
    high, low = halves(a.T)
    both = mm(high, jnp.concatenate(right, axis=1))
    return both[:, :W] + both[:, W:] + mm(low, right[0])


def fold(parts, out):
    out[...] = jnp.sum(parts[...], axis=0)


def fold_turned(parts, out):
    out[...] = jnp.sum(parts[...], axis=0).T


def step_grams(place, table, mine, out):
    parts = mine.shape[0]
    step = blocks_of(mine, 0, W)
    start = turned_blocks(mine, place, table, W + 2 * W // parts, W, range(parts), place[1])
    out[:W, :] = cross(start, step)
    out[W:, :] = cross(step, step)


def corner():
    return lax.broadcasted_iota(jnp.int32, (W, W), 0), lax.broadcasted_iota(jnp.int32, (W, W), 1)


SPARE = 8


def next_grams(place, table, mine, following, out):
    parts = mine.shape[0]
    bit = W // parts
    step = blocks_of(mine, 0, W)
    then, g01, g11 = (
        turned_blocks(following, place, table, s, n, range(parts), place[1])
        for s, n in ((0, W), (W, bit), (W + bit, bit))
    )
    g12, g22 = cross(step, then), cross(then, then)
    i, j = corner()
    out[:W, :] = g01
    out[W : 2 * W, :] = g11
    out[2 * W : 3 * W, :] = jnp.where(j >= i, g22, g12)
    diagonal = jnp.sum(jnp.where(i == j, g12, 0.0), axis=0, keepdims=True)
    out[3 * W :, :] = jnp.broadcast_to(diagonal, (SPARE, W))


def unpacked(totals):
    total = jnp.sum(totals, axis=0)
    body = total[:W]
    i, j = corner()
    lower = jnp.where(j < i, body, 0.0)
    g12 = lower + lower.T + jnp.where(i == j, total[W : W + 1], 0.0)
    return g12, jnp.where(j >= i, body, 0.0) + jnp.where(j > i, body, 0.0).T


def second_product(place, covariance, mine, theirs, grams, out, small, buffer, sems, total):
    height, breadth = covariance.shape
    half = height // 2
    tall = height // CHUNKS
    chunks = chunks_of(covariance, None, buffer, sems)
    first = place[1] == 0
    parts = out.shape[0]
    bit = W // parts
    for p in range(parts):
        out[p, W : W + bit, :] = grams[p * bit : (p + 1) * bit, :]
        out[p, W + bit :, :] = grams[W + p * bit : W + (p + 1) * bit, :]
    for i in range(2):
        lines = W + i * bit
        small[i * W : (i + 1) * W, :] = blocks_of(mine, lines, bit) + blocks_of(theirs, lines, bit)
    for i, read in chunks:
        lines = slice(i * tall % half // W, (i * tall % half + tall) // W)
        own, other = (mine, theirs) if i * tall < half else (theirs, mine)
        block = jnp.where(first, own[lines, :W, :], other[lines, :W, :]).reshape(tall, W)
        v_high, v_low = halves(block.T)
        high, low = halves(read())
        both = mm(jnp.concatenate([v_high, v_low]), high)
        value = both[:W] + both[W:] + mm(v_high, low)
        if i == chunks[0][0]:
            total[...] = value
        elif i != chunks[-1][0]:
            total[...] += value
        else:
            value += total[...]
            for p in range(parts):
                out[p, :W, :] = value[:, p * W : (p + 1) * W].T


def image_of_step(place, covariance, mine, theirs, grams):
    breadth = covariance.shape[1]
    parts = breadth // W
    return pl.pallas_call(
        second_product,
        out_shape=[
            jax.ShapeDtypeStruct((parts, W + 2 * (W // parts), W), f32),
            jax.ShapeDtypeStruct((2 * W, W), f32),
        ],
        in_specs=[SMEM, HBM] + [VMEM] * 3,
        out_specs=[VMEM] * 2,
        scratch_shapes=chunk_scratch(covariance, 0) + [pltpu.VMEM((W, breadth), f32)],
        compiler_params=room(50),
    )(place, covariance, mine, theirs, grams)


def basis_rows(place, table, mine, mine_next, theirs, theirs_next, mix, *refs):
    small_in, (out, *small_out), (stage, sems, small_sems) = refs[:2], refs[2:5], refs[5:]
    copies = [pltpu.make_async_copy(a, b, small_sems.at[i]) for i, (a, b) in enumerate(zip(small_in, small_out))]
    for copy in copies:
        copy.start()
    parts = mine.shape[0]
    bit = 2 * W // parts
    count, tall, _ = stage.shape
    half = count * tall // 2
    high, low = halves(mix[: 2 * W, : 2 * W])
    tip_high, tip_low = halves(mix[:, 2 * W :])
    tip = jnp.concatenate([tip_high, tip_low], axis=1)
    for i in range(count):
        line = i * tall % half
        pair, following, side = (mine, mine_next, place[1]) if i * tall < half else (theirs, theirs_next, 1 - place[1])
        order = range(line // W, (line + tall) // W)
        left = jnp.concatenate(
            [
                turned_blocks(pair, place, table, W + bit, W, order, side),
                pair[line // W : (line + tall) // W, :W, :].reshape(tall, W),
                turned_blocks(following, place, table, 0, W, order, side),
            ],
            axis=1,
        )
        l_high, l_low = halves(left)
        h2, l2 = l_high[:, : 2 * W], l_low[:, : 2 * W]
        stage[i, :, : 2 * W] = mm(h2, high) + mm(h2, low) + mm(l2, high)
        both = mm(l_high, tip)
        stage[i, :, 2 * W :] = both[:, :W] + both[:, W:] + mm(l_low, tip_high)
        rows = pl.ds(pl.multiple_of(side * half + line, tall), tall)
        copies.append(pltpu.make_async_copy(stage.at[i], out.at[rows, :], sems.at[i]))
        copies[-1].start()
    for copy in copies:
        copy.wait()


def basis_of(place, table, mine, mine_next, theirs, theirs_next, mix, *small):
    height = 2 * mine.shape[0] * W
    tall = 256
    breadth = mix.shape[1]
    return pl.pallas_call(
        basis_rows,
        out_shape=[jax.ShapeDtypeStruct(s, f32) for s in ((height, breadth), *(a.shape for a in small))],
        in_specs=[SMEM] * 2 + [VMEM] * 7,
        out_specs=[HBM] * 3,
        scratch_shapes=[
            pltpu.VMEM((height // tall, tall, breadth), f32),
            pltpu.SemaphoreType.DMA((height // tall,)),
            pltpu.SemaphoreType.DMA((2,)),
        ],
        compiler_params=room(24),
    )(place, table, mine, mine_next, theirs, theirs_next, mix, *small)


def scattered(parts, axis):
    return jnp.sum(lax.all_to_all(parts, axis, 0, 0, tiled=True), axis=0)


def gathered(part, axis):
    copies = jnp.broadcast_to(part, (lax.axis_size(axis), *part.shape))
    return lax.all_to_all(copies, axis, 0, 0, tiled=True)


def other_core(value):
    return lax.ppermute(value, CORE, SWAP)


def turned(rows, chips, cores):
    return [
        ((r * chips + a) * cores + b, (a * chips + SLOTS[b][a][r]) * cores + b)
        for r in range(rows)
        for a in range(chips)
        for b in range(cores)
    ]


def local(covariance, seed_index):
    height, breadth = covariance.shape
    width = seed_index.shape[0]
    rows, chips, cores = (lax.axis_size(a) for a in ALL)
    row, chip, core = (lax.axis_index(a) for a in ALL)
    order = height * rows
    turn = turned(rows, chips, cores)
    table = jnp.array(SLOTS, jnp.int32).reshape(-1)
    place = jnp.stack([row, core, chip * cores + core]).astype(jnp.int32)
    picked = picked_rows(place, seed_index, covariance, rows)
    (start_piece,) = kernel(fold_turned, [(breadth // rows, width)], lax.all_to_all(picked, ROWS, 0, 0, tiled=True))
    block, start_piece = lax.optimization_barrier((covariance, start_piece))
    held = held_rows(block, 2)
    start_turned = lax.ppermute(start_piece, ALL, turn)
    start = gathered(start_piece, ROWS).reshape(breadth, width)
    start, start_turned, held = lax.optimization_barrier((start, start_turned, held))
    keep, send = image_of_start(place, seed_index, covariance, held, start)
    got = other_core(send)
    small = grams_of_start(place, seed_index, start, chips)
    parts = jnp.concatenate([keep + got, small], axis=1)
    mine = gathered(jnp.concatenate([scattered(parts, CHIP), start_turned]), CHIP)
    theirs = other_core(mine)
    (grams,) = kernel(step_grams, [(2 * width, width)], place, table, mine)
    parts, zero_grams = image_of_step(place, covariance, mine, theirs, grams)
    (piece,) = kernel(fold, [parts.shape[1:]], lax.all_to_all(parts, ROWS, 0, 0, tiled=True))
    piece = lax.ppermute(piece, ALL, turn)
    (ready,) = kernel(first_factor, [(4 * width, width)], zero_grams)
    mine_next, ready = lax.optimization_barrier((gathered(piece, CHIP), ready))
    (keep,) = kernel(next_grams, [(3 * width + SPARE, width)], place, table, mine, mine_next)
    got = other_core(keep)
    totals = gathered(keep[2 * width :] + got[2 * width :], ROWS)
    theirs_next = other_core(mine_next)
    stage = [pltpu.VMEM((PACK, width), f32), pltpu.SemaphoreType.DMA((2,))]
    pack = pl.pallas_call(
        middle,
        out_shape=jax.ShapeDtypeStruct((PACK, width), f32),
        in_specs=[VMEM] * 4,
        out_specs=HBM,
        scratch_shapes=stage,
        compiler_params=room(60),
    )(zero_grams, ready, keep, got)
    totals, pack = lax.optimization_barrier((totals, pack))
    scale = float(order) ** 0.5

    def last_step(*refs):
        last(f32(scale), *refs)

    shapes = [(3 * width, 3 * width), (3 * width, 2 * width), (3 * width, 2 * width)]
    mix, projection, first_pass = pl.pallas_call(
        last_step,
        out_shape=[jax.ShapeDtypeStruct(s, f32) for s in shapes],
        in_specs=[HBM, HBM],
        out_specs=[VMEM] * 3,
        scratch_shapes=stage + [pltpu.VMEM(totals.shape, f32), pltpu.SemaphoreType.DMA],
        compiler_params=room(52),
    )(pack, totals)
    return tuple(basis_of(place, table, mine, mine_next, theirs, theirs_next, mix, projection, first_pass))


def solution(mesh):
    rows, cols = mesh.devices.shape
    fine = Mesh(mesh.devices.reshape(rows, cols // 2, 2), ALL)
    return jax.shard_map(
        local,
        mesh=fine,
        in_specs=(P(ROWS, (CHIP, CORE)), P()),
        out_specs=(P(ROWS, None), P(), P()),
        check_vma=False,
    )
```

```python
import jax
import jax.numpy as jnp
from jax import lax
from jax.experimental import pallas as pl
from jax.experimental.pallas import tpu as pltpu
from jax.sharding import Mesh, PartitionSpec as P

ROWS = "row"
CHIP = "chip"
CORE = "core"
ALL = (ROWS, CHIP, CORE)
SWAP = [(0, 1), (1, 0)]
SLOTS = (
    (
        (2, 6, 3, 5, 0, 4, 1, 7),
        (7, 3, 6, 2, 5, 1, 4, 0),
        (3, 5, 0, 4, 1, 7, 2, 6),
        (4, 0, 5, 1, 6, 2, 7, 3),
        (4, 0, 7, 3, 6, 2, 5, 1),
        (1, 5, 2, 6, 3, 7, 0, 4),
        (7, 3, 6, 2, 5, 1, 4, 0),
        (2, 4, 3, 7, 0, 6, 1, 5),
    ),
    (
        (2, 6, 1, 7, 0, 4, 3, 5),
        (7, 3, 4, 0, 5, 1, 6, 2),
        (3, 7, 0, 4, 1, 5, 2, 6),
        (6, 0, 5, 1, 4, 2, 7, 3),
        (4, 0, 7, 1, 6, 2, 5, 3),
        (1, 5, 0, 6, 3, 7, 2, 4),
        (7, 3, 6, 2, 5, 1, 4, 0),
        (2, 4, 3, 7, 0, 6, 1, 5),
    ),
)
W = 128
f32 = jnp.float32
bf16 = jnp.bfloat16
HI = lax.Precision.HIGHEST


def dot(a, b, dims):
    return lax.dot_general(a, b, (dims, ((), ())), precision=HI, preferred_element_type=f32)


def nn(a, b):
    return dot(a, b, ((1,), (0,)))


def tn(a, b):
    return dot(a, b, ((0,), (0,)))


def nt(a, b):
    return dot(a, b, ((1,), (1,)))


def pieces(x):
    a = x.astype(bf16)
    rest = x - a.astype(f32)
    b = rest.astype(bf16)
    return a, b, (rest - b.astype(f32)).astype(bf16)


def outer(left, panel):
    a0, a1, a2 = pieces(left)
    b0, b1, b2 = pieces(panel)
    return lax.dot_general(
        jnp.concatenate([a0, a0, a1, a0, a2, a1]),
        jnp.concatenate([b0, b1, b0, b2, b0, b1]),
        (((0,), (0,)), ((), ())),
        preferred_element_type=f32,
    )


BAND = 16


def factor(gram):
    sub = lax.broadcasted_iota(jnp.int32, (BAND, W), 0)
    lane = lax.broadcasted_iota(jnp.int32, (BAND, W), 1)
    eye = lax.broadcasted_iota(jnp.int32, (W, W), 0) == lax.broadcasted_iota(jnp.int32, (W, W), 1)
    rest = jnp.concatenate([gram, eye.astype(f32)], axis=1)
    now, rest = rest[:BAND], rest[BAND:]
    upper, inverse = [], []
    for base in range(0, W, BAND):
        left, right = now[:, :W], now[:, W:]
        cols = [jnp.broadcast_to(left[:, base + k : base + k + 1], (BAND, W)) for k in range(BAND)]
        scale = jnp.zeros((BAND, W), f32)
        for k in range(0, BAND, 2):
            top = k // 8 * 8
            here = sub[top:]

            def line(x, i):
                return jnp.broadcast_to(x[i : i + 1, :], (BAND - top, W))

            def below(old, new):
                return new if top == 0 else jnp.concatenate([old[:top], new])

            c, d = cols[k][top:], cols[k + 1][top:]
            p, q, r = line(cols[k], k), line(cols[k + 1], k), line(cols[k + 1], k + 1)
            det = p * r - q * q
            inv_p = 1.0 / p
            inv = 1.0 / det
            later = here > k + 1
            u = jnp.where(later, (c * r - d * q) * inv, jnp.where(here == k + 1, q * inv_p, 0.0))
            v = jnp.where(later, (d * p - c * q) * inv, 0.0)
            last_scale = jnp.where(here == k + 1, lax.rsqrt(det * inv_p), scale[top:])
            scale = below(scale, jnp.where(here == k, lax.rsqrt(p), last_scale))

            def update(x):
                return below(x, x[top:] - u * line(x, k) - v * line(x, k + 1))

            for m in range(k + 2, BAND):
                cols[m] = update(cols[m])
            left = update(left)
            right = update(right)
        left = jnp.where(lane >= base + sub, left * scale, 0.0)
        right = right * scale
        upper.append(left)
        inverse.append(right)
        end = base + BAND
        if end < W:
            panel = jnp.concatenate([left, right], axis=1)
            now = rest[:BAND] - outer(left[:, end : end + BAND], panel)
            if end + BAND < W:
                rest = rest[BAND:] - outer(left[:, end + BAND :], panel)
    return jnp.concatenate(upper), jnp.concatenate(inverse)


def blocks_of(ref, start, count):
    return ref[:, start : start + count, :].reshape(ref.shape[0] * count, W)


def turned_blocks(ref, place, table, start, count, parts, core):
    first = (core * ref.shape[0] + place[0]) * ref.shape[0]
    return jnp.concatenate([ref[table[first + p], start : start + count, :] for p in parts])


def first_factor(start, out):
    g00, cee = start[:W, :], start[W:, :]
    li0 = factor(g00)[1]
    u = nt(cee, li0)
    side = nn(li0, g00)
    for i, block in enumerate([li0, u, nn(side, u), nt(side, li0)]):
        out[i * W : (i + 1) * W, :] = block


def middle(start, ready, keep, got, pack, stage, sems):
    g00, cee = start[:W, :], start[W:, :]
    li0, u, h0, m00 = (ready[i * W : (i + 1) * W, :] for i in range(4))
    g01, g11 = (keep[i * W : (i + 1) * W, :] + got[i * W : (i + 1) * W, :] for i in range(2))
    x0 = li0.T
    side = jnp.concatenate([g00, g01], axis=1)
    gram = jnp.concatenate([side, jnp.concatenate([g01.T, g11], axis=1)])
    h = h0 + nt(nn(li0, g01), li0)
    h_full = h + (h - nn(m00, h))
    g02 = g11 + tn(cee, g01)
    for i, block in enumerate([h, h_full, m00, g02, li0]):
        stage[i * W : (i + 1) * W, :] = block
    pack_copy(stage, pack, sems, 0).start()
    comb = jnp.concatenate([u - nn(x0, h_full), x0])
    y = nn(gram, comb)
    upper1, li1 = factor(tn(comb, y))
    c1 = nt(comb, li1)
    y1 = nt(y, li1)
    m01 = nn(li0, y1[:W])
    i1 = jnp.concatenate([nn(cee, c1[:W]), c1])
    s0 = nn(jnp.concatenate([side, g02], axis=1), i1)
    s1 = nn(gram[W:], i1[: 2 * W])
    late = [upper1, i1[:W], i1[W : 2 * W], i1[2 * W :], m01, tn(c1, y1), nn(li0, s0), tn(c1[:W], s0), s1]
    late.append(tn(i1[:W], s0))
    for i, block in enumerate(late):
        stage[EARLY + i * W : EARLY + (i + 1) * W, :] = block
    second = pack_copy(stage, pack, sems, 1)
    second.start()
    pack_copy(stage, pack, sems, 0).wait()
    second.wait()


EARLY = 5 * W
PACK = 15 * W


def pack_copy(source, target, sems, late):
    lines = pl.ds(EARLY, PACK - EARLY) if late else pl.ds(0, EARLY)
    return pltpu.make_async_copy(source.at[lines, :], target.at[lines, :], sems.at[late])


def last(scale, packed, totals, mix, projection, first_pass, pack, sems, parts, total_sem):
    copies = [pack_copy(packed, pack, sems, i) for i in range(2)]
    summands = pltpu.make_async_copy(totals, parts, total_sem)
    summands.start()
    for copy in copies:
        copy.start()
    summands.wait()
    a12, a22 = unpacked(parts[...])
    for copy in copies:
        copy.wait()
    first, full, m00, a02, li0, upper1, _, _, c1_low, m01, m11, first0, part1, s1, square = (
        pack[i * W : (i + 1) * W, :] for i in range(PACK // W)
    )
    i1 = pack[EARLY + W : EARLY + 4 * W, :]
    c1 = i1[W:]
    s1 = s1 + nn(a12, c1_low)
    s2 = nn(jnp.concatenate([a02.T, a12, a22], axis=1), i1)
    square = square + tn(c1, jnp.concatenate([s1, s2]))
    h = jnp.concatenate([first0, part1 + tn(c1_low, s1)])
    gram_p = jnp.concatenate([jnp.concatenate([m00, m01], axis=1), jnp.concatenate([m01.T, m11], axis=1)])
    h_full = h + (h - nn(gram_p, h))
    inner = tn(h, h_full)
    upper2, li2 = factor(square - inner - inner.T + tn(h_full, nn(gram_p, h_full)))
    zero = jnp.zeros((W, W), f32)
    places = jnp.concatenate([jnp.concatenate([li0.T, zero]), c1], axis=1)
    comb = jnp.concatenate([i1[: 2 * W] - nn(places, h_full), i1[2 * W :]])
    mix[: 2 * W, : 2 * W] = places * scale
    mix[2 * W :, : 2 * W] = jnp.zeros((W, 2 * W), f32)
    mix[:, 2 * W :] = nt(comb, li2) * scale
    projection[:W, :W] = full
    projection[W : 2 * W, :W] = upper1
    projection[2 * W :, :W] = zero
    projection[: 2 * W, W:] = h_full
    projection[2 * W :, W:] = upper2
    first_pass[:W, :W] = first
    first_pass[W:, :W] = jnp.zeros((2 * W, W), f32)
    first_pass[: 2 * W, W:] = h
    first_pass[2 * W :, W:] = zero


HBM = pl.BlockSpec(memory_space=pltpu.HBM)
VMEM = pl.BlockSpec(memory_space=pltpu.VMEM)
SMEM = pl.BlockSpec(memory_space=pltpu.SMEM)


def room(mib):
    return pltpu.CompilerParams(vmem_limit_bytes=mib * 2**20)


def kernel(body, shapes, *args):
    return pl.pallas_call(
        body,
        out_shape=[jax.ShapeDtypeStruct(s, f32) for s in shapes],
        in_specs=[VMEM if a.dtype == f32 else SMEM for a in args],
        out_specs=[VMEM] * len(shapes),
        compiler_params=room(16),
    )(*args)


def halves(x):
    high = x.astype(bf16)
    return high, (x - high.astype(f32)).astype(bf16)


def mm(a, b):
    return lax.dot_general(a, b, (((1,), (0,)), ((), ())), preferred_element_type=f32)


def pick_rows(place, seeds, lanes, covariance, out, buffer, sem):
    count = seeds.shape[0]
    height = covariance.shape[0]
    base = place[0] * height

    def row(line, i):
        return pltpu.make_async_copy(covariance.at[pl.ds(line, 1), :], buffer.at[pl.ds(i, 1), :], sem)

    def body(i, found):
        line = seeds[i] - base
        here = (line >= 0) & (line < height)

        @pl.when(here)
        def _():
            row(line, i).start()

        return found + here.astype(jnp.int32)

    found = lax.fori_loop(0, count, body, 0, unroll=8)
    offsets = jnp.broadcast_to(lanes[...] - base, (count, count))
    held = jnp.where((offsets >= 0) & (offsets < height), 1.0, 0.0).T > 0

    def done(i, carry):
        row(0, 0).wait()
        return carry

    lax.fori_loop(0, found, done, 0)
    for p in range(out.shape[0]):
        out[p] = jnp.where(held, buffer[:, p * W : (p + 1) * W], 0.0)


def picked_rows(place, seeds, covariance, parts):
    count = seeds.shape[0]
    return pl.pallas_call(
        pick_rows,
        out_shape=jax.ShapeDtypeStruct((parts, count, W), f32),
        in_specs=[SMEM, SMEM, VMEM, HBM],
        out_specs=VMEM,
        scratch_shapes=[pltpu.VMEM((count, covariance.shape[1]), f32), pltpu.SemaphoreType.DMA],
        compiler_params=room(50),
    )(place, seeds, seeds.reshape(1, count), covariance)


CHUNKS = 8


def hold_rows(covariance, out, sem):
    tall = out.shape[0]
    copy = pltpu.make_async_copy(covariance.at[pl.ds(covariance.shape[0] - tall, tall), :], out, sem)
    copy.start()
    copy.wait()


def held_rows(covariance, chunks):
    height, breadth = covariance.shape
    return pl.pallas_call(
        hold_rows,
        out_shape=pltpu.VMEM((height // CHUNKS * chunks, breadth), f32),
        in_specs=[HBM],
        out_specs=VMEM,
        scratch_shapes=[pltpu.SemaphoreType.DMA],
        compiler_params=room(57),
    )(covariance)


def chunks_of(covariance, held, buffer, sems):
    tall = covariance.shape[0] // CHUNKS
    streamed = buffer.shape[0]
    copies = [
        pltpu.make_async_copy(covariance.at[pl.ds(i * tall, tall), :], buffer.at[i], sems.at[i]) for i in range(streamed)
    ]
    for copy in copies:
        copy.start()
    chunks = [(streamed + i, lambda i=i: held[i * tall : (i + 1) * tall, :]) for i in range(CHUNKS - streamed)]

    def arrived(i):
        copies[i].wait()
        return buffer[i]

    return chunks + [(i, lambda i=i: arrived(i)) for i in range(streamed)]


def chunk_scratch(covariance, held):
    height, breadth = covariance.shape
    streamed = CHUNKS - held * CHUNKS // height
    return [pltpu.VMEM((streamed, height // CHUNKS, breadth), f32), pltpu.SemaphoreType.DMA((streamed,))]


def first_product(place, lanes, covariance, held, start, keep, send, buffer, sems):
    height, breadth = covariance.shape
    half = height // 2
    tall = height // CHUNKS
    chunks = chunks_of(covariance, held, buffer, sems)
    lines = lax.broadcasted_iota(jnp.int32, (breadth, W), 0) + place[2] * breadth
    hot = jnp.where(lines == lanes[...], 1.0, 0.0)
    hit = jnp.max(hot, axis=1, keepdims=True) > 0
    weights = jnp.concatenate(halves(jnp.where(hit, 0.0, start[...])), axis=1)
    first = place[1] == 0
    for i, read in chunks:
        high, low = halves(read())
        both = mm(high, weights)
        value = both[:, :W] + both[:, W:] + mm(low, weights[:, :W])
        mine = first if i * tall < half else jnp.logical_not(first)

        def store(out):
            for q in range(tall // W):
                out[i * tall % half // W + q] = value[q * W : (q + 1) * W, :]

        @pl.when(mine)
        def _():
            store(keep)

        @pl.when(jnp.logical_not(mine))
        def _():
            store(send)


def image_of_start(place, seeds, covariance, held, start):
    height = covariance.shape[0]
    shape = jax.ShapeDtypeStruct((height // 2 // W, W, W), f32)
    return pl.pallas_call(
        first_product,
        out_shape=[shape, shape],
        in_specs=[SMEM, VMEM, HBM, VMEM, VMEM],
        out_specs=[VMEM] * 2,
        scratch_shapes=chunk_scratch(covariance, held.shape[0]),
        compiler_params=room(50),
    )(place, seeds.reshape(1, W), covariance, held, start)


def start_grams(place, lanes, start, out):
    block = start[...]
    lines = lax.broadcasted_iota(jnp.int32, block.shape, 0) + place[2] * block.shape[0]
    hot_t = jnp.where(lines == lanes[...], 1.0, 0.0).T.astype(bf16)
    b0, b1, b2 = pieces(block)
    turned_block = block.T
    high_t, low_t = halves(turned_block)
    both = mm(jnp.concatenate([hot_t, high_t]), jnp.concatenate([b0, b1], axis=1))
    cee = both[:W, :W] + both[:W, W:] + mm(hot_t, b2)
    g00 = both[W:, :W] + both[W:, W:] + mm(low_t, b0)
    parts = out.shape[0]
    bit = W // parts
    for p in range(parts):
        lines = slice(p * bit, (p + 1) * bit)
        out[p, :bit, :] = g00[lines]
        out[p, bit:, :] = cee[lines]


def grams_of_start(place, seeds, start, parts):
    return pl.pallas_call(
        start_grams,
        out_shape=jax.ShapeDtypeStruct((parts, 2 * W // parts, W), f32),
        in_specs=[SMEM, VMEM, VMEM],
        out_specs=VMEM,
        compiler_params=room(16),
    )(place, seeds.reshape(1, W), start)


def cross(a, b):
    right = halves(b)
    high, low = halves(a.T)
    both = mm(high, jnp.concatenate(right, axis=1))
    return both[:, :W] + both[:, W:] + mm(low, right[0])


def fold(parts, out):
    out[...] = jnp.sum(parts[...], axis=0)


def fold_turned(parts, out):
    out[...] = jnp.sum(parts[...], axis=0).T


def step_grams(place, table, mine, out):
    parts = mine.shape[0]
    step = blocks_of(mine, 0, W)
    start = turned_blocks(mine, place, table, W + 2 * W // parts, W, range(parts), place[1])
    out[:W, :] = cross(start, step)
    out[W:, :] = cross(step, step)


def corner():
    return lax.broadcasted_iota(jnp.int32, (W, W), 0), lax.broadcasted_iota(jnp.int32, (W, W), 1)


SPARE = 8


def next_grams(place, table, mine, following, out):
    parts = mine.shape[0]
    bit = W // parts
    step = blocks_of(mine, 0, W)
    then, g01, g11 = (
        turned_blocks(following, place, table, s, n, range(parts), place[1])
        for s, n in ((0, W), (W, bit), (W + bit, bit))
    )
    g12, g22 = cross(step, then), cross(then, then)
    i, j = corner()
    out[:W, :] = g01
    out[W : 2 * W, :] = g11
    out[2 * W : 3 * W, :] = jnp.where(j >= i, g22, g12)
    diagonal = jnp.sum(jnp.where(i == j, g12, 0.0), axis=0, keepdims=True)
    out[3 * W :, :] = jnp.broadcast_to(diagonal, (SPARE, W))


def unpacked(totals):
    total = jnp.sum(totals, axis=0)
    body = total[:W]
    i, j = corner()
    lower = jnp.where(j < i, body, 0.0)
    g12 = lower + lower.T + jnp.where(i == j, total[W : W + 1], 0.0)
    return g12, jnp.where(j >= i, body, 0.0) + jnp.where(j > i, body, 0.0).T


def second_product(place, covariance, mine, theirs, grams, out, small, buffer, sems, total):
    height, _ = covariance.shape
    half = height // 2
    tall = height // CHUNKS
    chunks = chunks_of(covariance, None, buffer, sems)
    first = place[1] == 0
    parts = out.shape[0]
    bit = W // parts
    for p in range(parts):
        out[p, W : W + bit, :] = grams[p * bit : (p + 1) * bit, :]
        out[p, W + bit :, :] = grams[W + p * bit : W + (p + 1) * bit, :]
    for i in range(2):
        lines = W + i * bit
        small[i * W : (i + 1) * W, :] = blocks_of(mine, lines, bit) + blocks_of(theirs, lines, bit)
    for i, read in chunks:
        lines = slice(i * tall % half // W, (i * tall % half + tall) // W)
        own, other = (mine, theirs) if i * tall < half else (theirs, mine)
        block = jnp.where(first, own[lines, :W, :], other[lines, :W, :]).reshape(tall, W)
        v_high, v_low = halves(block.T)
        high, low = halves(read())
        both = mm(jnp.concatenate([v_high, v_low]), high)
        value = both[:W] + both[W:] + mm(v_high, low)
        if i == chunks[0][0]:
            total[...] = value
        elif i != chunks[-1][0]:
            total[...] += value
        else:
            value += total[...]
            for p in range(parts):
                out[p, :W, :] = value[:, p * W : (p + 1) * W].T


def image_of_step(place, covariance, mine, theirs, grams):
    breadth = covariance.shape[1]
    parts = breadth // W
    return pl.pallas_call(
        second_product,
        out_shape=[
            jax.ShapeDtypeStruct((parts, W + 2 * (W // parts), W), f32),
            jax.ShapeDtypeStruct((2 * W, W), f32),
        ],
        in_specs=[SMEM, HBM] + [VMEM] * 3,
        out_specs=[VMEM] * 2,
        scratch_shapes=chunk_scratch(covariance, 0) + [pltpu.VMEM((W, breadth), f32)],
        compiler_params=room(50),
    )(place, covariance, mine, theirs, grams)


def basis_rows(place, table, mine, mine_next, theirs, theirs_next, mix, *refs):
    small_in, (out, *small_out), (stage, sems, small_sems) = refs[:2], refs[2:5], refs[5:]
    copies = [pltpu.make_async_copy(a, b, small_sems.at[i]) for i, (a, b) in enumerate(zip(small_in, small_out))]
    for copy in copies:
        copy.start()
    parts = mine.shape[0]
    bit = 2 * W // parts
    count, tall, _ = stage.shape
    half = count * tall // 2
    high, low = halves(mix[: 2 * W, : 2 * W])
    tip_high, tip_low = halves(mix[:, 2 * W :])
    tip = jnp.concatenate([tip_high, tip_low], axis=1)
    for i in range(count):
        line = i * tall % half
        pair, following, side = (mine, mine_next, place[1]) if i * tall < half else (theirs, theirs_next, 1 - place[1])
        order = range(line // W, (line + tall) // W)
        left = jnp.concatenate(
            [
                turned_blocks(pair, place, table, W + bit, W, order, side),
                pair[line // W : (line + tall) // W, :W, :].reshape(tall, W),
                turned_blocks(following, place, table, 0, W, order, side),
            ],
            axis=1,
        )
        l_high, l_low = halves(left)
        h2, l2 = l_high[:, : 2 * W], l_low[:, : 2 * W]
        stage[i, :, : 2 * W] = mm(h2, high) + mm(h2, low) + mm(l2, high)
        both = mm(l_high, tip)
        stage[i, :, 2 * W :] = both[:, :W] + both[:, W:] + mm(l_low, tip_high)
        rows = pl.ds(pl.multiple_of(side * half + line, tall), tall)
        copies.append(pltpu.make_async_copy(stage.at[i], out.at[rows, :], sems.at[i]))
        copies[-1].start()
    for copy in copies:
        copy.wait()


def basis_of(place, table, mine, mine_next, theirs, theirs_next, mix, *small):
    height = 2 * mine.shape[0] * W
    tall = 256
    breadth = mix.shape[1]
    return pl.pallas_call(
        basis_rows,
        out_shape=[jax.ShapeDtypeStruct(s, f32) for s in ((height, breadth), *(a.shape for a in small))],
        in_specs=[SMEM] * 2 + [VMEM] * 7,
        out_specs=[HBM] * 3,
        scratch_shapes=[
            pltpu.VMEM((height // tall, tall, breadth), f32),
            pltpu.SemaphoreType.DMA((height // tall,)),
            pltpu.SemaphoreType.DMA((2,)),
        ],
        compiler_params=room(24),
    )(place, table, mine, mine_next, theirs, theirs_next, mix, *small)


def scattered(parts, axis):
    return jnp.sum(lax.all_to_all(parts, axis, 0, 0, tiled=True), axis=0)


def gathered(part, axis):
    copies = jnp.broadcast_to(part, (lax.axis_size(axis), *part.shape))
    return lax.all_to_all(copies, axis, 0, 0, tiled=True)


def other_core(value):
    return lax.ppermute(value, CORE, SWAP)


def turned(rows, chips, cores):
    return [
        ((r * chips + a) * cores + b, (a * chips + SLOTS[b][a][r]) * cores + b)
        for r in range(rows)
        for a in range(chips)
        for b in range(cores)
    ]


def local(covariance, seed_index):
    height, breadth = covariance.shape
    width = seed_index.shape[0]
    rows, chips, cores = (lax.axis_size(a) for a in ALL)
    row, chip, core = (lax.axis_index(a) for a in ALL)
    order = height * rows
    turn = turned(rows, chips, cores)
    table = jnp.array(SLOTS, jnp.int32).reshape(-1)
    place = jnp.stack([row, core, chip * cores + core]).astype(jnp.int32)
    picked = picked_rows(place, seed_index, covariance, rows)
    (start_piece,) = kernel(fold_turned, [(breadth // rows, width)], lax.all_to_all(picked, ROWS, 0, 0, tiled=True))
    block, start_piece = lax.optimization_barrier((covariance, start_piece))
    held = held_rows(block, 2)
    start = gathered(start_piece, ROWS).reshape(breadth, width)
    start, held = lax.optimization_barrier((start, held))
    keep, send = image_of_start(place, seed_index, covariance, held, start)
    send, start_piece = lax.optimization_barrier((send, start_piece))
    got = other_core(send)
    start_turned = lax.ppermute(start_piece, ALL, turn)
    small = grams_of_start(place, seed_index, start, chips)
    parts = jnp.concatenate([keep + got, small], axis=1)
    mine = gathered(jnp.concatenate([scattered(parts, CHIP), start_turned]), CHIP)
    theirs = other_core(mine)
    (grams,) = kernel(step_grams, [(2 * width, width)], place, table, mine)
    parts, zero_grams = image_of_step(place, covariance, mine, theirs, grams)
    (piece,) = kernel(fold, [parts.shape[1:]], lax.all_to_all(parts, ROWS, 0, 0, tiled=True))
    piece = lax.ppermute(piece, ALL, turn)
    (ready,) = kernel(first_factor, [(4 * width, width)], zero_grams)
    mine_next, ready = lax.optimization_barrier((gathered(piece, CHIP), ready))
    (keep,) = kernel(next_grams, [(3 * width + SPARE, width)], place, table, mine, mine_next)
    got = other_core(keep)
    totals = gathered(keep[2 * width :] + got[2 * width :], ROWS)
    theirs_next = other_core(mine_next)
    stage = [pltpu.VMEM((PACK, width), f32), pltpu.SemaphoreType.DMA((2,))]
    pack = pl.pallas_call(
        middle,
        out_shape=jax.ShapeDtypeStruct((PACK, width), f32),
        in_specs=[VMEM] * 4,
        out_specs=HBM,
        scratch_shapes=stage,
        compiler_params=room(60),
    )(zero_grams, ready, keep, got)
    totals, pack = lax.optimization_barrier((totals, pack))
    scale = float(order) ** 0.5

    def last_step(*refs):
        last(f32(scale), *refs)

    shapes = [(3 * width, 3 * width), (3 * width, 2 * width), (3 * width, 2 * width)]
    mix, projection, first_pass = pl.pallas_call(
        last_step,
        out_shape=[jax.ShapeDtypeStruct(s, f32) for s in shapes],
        in_specs=[HBM, HBM],
        out_specs=[VMEM] * 3,
        scratch_shapes=stage + [pltpu.VMEM(totals.shape, f32), pltpu.SemaphoreType.DMA],
        compiler_params=room(52),
    )(pack, totals)
    return tuple(basis_of(place, table, mine, mine_next, theirs, theirs_next, mix, projection, first_pass))


def solution(mesh):
    rows, cols = mesh.devices.shape
    fine = Mesh(mesh.devices.reshape(rows, cols // 2, 2), ALL)

    return jax.shard_map(
        local,
        mesh=fine,
        in_specs=(P(ROWS, (CHIP, CORE)), P()),
        out_specs=(P(ROWS, None), P(), P()),
        check_vma=False,
    )
```
